32 devices in a mesh: dp: 2 (over x), fsdp: 16 (over z, y, core).
Axes of the slice: x: 2, y: 2, z: 4, core: 2. Of those that a mesh axis runs over, the one named last changes fastest.
Arguments:
- tok_ids: int32 [96, 96], P(('dp', 'fsdp')), parts along dimension 0
- grad_out: bfloat16 [96, 96, 2048], P(('dp', 'fsdp')), parts along dimension 0
- emb_table: bfloat16 [102400, 2048], P('fsdp')
- norm_gain: bfloat16 [2048], P('fsdp')
- w_query: bfloat16 [2048, 3072], P('fsdp')
- w_kv_down: bfloat16 [2048, 576], P('fsdp')
- kv_gain: bfloat16 [512], P('fsdp')
- w_kv_up: bfloat16 [512, 4096], P('fsdp')
- w_out: bfloat16 [2048, 2048], P('fsdp')
Outputs:
- output 1: bfloat16 [96, 96, 2048], P(('dp', 'fsdp')), parts along dimension 0
- output 2: bfloat16 [204800, 2048], P(('dp', 'fsdp')), parts along dimension 0
- output 3: float32 [4096], P(('dp', 'fsdp')), parts along dimension 0
- output 4: float32 [4096, 3072], P(('dp', 'fsdp')), parts along dimension 0
- output 5: float32 [4096, 576], P(('dp', 'fsdp')), parts along dimension 0
- output 6: float32 [1024], P(('dp', 'fsdp')), parts along dimension 0
- output 7: float32 [1024, 4096], P(('dp', 'fsdp')), parts along dimension 0
- output 8: float32 [4096, 2048], P(('dp', 'fsdp')), parts along dimension 0
There are 2 independent parts. The reference program is written for one: setup_inputs(seed, part) draws one part's arguments, and reference() takes and returns one part's arrays. A program takes and returns all parts, laid end to end along the dimension named above; an argument that names none is the same for every part.
All inputs are finite; a program needn't handle non-finite values.
Results may differ from the reference program's by a relative error of at most 0.0117806.
Values are sent between devices in bfloat16 or wider.
A program may use at most 1 GiB of HBM per device.

```python
import math
import jax
import jax.numpy as jnp
from jax import lax

D_MODEL = 2048
N_HEADS = 16
VOCAB_SIZE = 102400
KV_RANK = 512
BATCH_SEQS = 48
SEQ_LEN = 96
NOPE_DIM = 128
ROPE_DIM = 64
VALUE_DIM = 128
HOT_IDS = 64
ROPE_THETA = 50000.0
RMS_EPS = 1e-6
ATTN_SCALE = (NOPE_DIM + ROPE_DIM) ** -0.5 * (0.1 * math.log(32.0) + 1.0) ** 2


def draw_ids(id_key):
    tok_count = BATCH_SEQS * SEQ_LEN
    kind_key, hot_key, mid_key, any_key = jax.random.split(id_key, 4)
    id_kind = jax.random.randint(kind_key, (tok_count,), 0, 4)
    hot_draw = jax.random.randint(hot_key, (tok_count,), 0, HOT_IDS)
    mid_draw = jax.random.randint(mid_key, (tok_count,), 0, VOCAB_SIZE // 8)
    any_draw = jax.random.randint(any_key, (tok_count,), 0, VOCAB_SIZE)
    tok_list = jnp.where(id_kind == 0, hot_draw, jnp.where(id_kind == 1, mid_draw, any_draw))
    tok_list = tok_list.at[0].set(VOCAB_SIZE - 1).at[1].set(0)
    return tok_list.reshape(BATCH_SEQS, SEQ_LEN).astype(jnp.int32)


def setup_inputs(seed: int = 0, part: int = 0) -> dict:
    base_key = jax.random.key(seed)
    shared = jax.random.split(base_key, 7)
    part_keys = jax.random.split(jax.random.fold_in(base_key, part), 2)
    q_width = N_HEADS * (NOPE_DIM + ROPE_DIM)
    up_width = N_HEADS * (NOPE_DIM + VALUE_DIM)
    o_width = N_HEADS * VALUE_DIM
    emb_table = jax.random.normal(shared[0], (VOCAB_SIZE, D_MODEL), jnp.float32).astype(jnp.bfloat16)
    norm_gain = (1.0 + 0.3 * jax.random.normal(shared[1], (D_MODEL,), jnp.float32)).astype(jnp.bfloat16)
    w_query = (jax.random.normal(shared[2], (D_MODEL, q_width), jnp.float32) * D_MODEL ** -0.5).astype(jnp.bfloat16)
    w_kv_down = (jax.random.normal(shared[3], (D_MODEL, KV_RANK + ROPE_DIM), jnp.float32) * D_MODEL ** -0.5).astype(jnp.bfloat16)
    kv_gain = (1.0 + 0.3 * jax.random.normal(shared[4], (KV_RANK,), jnp.float32)).astype(jnp.bfloat16)
    w_kv_up = (jax.random.normal(shared[5], (KV_RANK, up_width), jnp.float32) * KV_RANK ** -0.5).astype(jnp.bfloat16)
    w_out = (jax.random.normal(shared[6], (o_width, D_MODEL), jnp.float32) * o_width ** -0.5).astype(jnp.bfloat16)
    tok_ids = draw_ids(part_keys[0])
    grad_out = jax.random.normal(part_keys[1], (BATCH_SEQS, SEQ_LEN, D_MODEL), jnp.float32).astype(jnp.bfloat16)
    return {'tok_ids': tok_ids, 'grad_out': grad_out, 'emb_table': emb_table, 'norm_gain': norm_gain, 'w_query': w_query, 'w_kv_down': w_kv_down, 'kv_gain': kv_gain, 'w_kv_up': w_kv_up, 'w_out': w_out}


def rms_scale(in_vals, gain_vec):
    vals_f32 = in_vals.astype(jnp.float32)
    inv_rms = lax.rsqrt(jnp.mean(vals_f32 * vals_f32, axis=-1, keepdims=True) + RMS_EPS)
    return (vals_f32 * inv_rms * gain_vec.astype(jnp.float32)).astype(jnp.bfloat16)


def rope_tables():
    positions = jnp.arange(SEQ_LEN, dtype=jnp.float32)
    inv_freq = ROPE_THETA ** (-2.0 * jnp.arange(ROPE_DIM // 2, dtype=jnp.float32) / ROPE_DIM)
    rot_angle = positions[:, None] * inv_freq[None, :]
    rot_angle = jnp.concatenate([rot_angle, rot_angle], axis=-1)
    return jnp.cos(rot_angle), jnp.sin(rot_angle)


def apply_rope(in_vals, cos_tab, sin_tab):
    half_dim = ROPE_DIM // 2
    vals_f32 = in_vals.astype(jnp.float32)
    turned = jnp.concatenate([-vals_f32[..., half_dim:], vals_f32[..., :half_dim]], axis=-1)
    return (vals_f32 * cos_tab + turned * sin_tab).astype(jnp.bfloat16)


def attend_one(q_seq, pe_seq, kv_seq):
    cos_tab, sin_tab = rope_tables()
    q_rot = apply_rope(q_seq[:, :, NOPE_DIM:], cos_tab[:, None, :], sin_tab[:, None, :])
    k_rot = apply_rope(pe_seq, cos_tab, sin_tab)
    scores = jnp.einsum('shd,thd->hst', q_seq[:, :, :NOPE_DIM].astype(jnp.float32), kv_seq[:, :, :NOPE_DIM].astype(jnp.float32))
    scores = scores + jnp.einsum('shd,td->hst', q_rot.astype(jnp.float32), k_rot.astype(jnp.float32))
    positions = jnp.arange(SEQ_LEN)
    causal = positions[:, None] >= positions[None, :]
    scores = jnp.where(causal[None, :, :], scores * ATTN_SCALE, -1e30)
    attn_probs = jax.nn.softmax(scores, axis=-1).astype(jnp.bfloat16)
    attn_mix = jnp.einsum('hst,thd->shd', attn_probs.astype(jnp.float32), kv_seq[:, :, NOPE_DIM:].astype(jnp.float32))
    return attn_mix.astype(jnp.bfloat16).reshape(SEQ_LEN, N_HEADS * VALUE_DIM)


def block_forward(rows_f32, gain_vec, w_query_f, w_down_f, kv_gain_vec, w_up_f, w_out_f):
    normed = rms_scale(rows_f32, gain_vec)
    q_proj = jnp.dot(normed.astype(jnp.float32), w_query_f, preferred_element_type=jnp.float32).astype(jnp.bfloat16)
    kv_down = jnp.dot(normed.astype(jnp.float32), w_down_f, preferred_element_type=jnp.float32).astype(jnp.bfloat16)
    latent = rms_scale(kv_down[:, :KV_RANK], kv_gain_vec)
    kv_up = jnp.dot(latent.astype(jnp.float32), w_up_f, preferred_element_type=jnp.float32).astype(jnp.bfloat16)
    seq_parts = (q_proj.reshape(BATCH_SEQS, SEQ_LEN, N_HEADS, NOPE_DIM + ROPE_DIM), kv_down[:, KV_RANK:].reshape(BATCH_SEQS, SEQ_LEN, ROPE_DIM), kv_up.reshape(BATCH_SEQS, SEQ_LEN, N_HEADS, NOPE_DIM + VALUE_DIM))
    attn_mix = lax.map(jax.checkpoint(lambda seq_item: attend_one(*seq_item)), seq_parts)
    attn_out = jnp.dot(attn_mix.reshape(BATCH_SEQS * SEQ_LEN, N_HEADS * VALUE_DIM).astype(jnp.float32), w_out_f, preferred_element_type=jnp.float32)
    return rows_f32 + attn_out


def reference(tok_ids, grad_out, emb_table, norm_gain, w_query, w_kv_down, kv_gain, w_kv_up, w_out):
    flat_ids = tok_ids.reshape(BATCH_SEQS * SEQ_LEN)
    rows_f32 = jnp.take(emb_table, flat_ids, axis=0).astype(jnp.float32)
    weight_list = tuple(weight_arr.astype(jnp.float32) for weight_arr in (norm_gain, w_query, w_kv_down, kv_gain, w_kv_up, w_out))
    out_f32, pullback = jax.vjp(block_forward, rows_f32, *weight_list)
    grad_list = pullback(grad_out.reshape(BATCH_SEQS * SEQ_LEN, D_MODEL).astype(jnp.float32))
    grad_table = jax.ops.segment_sum(grad_list[0], flat_ids, num_segments=VOCAB_SIZE).astype(jnp.bfloat16)
    block_out = out_f32.astype(jnp.bfloat16).reshape(BATCH_SEQS, SEQ_LEN, D_MODEL)
    return (block_out, grad_table, grad_list[1], grad_list[2], grad_list[3], grad_list[4], grad_list[5], grad_list[6])
```

```python
import math
import jax
import jax.numpy as jnp
from jax import lax
from jax.sharding import PartitionSpec as P
from jax.experimental import pallas as pl
from jax.experimental.pallas import tpu as pltpu

NOPE_DIM = 128
ROPE_DIM = 64
VALUE_DIM = 128
ROPE_THETA = 50000.0
RMS_EPS = 1e-6
ATTN_SCALE = (NOPE_DIM + ROPE_DIM) ** -0.5 * (0.1 * math.log(32.0) + 1.0) ** 2
ROW_DIMS = (((0,), (0,)), ((), ()))
COL_DIMS = (((1,), (1,)), ((), ()))


def rms_scale(in_vals, gain_vec):
    vals_f32 = in_vals.astype(jnp.float32)
    inv_rms = lax.rsqrt(jnp.mean(vals_f32 * vals_f32, axis=-1, keepdims=True) + RMS_EPS)
    return (vals_f32 * inv_rms * gain_vec).astype(jnp.bfloat16)


def rope_tables(seq_len):
    positions = jnp.arange(seq_len, dtype=jnp.float32)
    inv_freq = ROPE_THETA ** (-2.0 * jnp.arange(ROPE_DIM // 2, dtype=jnp.float32) / ROPE_DIM)
    rot_angle = positions[:, None] * inv_freq[None, :]
    rot_angle = jnp.concatenate([rot_angle, rot_angle], axis=-1)
    return jnp.cos(rot_angle), jnp.sin(rot_angle)


def apply_rope(in_vals, cos_tab, sin_tab):
    half_dim = ROPE_DIM // 2
    vals_f32 = in_vals.astype(jnp.float32)
    turned = jnp.concatenate([-vals_f32[..., half_dim:], vals_f32[..., :half_dim]], axis=-1)
    return (vals_f32 * cos_tab + turned * sin_tab).astype(jnp.bfloat16)


def attend_local(q_proj, pe_raw, kv_up):
    seq_len = q_proj.shape[1]
    cos_tab, sin_tab = rope_tables(seq_len)
    q_rot = apply_rope(q_proj[..., NOPE_DIM:], cos_tab[:, None, :], sin_tab[:, None, :])
    k_rot = apply_rope(pe_raw, cos_tab, sin_tab)
    scores = jnp.einsum('bshd,bthd->bhst', q_proj[..., :NOPE_DIM], kv_up[..., :NOPE_DIM], preferred_element_type=jnp.float32)
    scores = scores + jnp.einsum('bshd,btd->bhst', q_rot, k_rot, preferred_element_type=jnp.float32)
    positions = jnp.arange(seq_len)
    causal = positions[:, None] >= positions[None, :]
    scores = jnp.where(causal, scores * ATTN_SCALE, -1e30)
    attn_probs = jax.nn.softmax(scores, axis=-1).astype(jnp.bfloat16)
    attn_mix = jnp.einsum('bhst,bthd->bshd', attn_probs, kv_up[..., NOPE_DIM:], preferred_element_type=jnp.float32)
    return attn_mix.astype(jnp.bfloat16)


F32, BF16 = jnp.float32, jnp.bfloat16
MESH = pl.DeviceIdType.MESH
ANY = pl.BlockSpec(memory_space=pl.ANY)
RING = 8
GROUP = 16

def chip_at(pos):
    side = pos // 4
    return (pos + side * (7 - 2 * pos)) * 2 + side

def place():
    me = lax.axis_index('fsdp')
    core = me % 2
    chip = me // 2
    side = chip % 2
    zz = chip // 2
    return me, core, zz + side * (7 - 2 * zz)

def at_pos(pos, core):
    return chip_at(pos % RING) * 2 + core

def meet_all(me):
    barrier = pltpu.get_barrier_semaphore()
    for step in range(1, GROUP):
        pl.semaphore_signal(barrier, inc=1, device_id={'fsdp': (me + step) % GROUP}, device_id_type=MESH)
    pl.semaphore_wait(barrier, GROUP - 1)

TOK = 288
D_OUT, D_CAT, D_UP, D_DOWN = 2048, 3712, 4096, 640
CUT = 1792
PARTS = (('o', 0, 0, 1024), ('o', 1, 1024, 1024), ('n', 0, 0, CUT), ('n', 1, CUT, D_CAT - CUT), ('u', 0, 0, 2048), ('u', 1, 2048, 2048))
ROWS = {'o': 128, 'n': 128, 'u': 32}

def col_tiles(width):
    step = 512
    return [(c, min(step, width - c)) for c in range(0, width, step)]

def grad_kernel(mix_h, dy_h, nrm_h, dd_h, dq_h, lat_h, du_h, sm_h, go_h, gn_h, gu_h, gs_h,
                mix, dy, nrm, cat, lat, du, b0, b1, b2, b3, b4, b5, smr, ssum, loc_sem, xs_sem, xr_sem, s_sem, r_sem, ms_sem, mr_sem, out_sem):
    me, core, pos = place()
    partner = me + 1 - 2 * core
    meet_all(me)
    acts = ((mix_h, mix), (dy_h, dy), (nrm_h, nrm), (dd_h, cat.at[:, :, 0:D_DOWN]), (dq_h, cat.at[:, :, D_DOWN:D_CAT]), (lat_h, lat), (du_h, du))
    local, cross = [], []
    for i, (src, dst) in enumerate(acts):
        cp = pltpu.make_async_copy(src, dst.at[core], loc_sem.at[i]); cp.start(); local.append(cp)
        rc = pltpu.make_async_remote_copy(src, dst.at[core], xs_sem.at[i], xr_sem.at[i], device_id={'fsdp': partner}, device_id_type=MESH)
        rc.start(); cross.append(rc)
    own_small = pltpu.make_async_copy(sm_h.at[me], smr.at[0], loc_sem.at[7]); own_small.start()
    smalls = []
    for i in range(1, GROUP):
        peer = (me + i) % GROUP
        rc = pltpu.make_async_remote_copy(sm_h.at[peer], smr.at[i], ms_sem.at[i], mr_sem.at[i], device_id={'fsdp': peer}, device_id_type=MESH)
        rc.start(); smalls.append(rc)
    bufs = (b0, b1, b2, b3, b4, b5)
    peers = (at_pos(pos + 1, core), at_pos(pos + 7, core))
    left_ops = {'o': (mix, dy), 'n': (nrm, cat), 'u': (lat, du)}

    def hop(p, step):
        return pltpu.make_async_remote_copy(bufs[p].at[step], bufs[p].at[step + 1], s_sem.at[p, step], r_sem.at[p, step + 1],
                                            device_id={'fsdp': peers[PARTS[p][1]]}, device_id_type=MESH)

    def work(p, step, first):
        kind, way, c0, width = PARTS[p]
        chip = chip_at((pos + 7 - step + way * (2 * step + 2)) % RING)
        lhs_ref, rhs_ref = left_ops[kind]
        if kind == 'u':
            row = pl.multiple_of(chip * 64 + core * 32, 32)
            lhs = [lhs_ref[b, pl.ds(row, 32), :] for b in range(2)]
            dims = (((1,), (0,)), ((), ()))
        else:
            col = pl.multiple_of(chip * 256 + core * 128, 128)
            lhs = [lhs_ref[b, :, pl.ds(col, 128)] for b in range(2)]
            dims = (((0,), (0,)), ((), ()))
        for c, w in col_tiles(width):
            part = sum(lax.dot_general(lhs[b], rhs_ref[b, :, c0 + c:c0 + c + w], dims, preferred_element_type=F32) for b in range(2))
            if first:
                bufs[p][step, :, c:c + w] = part
            else:
                bufs[p][step, :, c:c + w] = bufs[p][step, :, c:c + w] + part

    need = {'o': (0, 1), 'n': (2, 3, 4), 'u': (5, 6)}
    for p in range(6):
        if PARTS[p][1] == 0:
            for i in need[PARTS[p][0]]:
                local[i].wait(); cross[i].wait_recv()
        work(p, 0, True)
        hop(p, 0).start()

    @pl.loop(1, RING - 1)
    def _(step):
        for p in range(6):
            hop(p, step - 1).wait_recv()
            work(p, step, False)
            hop(p, step).start()

    last = RING - 1
    outs = []
    targets = (go_h.at[:, 0:1024], go_h.at[:, 1024:2048], gn_h.at[:, 0:CUT], gn_h.at[:, CUT:D_CAT], gu_h.at[:, 0:2048], gu_h.at[:, 2048:4096])
    for p in range(6):
        hop(p, last - 1).wait_recv()
        work(p, last, False)
        cp = pltpu.make_async_copy(bufs[p].at[last], targets[p], out_sem.at[p]); cp.start(); outs.append(cp)
    own_small.wait()
    for rc in smalls:
        rc.wait()
    ssum[...] = jnp.sum(smr[...], axis=0)
    cp = pltpu.make_async_copy(ssum, gs_h, out_sem.at[6]); cp.start(); outs.append(cp)
    for rc in cross:
        rc.wait_send()
    for p in range(6):
        @pl.loop(0, last)
        def _(step):
            hop(p, step).wait_send()
    for cp in outs:
        cp.wait()

def grad_shards(mix, dy, nrm, dd, dq, lat_t, du, small):
    shapes = [(ROWS[k], RING, w) for k, _, _, w in PARTS]
    scratch = [pltpu.VMEM((2, TOK, 2048), BF16), pltpu.VMEM((2, TOK, 2048), BF16), pltpu.VMEM((2, TOK, 2048), BF16),
               pltpu.VMEM((2, TOK, D_CAT), BF16), pltpu.VMEM((2, 512, TOK), BF16), pltpu.VMEM((2, TOK, D_UP), BF16)]
    scratch += [pltpu.VMEM((RING, r, w), F32) for r, _, w in shapes]
    scratch += [pltpu.VMEM((GROUP, 8, 128), F32), pltpu.VMEM((8, 128), F32)]
    dma = pltpu.SemaphoreType.DMA
    scratch += [dma((8,)), dma((7,)), dma((7,)), dma((6, RING)), dma((6, RING)), dma((GROUP,)), dma((GROUP,)), dma((7,))]
    return pl.pallas_call(
        grad_kernel,
        out_shape=(jax.ShapeDtypeStruct((128, 2048), F32), jax.ShapeDtypeStruct((128, D_CAT), F32), jax.ShapeDtypeStruct((32, D_UP), F32), jax.ShapeDtypeStruct((8, 128), F32)),
        in_specs=[ANY] * 8, out_specs=(ANY,) * 4, scratch_shapes=scratch,
        compiler_params=pltpu.CompilerParams(collective_id=1, has_side_effects=True, vmem_limit_bytes=60 * 1024 * 1024),
        cost_estimate=pl.CostEstimate(flops=8 * 10**9, bytes_accessed=20 * 10**6, transcendentals=0), name='grad_shards',
    )(mix, dy, nrm, dd, dq, lat_t, du, small)


W_SHARDS = ((128, 3072), (128, 576), (32, 4096), (128, 2048))
HALF_TOK = TOK // 2


def spread_kernel(n_w, *refs):
    rows_h = refs[0]
    srcs = refs[1:1 + n_w]
    got_h = refs[1 + n_w]
    outs = refs[2 + n_w:2 + 2 * n_w]
    stage = refs[2 + 2 * n_w:2 + 3 * n_w]
    own, mate, way0, way1 = refs[2 + 3 * n_w:6 + 3 * n_w]
    in_sem, own_sem, s_sem, r_sem, ps_sem, pr_sem, h_in, m_s, m_r, hs_sem, hr_sem, out_sem = refs[6 + 3 * n_w:]
    me, core, pos = place()
    partner = me + 1 - 2 * core
    barrier = pltpu.get_barrier_semaphore()
    peers = (at_pos(pos + 1, core), at_pos(pos + 7, core))
    for peer in peers + (partner,):
        pl.semaphore_signal(barrier, inc=1, device_id={'fsdp': peer}, device_id_type=MESH)
    pl.semaphore_wait(barrier, 3)
    loads = []
    for i in range(n_w):
        cp = pltpu.make_async_copy(srcs[i], stage[i], in_sem.at[i])
        cp.start()
        loads.append(cp)

    def row_load(q):
        return pltpu.make_async_copy(rows_h.at[at_pos(q, core)], own.at[q], h_in.at[q])

    def row_share(q):
        return pltpu.make_async_remote_copy(rows_h.at[at_pos(q, 1 - core)], mate.at[q], m_s.at[q], m_r.at[q],
                                            device_id={'fsdp': partner}, device_id_type=MESH)
    for j in (7, 1, 6, 2, 5, 3, 4, 0):
        row_share((pos + j) % RING).start()
        row_load((pos + j) % RING).start()

    def where(i, way, source):
        rows = W_SHARDS[i][0]
        half = rows // 2
        return outs[i].at[pl.ds(pl.multiple_of(source * rows + way * half, half), half), :]

    def origin(way, step):
        return at_pos(pos + 8 - step + way * 2 * step, core)

    def hop(i, way, step, src=None):
        spot = where(i, way, origin(way, step))
        return pltpu.make_async_remote_copy(spot if src is None else src, spot, s_sem.at[i, way, step], r_sem.at[i, way, step + 1],
                                            device_id={'fsdp': peers[way]}, device_id_type=MESH)

    def arrive(i, way, step):
        spot = where(i, way, origin(way, step))
        return pltpu.make_async_remote_copy(spot, spot, s_sem.at[i, way, step], r_sem.at[i, way, step],
                                            device_id={'fsdp': peers[way]}, device_id_type=MESH)

    def share(i, way, step, src=None):
        spot = where(i, way, origin(way, step))
        return pltpu.make_async_remote_copy(spot if src is None else src, spot, ps_sem.at[i, way, step], pr_sem.at[i, way, step],
                                            device_id={'fsdp': partner}, device_id_type=MESH)
    ways = (way0, way1)

    def row_hop(way, step):
        return pltpu.make_async_remote_copy(ways[way].at[step], ways[way].at[step + 1], hs_sem.at[way, step], hr_sem.at[way, step + 1],
                                            device_id={'fsdp': peers[way]}, device_id_type=MESH)

    def fill(way, step, first):
        q = (pos + 7 - step + way * (2 * step + 2)) % RING
        for c in range(0, HALF_TOK, 48):
            lo = way * HALF_TOK + c
            part = own[q, lo:lo + 48, :] + mate[q, lo:lo + 48, :]
            if not first:
                part = part + ways[way][step, c:c + 48, :]
            ways[way][step, c:c + 48, :] = part

    kept = []
    for i in range(n_w):
        loads[i].wait()
        half = W_SHARDS[i][0] // 2
        for way in range(2):
            src = stage[i].at[way * half:(way + 1) * half, :]
            hop(i, way, 0, src).start()
            share(i, way, 0, src).start()
            cp = pltpu.make_async_copy(src, where(i, way, me), own_sem.at[i, way])
            cp.start()
            kept.append(cp)
    for j in (7, 1, 6, 2, 5, 3, 4, 0):
        row_load((pos + j) % RING).wait()
        row_share((pos + j) % RING).wait_recv()
        if j in (7, 1):
            way = 0 if j == 7 else 1
            fill(way, 0, True)
            row_hop(way, 0).start()

    @pl.loop(1, RING)
    def _(step):
        for i in range(n_w):
            for way in range(2):
                arrive(i, way, step).wait_recv()

                @pl.when(step < RING - 1)
                def _():
                    hop(i, way, step).start()
                share(i, way, step).start()
        for way in range(2):
            row_hop(way, step - 1).wait_recv()
            fill(way, step, False)

            @pl.when(step < RING - 1)
            def _():
                row_hop(way, step).start()

    for way in range(2):
        cp = pltpu.make_async_copy(ways[way].at[RING - 1], got_h.at[way * HALF_TOK:(way + 1) * HALF_TOK, :], out_sem.at[way])
        cp.start()
        kept.append(cp)
    for cp in kept:
        cp.wait()

    @pl.loop(0, RING)
    def _(step):
        row_share(step).wait_send()

        @pl.when(step < RING - 1)
        def _():
            for way in range(2):
                row_hop(way, step).wait_send()
        for i in range(n_w):
            for way in range(2):
                @pl.when(step < RING - 1)
                def _():
                    hop(i, way, step).wait_send()
                share(i, way, step).wait()


def spread(rows, shards):
    dma = pltpu.SemaphoreType.DMA
    n_w = len(shards)
    return pl.pallas_call(
        lambda *refs: spread_kernel(n_w, *refs),
        out_shape=(jax.ShapeDtypeStruct((TOK, 2048), BF16),) + tuple(jax.ShapeDtypeStruct((GROUP * r, w), BF16) for r, w in W_SHARDS[:n_w]),
        in_specs=[ANY] * (n_w + 1), out_specs=(ANY,) * (n_w + 1),
        scratch_shapes=[pltpu.VMEM(s, BF16) for s in W_SHARDS[:n_w]] + [pltpu.VMEM((RING, TOK, 2048), BF16)] * 2 + [pltpu.VMEM((RING, HALF_TOK, 2048), BF16)] * 2
        + [dma((n_w,)), dma((n_w, 2))] + [dma((n_w, 2, RING)) for _ in range(4)] + [dma((RING,)) for _ in range(3)] + [dma((2, RING)) for _ in range(2)] + [dma((2,))],
        compiler_params=pltpu.CompilerParams(collective_id=2, has_side_effects=True, vmem_limit_bytes=60 * 1024 * 1024),
        cost_estimate=pl.CostEstimate(flops=8 * 10**9, bytes_accessed=27 * 10**6, transcendentals=0), name='spread',
    )(rows, *shards)


def small_kernel(src, out, loc_sem, s_sem, r_sem):
    me = lax.axis_index('fsdp')
    meet_all(me)
    own = pltpu.make_async_copy(src, out.at[me], loc_sem)
    own.start()

    def send(step):
        return pltpu.make_async_remote_copy(src, out.at[me], s_sem.at[step], r_sem.at[step],
                                            device_id={'fsdp': (me + step) % GROUP}, device_id_type=MESH)
    for step in range(1, GROUP):
        send(step).start()
    for step in range(1, GROUP):
        send(step).wait()
    own.wait()


def small_gather(tile):
    dma = pltpu.SemaphoreType.DMA
    return pl.pallas_call(
        small_kernel, out_shape=jax.ShapeDtypeStruct((GROUP, 8, 128), F32),
        in_specs=[pl.BlockSpec(memory_space=pltpu.VMEM)], out_specs=pl.BlockSpec(memory_space=pltpu.VMEM),
        scratch_shapes=[dma, dma((GROUP,)), dma((GROUP,))],
        compiler_params=pltpu.CompilerParams(collective_id=0, has_side_effects=True),
        cost_estimate=pl.CostEstimate(flops=10**7, bytes_accessed=10**5, transcendentals=0), name='small_gather',
    )(tile)


def blank(shape, dtype):
    return pl.pallas_call(lambda out: None, out_shape=jax.ShapeDtypeStruct(shape, dtype), out_specs=ANY, name='blank')()


def block_step(rows_f32, grad_rows, full_weights, seq_count):
    gain_vec, w_query, w_kv_down, kv_gain, w_kv_up, w_out = full_weights
    kv_rank = kv_gain.shape[0]
    tok_count = rows_f32.shape[0]
    seq_len = tok_count // seq_count
    normed, norm_pull = jax.vjp(rms_scale, rows_f32, gain_vec)
    q_proj = jnp.dot(normed, w_query, preferred_element_type=jnp.float32).astype(jnp.bfloat16)
    kv_down = jnp.dot(normed, w_kv_down, preferred_element_type=jnp.float32).astype(jnp.bfloat16)
    latent, latent_pull = jax.vjp(rms_scale, kv_down[:, :kv_rank], kv_gain)
    kv_up = jnp.dot(latent, w_kv_up, preferred_element_type=jnp.float32).astype(jnp.bfloat16)
    attn_mix, attn_pull = jax.vjp(attend_local, q_proj.reshape(seq_count, seq_len, -1, NOPE_DIM + ROPE_DIM), kv_down[:, kv_rank:].reshape(seq_count, seq_len, ROPE_DIM), kv_up.reshape(seq_count, seq_len, -1, NOPE_DIM + VALUE_DIM))
    mix_rows = attn_mix.reshape(tok_count, -1)
    out_f32 = rows_f32 + jnp.dot(mix_rows, w_out, preferred_element_type=jnp.float32)
    d_mix = lax.dot_general(grad_rows, w_out, COL_DIMS, preferred_element_type=jnp.float32).astype(jnp.bfloat16)
    d_query, d_pe, d_up = attn_pull(d_mix.reshape(attn_mix.shape))
    d_query = d_query.reshape(tok_count, -1)
    d_up = d_up.reshape(tok_count, -1)
    d_latent = lax.dot_general(d_up, w_kv_up, COL_DIMS, preferred_element_type=jnp.float32).astype(jnp.bfloat16)
    d_ckv, d_kv_gain = latent_pull(d_latent)
    d_down = jnp.concatenate([d_ckv, d_pe.reshape(tok_count, ROPE_DIM)], axis=1)
    d_normed = lax.dot_general(d_query, w_query, COL_DIMS, preferred_element_type=jnp.float32)
    d_normed = d_normed + lax.dot_general(d_down, w_kv_down, COL_DIMS, preferred_element_type=jnp.float32)
    d_rows, d_gain = norm_pull(d_normed.astype(jnp.bfloat16))
    d_rows = d_rows + grad_rows.astype(jnp.float32)
    return out_f32.astype(jnp.bfloat16), d_rows, normed, mix_rows, latent, d_query, d_down, d_up, d_gain, d_kv_gain


def solution(mesh):
    tok_spec = P(('dp', 'fsdp'), None)
    seq_spec = P(('dp', 'fsdp'), None, None)
    part_vec = P(('dp', 'fsdp'))
    vec_spec = P('fsdp')
    mat_spec = P('fsdp', None)

    def device_step(tok_ids, grad_out, emb_table, norm_gain, w_query, w_kv_down, kv_gain, w_kv_up, w_out):
        seq_count, seq_len = tok_ids.shape
        vocab_dev, d_model = emb_table.shape
        tok_count = seq_count * seq_len
        me = lax.axis_index('fsdp')
        fill = lambda rows: jnp.pad(rows, ((0, 0), (0, 128 - rows.shape[1])))
        tile = jnp.concatenate([fill(tok_ids.astype(F32)), norm_gain.astype(F32).reshape(1, 128), fill(kv_gain.astype(F32).reshape(1, 32)), jnp.zeros((3, 128), F32)], axis=0)
        table = small_gather(tile)
        all_ids = table[:, :seq_count, :seq_len].reshape(GROUP, tok_count).astype(jnp.int32)
        gain_full = table[:, 3, :].reshape(-1)
        kv_gain_full = table[:, 4, :32].reshape(-1)

        owner = all_ids // vocab_dev
        mine = (owner == me)
        picked = jnp.where(mine.reshape(-1, 1), jnp.take(emb_table, jnp.where(mine, all_ids - me * vocab_dev, 0).reshape(-1), axis=0), jnp.zeros((), BF16))
        tok_rows, full_wq, full_kva, full_kvb, full_wo = spread(picked.reshape(GROUP, tok_count, d_model), (w_query, w_kv_down, w_kv_up, w_out))
        grad_rows = grad_out.reshape(tok_count, d_model)
        block_out, d_rows, normed, mix, latent, d_query, d_down, d_up, d_gain, d_kv_gain = block_step(
            tok_rows.astype(F32), grad_rows, (gain_full, full_wq, full_kva, kv_gain_full, full_kvb, full_wo), seq_count)
        small = jnp.concatenate([d_gain.reshape(GROUP, 1, 128), jnp.pad(d_kv_gain.reshape(GROUP, 1, 32), ((0, 0), (0, 0), (0, 96))), jnp.zeros((GROUP, 6, 128), F32)], axis=1)
        g_out, g_cat, g_up, g_small = grad_shards(mix, grad_rows, normed, jnp.pad(d_down, ((0, 0), (0, D_DOWN - d_down.shape[1]))), d_query, latent.T, d_up, small)
        all_grads = lax.all_gather(d_rows, 'fsdp', tiled=True)
        seg = jnp.where(mine, all_ids - me * vocab_dev, vocab_dev).reshape(-1)
        grad_table = jax.ops.segment_sum(all_grads, seg, num_segments=vocab_dev).astype(jnp.bfloat16)
        return (block_out.reshape(seq_count, seq_len, d_model), grad_table, g_small[0], g_cat[:, D_DOWN:], g_cat[:, :576], g_small[1, :32], g_up, g_out)

    return jax.shard_map(device_step, mesh=mesh, in_specs=(tok_spec, seq_spec, mat_spec, vec_spec, mat_spec, mat_spec, vec_spec, mat_spec, mat_spec), out_specs=(seq_spec, tok_spec, part_vec, tok_spec, tok_spec, part_vec, tok_spec, tok_spec), check_vma=False)
```

```python
import math
import jax
import jax.numpy as jnp
from jax import lax
from jax.sharding import PartitionSpec as P
from jax.experimental import pallas as pl
from jax.experimental.pallas import tpu as pltpu

NOPE_DIM = 128
ROPE_DIM = 64
VALUE_DIM = 128
ROPE_THETA = 50000.0
RMS_EPS = 1e-6
ATTN_SCALE = (NOPE_DIM + ROPE_DIM) ** -0.5 * (0.1 * math.log(32.0) + 1.0) ** 2
ROW_DIMS = (((0,), (0,)), ((), ()))
COL_DIMS = (((1,), (1,)), ((), ()))


def rms_scale(in_vals, gain_vec):
    vals_f32 = in_vals.astype(jnp.float32)
    inv_rms = lax.rsqrt(jnp.mean(vals_f32 * vals_f32, axis=-1, keepdims=True) + RMS_EPS)
    return (vals_f32 * inv_rms * gain_vec).astype(jnp.bfloat16)


def rope_tables(seq_len):
    positions = jnp.arange(seq_len, dtype=jnp.float32)
    inv_freq = ROPE_THETA ** (-2.0 * jnp.arange(ROPE_DIM // 2, dtype=jnp.float32) / ROPE_DIM)
    rot_angle = positions[:, None] * inv_freq[None, :]
    rot_angle = jnp.concatenate([rot_angle, rot_angle], axis=-1)
    return jnp.cos(rot_angle), jnp.sin(rot_angle)


def apply_rope(in_vals, cos_tab, sin_tab):
    half_dim = ROPE_DIM // 2
    vals_f32 = in_vals.astype(jnp.float32)
    turned = jnp.concatenate([-vals_f32[..., half_dim:], vals_f32[..., :half_dim]], axis=-1)
    return (vals_f32 * cos_tab + turned * sin_tab).astype(jnp.bfloat16)


def attend_local(q_proj, pe_raw, kv_up):
    seq_len = q_proj.shape[1]
    cos_tab, sin_tab = rope_tables(seq_len)
    q_rot = apply_rope(q_proj[..., NOPE_DIM:], cos_tab[:, None, :], sin_tab[:, None, :])
    k_rot = apply_rope(pe_raw, cos_tab, sin_tab)
    scores = jnp.einsum('bshd,bthd->bhst', q_proj[..., :NOPE_DIM], kv_up[..., :NOPE_DIM], preferred_element_type=jnp.float32)
    scores = scores + jnp.einsum('bshd,btd->bhst', q_rot, k_rot, preferred_element_type=jnp.float32)
    positions = jnp.arange(seq_len)
    causal = positions[:, None] >= positions[None, :]
    scores = jnp.where(causal, scores * ATTN_SCALE, -1e30)
    attn_probs = jax.nn.softmax(scores, axis=-1).astype(jnp.bfloat16)
    attn_mix = jnp.einsum('bhst,bthd->bshd', attn_probs, kv_up[..., NOPE_DIM:], preferred_element_type=jnp.float32)
    return attn_mix.astype(jnp.bfloat16)


F32, BF16 = jnp.float32, jnp.bfloat16
MESH = pl.DeviceIdType.MESH
ANY = pl.BlockSpec(memory_space=pl.ANY)
RING = 8
GROUP = 16

def chip_at(pos):
    side = pos // 4
    return (pos + side * (7 - 2 * pos)) * 2 + side

def place():
    me = lax.axis_index('fsdp')
    core = me % 2
    chip = me // 2
    side = chip % 2
    zz = chip // 2
    return me, core, zz + side * (7 - 2 * zz)

def at_pos(pos, core):
    return chip_at(pos % RING) * 2 + core

def meet_all(me):
    barrier = pltpu.get_barrier_semaphore()
    for step in range(1, GROUP):
        pl.semaphore_signal(barrier, inc=1, device_id={'fsdp': (me + step) % GROUP}, device_id_type=MESH)
    pl.semaphore_wait(barrier, GROUP - 1)

TOK = 288
D_OUT, D_CAT, D_UP, D_DOWN = 2048, 3712, 4096, 640
CUT = 1792
PARTS = (('u', 0, 0, 2048), ('u', 1, 2048, 2048), ('n', 0, 0, CUT), ('n', 1, CUT, D_CAT - CUT))
N_PARTS = len(PARTS)
ROWS = {'n': 128, 'u': 32}

def col_tiles(width):
    step = 512
    return [(c, min(step, width - c)) for c in range(0, width, step)]

def grad_kernel(mix_h, dy_h, nrm_h, dd_h, dq_h, lat_h, du_h, sm_h, go_h, gq_h, gd_h, gu_h, gs_h,
                mix, dy, go, nrm, cat, lat, du, b0, b1, b2, b3, smr, ssum, loc_sem, xs_sem, xr_sem, s_sem, r_sem, ms_sem, mr_sem, cs_sem, cr_sem, dy_sem, out_sem):
    me, core, pos = place()
    partner = me + 1 - 2 * core
    meet_all(me)
    acts = ((lat_h, lat), (du_h, du), (nrm_h, nrm), (dd_h, cat.at[:, :, 0:D_DOWN]), (dq_h, cat.at[:, :, D_DOWN:D_CAT]))
    local, cross = [], []
    for i, (src, dst) in enumerate(acts):
        cp = pltpu.make_async_copy(src, dst.at[core], loc_sem.at[i])
        cp.start()
        local.append(cp)
        rc = pltpu.make_async_remote_copy(src, dst.at[core], xs_sem.at[i], xr_sem.at[i], device_id={'fsdp': partner}, device_id_type=MESH)
        rc.start()
        cross.append(rc)
    own_small = pltpu.make_async_copy(sm_h.at[me], smr.at[0], loc_sem.at[5])
    own_small.start()
    own_mix = pltpu.make_async_copy(mix_h.at[:, pl.ds(pl.multiple_of(me * 128, 128), 128)], mix.at[me], loc_sem.at[6])
    own_mix.start()
    smalls, mixes = [], []
    for i in range(1, GROUP):
        peer = (me + i) % GROUP
        rc = pltpu.make_async_remote_copy(sm_h.at[peer], smr.at[i], ms_sem.at[i], mr_sem.at[i], device_id={'fsdp': peer}, device_id_type=MESH)
        rc.start()
        smalls.append(rc)
    bufs = (b0, b1, b2, b3)
    peers = (at_pos(pos + 1, core), at_pos(pos + 7, core))
    left_ops = {'n': (nrm, cat), 'u': (lat, du)}

    def mix_send(i):
        peer = (me + i) % GROUP
        return pltpu.make_async_remote_copy(mix_h.at[:, pl.ds(pl.multiple_of(peer * 128, 128), 128)], mix.at[me], cs_sem.at[i], cr_sem.at[i],
                                            device_id={'fsdp': peer}, device_id_type=MESH)

    def dy_load(blk):
        return pltpu.make_async_copy(dy_h.at[pl.ds(pl.multiple_of(blk * TOK, TOK), TOK), :], dy.at[blk % 2], dy_sem.at[blk % 2])

    def hop(p, step):
        return pltpu.make_async_remote_copy(bufs[p].at[step], bufs[p].at[step + 1], s_sem.at[p, step], r_sem.at[p, step + 1],
                                            device_id={'fsdp': peers[PARTS[p][1]]}, device_id_type=MESH)

    def work(p, step, first):
        kind, way, c0, width = PARTS[p]
        chip = chip_at((pos + 7 - step + way * (2 * step + 2)) % RING)
        lhs_ref, rhs_ref = left_ops[kind]
        if kind == 'u':
            row = pl.multiple_of(chip * 64 + core * 32, 32)
            lhs = [lhs_ref[b, pl.ds(row, 32), :] for b in range(2)]
            dims = (((1,), (0,)), ((), ()))
        else:
            col = pl.multiple_of(chip * 256 + core * 128, 128)
            lhs = [lhs_ref[b, :, pl.ds(col, 128)] for b in range(2)]
            dims = (((0,), (0,)), ((), ()))
        for c, w in col_tiles(width):
            part = sum(lax.dot_general(lhs[b], rhs_ref[b, :, c0 + c:c0 + c + w], dims, preferred_element_type=F32) for b in range(2))
            if first:
                bufs[p][step, :, c:c + w] = part
            else:
                bufs[p][step, :, c:c + w] = bufs[p][step, :, c:c + w] + part

    need = {'u': (0, 1), 'n': (2, 3, 4)}
    for p in range(N_PARTS):
        if PARTS[p][1] == 0:
            for i in need[PARTS[p][0]]:
                local[i].wait()
                cross[i].wait_recv()
        work(p, 0, True)
        hop(p, 0).start()
    for i in range(1, GROUP):
        mix_send(i).start()
    dy_load(0).start()
    own_mix.wait()
    for i in range(1, GROUP):
        mix_send(i).wait()
    go[...] = jnp.zeros_like(go)

    @pl.loop(1, RING - 1)
    def _(step):
        for p in range(N_PARTS):
            hop(p, step - 1).wait_recv()
            work(p, step, False)
            hop(p, step).start()

        @pl.when(step < 5)
        def _():
            @pl.loop(0, 4)
            def _(j):
                blk = (step - 1) * 4 + j
                dy_load(blk).wait()

                @pl.when(blk < GROUP - 1)
                def _():
                    dy_load(blk + 1).start()
                for c, w in col_tiles(D_OUT):
                    go[:, c:c + w] += lax.dot_general(mix[blk], dy[blk % 2, :, c:c + w], (((0,), (0,)), ((), ())), preferred_element_type=F32)

    last = RING - 1
    outs = []
    cp = pltpu.make_async_copy(go, go_h, out_sem.at[7])
    cp.start()
    outs.append(cp)
    cut_q = CUT - D_DOWN
    targets = ((gu_h.at[:, 0:2048], 0, 2048),), ((gu_h.at[:, 2048:4096], 0, 2048),), ((gd_h, 0, D_DOWN), (gq_h.at[:, 0:cut_q], D_DOWN, CUT)), ((gq_h.at[:, cut_q:3072], 0, D_CAT - CUT),)
    for p in range(N_PARTS):
        hop(p, last - 1).wait_recv()
        work(p, last, False)
        for n, (dst, c0, c1) in enumerate(targets[p]):
            cp = pltpu.make_async_copy(bufs[p].at[last, :, c0:c1], dst, out_sem.at[p + 4 * n])
            cp.start()
            outs.append(cp)
    own_small.wait()
    for rc in smalls:
        rc.wait()
    ssum[...] = jnp.sum(smr[...], axis=0)
    cp = pltpu.make_async_copy(ssum, gs_h, out_sem.at[4])
    cp.start()
    outs.append(cp)
    for rc in cross:
        rc.wait_send()
    for p in range(N_PARTS):
        @pl.loop(0, last)
        def _(step):
            hop(p, step).wait_send()
    for cp in outs:
        cp.wait()


def grad_shards(mix, dy_all, nrm, dd, dq, lat_t, du, small):
    shapes = [(ROWS[k], RING, w) for k, _, _, w in PARTS]
    scratch = [pltpu.VMEM((GROUP, TOK, 128), BF16), pltpu.VMEM((2, TOK, 2048), BF16), pltpu.VMEM((128, 2048), F32), pltpu.VMEM((2, TOK, 2048), BF16),
               pltpu.VMEM((2, TOK, D_CAT), BF16), pltpu.VMEM((2, 512, TOK), BF16), pltpu.VMEM((2, TOK, D_UP), BF16)]
    scratch += [pltpu.VMEM((RING, r, w), F32) for r, _, w in shapes]
    scratch += [pltpu.VMEM((GROUP, 8, 128), F32), pltpu.VMEM((8, 128), F32)]
    dma = pltpu.SemaphoreType.DMA
    scratch += [dma((7,)), dma((5,)), dma((5,)), dma((N_PARTS, RING)), dma((N_PARTS, RING)), dma((GROUP,)), dma((GROUP,)), dma((GROUP,)), dma((GROUP,)), dma((2,)), dma((8,))]
    return pl.pallas_call(
        grad_kernel,
        out_shape=(jax.ShapeDtypeStruct((128, 2048), F32), jax.ShapeDtypeStruct((128, 3072), F32), jax.ShapeDtypeStruct((128, D_DOWN), F32), jax.ShapeDtypeStruct((32, D_UP), F32), jax.ShapeDtypeStruct((8, 128), F32)),
        in_specs=[ANY] * 8, out_specs=(ANY,) * 5, scratch_shapes=scratch,
        compiler_params=pltpu.CompilerParams(collective_id=1, has_side_effects=True, vmem_limit_bytes=60 * 1024 * 1024),
        cost_estimate=pl.CostEstimate(flops=8 * 10**9, bytes_accessed=20 * 10**6, transcendentals=0), name='grad_shards',
    )(mix, dy_all, nrm, dd, dq, lat_t, du, small)


W_SHARDS = ((32, 4096),)
HALF_TOK = TOK // 2


def spread_kernel(n_w, *refs):
    mask, rows_h = refs[0:2]
    srcs = refs[2:2 + n_w]
    got_h = refs[2 + n_w]
    outs = refs[3 + n_w:3 + 2 * n_w]
    stage = refs[3 + 2 * n_w:3 + 3 * n_w]
    own, mate, way0, way1 = refs[3 + 3 * n_w:7 + 3 * n_w]
    in_sem, own_sem, s_sem, r_sem, ps_sem, pr_sem, h_in, m_s, m_r, hs_sem, hr_sem, out_sem = refs[7 + 3 * n_w:]
    me, core, pos = place()
    partner = me + 1 - 2 * core
    barrier = pltpu.get_barrier_semaphore()
    peers = (at_pos(pos + 1, core), at_pos(pos + 7, core))
    for peer in peers + (partner,):
        pl.semaphore_signal(barrier, inc=1, device_id={'fsdp': peer}, device_id_type=MESH)
    pl.semaphore_wait(barrier, 3)
    loads = []
    for i in range(n_w):
        cp = pltpu.make_async_copy(srcs[i], stage[i], in_sem.at[i])
        cp.start()
        loads.append(cp)

    def row_load(q):
        return pltpu.make_async_copy(rows_h.at[at_pos(q, core)], own.at[q], h_in.at[q])

    def row_share(q):
        return pltpu.make_async_remote_copy(rows_h.at[at_pos(q, 1 - core)], mate.at[q], m_s.at[q], m_r.at[q],
                                            device_id={'fsdp': partner}, device_id_type=MESH)
    for j in (7, 1, 6, 2, 5, 3, 4, 0):
        row_share((pos + j) % RING).start()
        row_load((pos + j) % RING).start()

    def where(i, way, source):
        rows = W_SHARDS[i][0]
        half = rows // 2
        return outs[i].at[pl.ds(pl.multiple_of(source * rows + way * half, half), half), :]

    def origin(way, step):
        return at_pos(pos + 8 - step + way * 2 * step, core)

    def hop(i, way, step, src=None):
        spot = where(i, way, origin(way, step))
        return pltpu.make_async_remote_copy(spot if src is None else src, spot, s_sem.at[i, way, step], r_sem.at[i, way, step + 1],
                                            device_id={'fsdp': peers[way]}, device_id_type=MESH)

    def arrive(i, way, step):
        spot = where(i, way, origin(way, step))
        return pltpu.make_async_remote_copy(spot, spot, s_sem.at[i, way, step], r_sem.at[i, way, step],
                                            device_id={'fsdp': peers[way]}, device_id_type=MESH)

    def share(i, way, step, src=None):
        spot = where(i, way, origin(way, step))
        return pltpu.make_async_remote_copy(spot if src is None else src, spot, ps_sem.at[i, way, step], pr_sem.at[i, way, step],
                                            device_id={'fsdp': partner}, device_id_type=MESH)
    ways = (way0, way1)

    def row_hop(way, step):
        return pltpu.make_async_remote_copy(ways[way].at[step], ways[way].at[step + 1], hs_sem.at[way, step], hr_sem.at[way, step + 1],
                                            device_id={'fsdp': peers[way]}, device_id_type=MESH)

    def fill(way, step, first):
        q = (pos + 7 - step + way * (2 * step + 2)) % RING
        chip = chip_at(q)
        for c in range(0, HALF_TOK, 48):
            lo = way * HALF_TOK + c
            mine, theirs = mask[0, chip, lo:lo + 48, :], mask[1, chip, lo:lo + 48, :]
            for w in range(0, 2048, 128):
                part = own[q, lo:lo + 48, w:w + 128] * mine + mate[q, lo:lo + 48, w:w + 128] * theirs
                if not first:
                    part = part + ways[way][step, c:c + 48, w:w + 128]
                ways[way][step, c:c + 48, w:w + 128] = part

    kept = []
    for i in range(n_w):
        loads[i].wait()
        half = W_SHARDS[i][0] // 2
        for way in range(2):
            src = stage[i].at[way * half:(way + 1) * half, :]
            hop(i, way, 0, src).start()
            share(i, way, 0, src).start()
            cp = pltpu.make_async_copy(src, where(i, way, me), own_sem.at[i, way])
            cp.start()
            kept.append(cp)
    for j in (7, 1, 6, 2, 5, 3, 4, 0):
        row_load((pos + j) % RING).wait()
        row_share((pos + j) % RING).wait_recv()
        if j in (7, 1):
            way = 0 if j == 7 else 1
            fill(way, 0, True)
            row_hop(way, 0).start()

    @pl.loop(1, RING)
    def _(step):
        for i in range(n_w):
            for way in range(2):
                arrive(i, way, step).wait_recv()

                @pl.when(step < RING - 1)
                def _():
                    hop(i, way, step).start()
                share(i, way, step).start()
        for way in range(2):
            row_hop(way, step - 1).wait_recv()
            fill(way, step, False)

            @pl.when(step < RING - 1)
            def _():
                row_hop(way, step).start()

    for way in range(2):
        cp = pltpu.make_async_copy(ways[way].at[RING - 1], got_h.at[way * HALF_TOK:(way + 1) * HALF_TOK, :], out_sem.at[way])
        cp.start()
        kept.append(cp)
    for cp in kept:
        cp.wait()

    @pl.loop(0, RING)
    def _(step):
        row_share(step).wait_send()

        @pl.when(step < RING - 1)
        def _():
            for way in range(2):
                row_hop(way, step).wait_send()
        for i in range(n_w):
            for way in range(2):
                @pl.when(step < RING - 1)
                def _():
                    hop(i, way, step).wait_send()
                share(i, way, step).wait()


def spread(mask, rows, shards):
    dma = pltpu.SemaphoreType.DMA
    n_w = len(shards)
    return pl.pallas_call(
        lambda *refs: spread_kernel(n_w, *refs),
        out_shape=(jax.ShapeDtypeStruct((TOK, 2048), BF16),) + tuple(jax.ShapeDtypeStruct((GROUP * r, w), BF16) for r, w in W_SHARDS),
        in_specs=[pl.BlockSpec(memory_space=pltpu.VMEM)] + [ANY] * (n_w + 1), out_specs=(ANY,) * (n_w + 1),
        scratch_shapes=[pltpu.VMEM(s, BF16) for s in W_SHARDS] + [pltpu.VMEM((RING, TOK, 2048), BF16)] * 2 + [pltpu.VMEM((RING, HALF_TOK, 2048), BF16)] * 2
        + [dma((max(n_w, 1),)), dma((max(n_w, 1), 2))] + [dma((max(n_w, 1), 2, RING)) for _ in range(4)] + [dma((RING,)) for _ in range(3)] + [dma((2, RING)) for _ in range(2)] + [dma((2,))],
        compiler_params=pltpu.CompilerParams(collective_id=2, has_side_effects=True, vmem_limit_bytes=60 * 1024 * 1024),
        cost_estimate=pl.CostEstimate(flops=8 * 10**9, bytes_accessed=27 * 10**6, transcendentals=0), name='spread',
    )(mask, rows, *shards)
ROW_BLK = 128
IN_BLK = 144
SUB = 48
PIECE = 16
IN_SLOTS = 4
OUT_SLOTS = 4


def table_kernel(starts, toks, rows, flags, gain, dy_h, dn_h, h_h, out_h, grad, dy, dn, hh, acc, ob, nil, in_sem, out_sem):
    n_in = GROUP * TOK // IN_BLK
    n_out = out_h.shape[0] // ROW_BLK

    def loads(blk):
        span = pl.ds(pl.multiple_of(blk * IN_BLK, IN_BLK), IN_BLK)
        slot = blk % IN_SLOTS
        return [pltpu.make_async_copy(src.at[span, :], dst.at[slot], in_sem.at[i, slot]) for i, (src, dst) in enumerate(((dy_h, dy), (dn_h, dn), (h_h, hh)))]
    for blk in range(IN_SLOTS - 1):
        for cp in loads(blk):
            cp.start()

    @pl.loop(0, n_in)
    def _(blk):
        slot = blk % IN_SLOTS
        for cp in loads(blk):
            cp.wait()

        @pl.when(blk < n_in - IN_SLOTS + 1)
        def _():
            for cp in loads(blk + IN_SLOTS - 1):
                cp.start()

        @pl.loop(0, IN_BLK // SUB)
        def _(g):
            @pl.when(flags[blk * (IN_BLK // SUB) + g] > 0)
            def _():
                r0 = pl.multiple_of(g * SUB, PIECE)
                o0 = pl.multiple_of(blk * IN_BLK + g * SUB, PIECE)
                pieces = range(0, SUB, PIECE)

                def tile(ref, p, c):
                    return ref[slot, pl.ds(r0 + p, PIECE), c:c + 128].astype(F32)
                scale = []
                for p in pieces:
                    sq = jnp.zeros((PIECE, 128), F32)
                    al = jnp.zeros((PIECE, 128), F32)
                    for c in range(0, 2048, 128):
                        h = tile(hh, p, c)
                        sq = sq + h * h
                        al = al + h * (tile(dn, p, c) * gain[:, c:c + 128])
                    scale.append((jnp.sum(sq, axis=1, keepdims=True), jnp.sum(al, axis=1, keepdims=True)))
                for p, (sq, al) in zip(pieces, scale):
                    inv = lax.rsqrt(sq * (1.0 / 2048) + RMS_EPS)
                    coef = inv * inv * inv * (al * (1.0 / 2048))
                    for c in range(0, 2048, 128):
                        s = tile(dn, p, c) * gain[:, c:c + 128]
                        grad[pl.ds(o0 + p, PIECE), c:c + 128] = tile(dy, p, c) + inv * s - coef * tile(hh, p, c)

    def store(blk, src):
        return pltpu.make_async_copy(src, out_h.at[pl.ds(pl.multiple_of(blk * ROW_BLK, ROW_BLK), ROW_BLK), :], out_sem.at[blk % OUT_SLOTS])
    nil[...] = jnp.zeros_like(nil)

    @pl.loop(0, n_out)
    def _(blk):
        first, last = starts[blk], starts[blk + 1]
        slot = blk % OUT_SLOTS

        @pl.when(blk >= OUT_SLOTS)
        def _():
            store(blk - OUT_SLOTS, nil).wait()

        @pl.when(first == last)
        def _():
            store(blk, nil).start()

        @pl.when(first < last)
        def _():
            acc[...] = jnp.zeros_like(acc)

            @pl.loop(first, last)
            def _(k):
                r = rows[k]
                acc[pl.ds(r, 1), :] += grad[pl.ds(toks[k], 1), :]
            ob[slot] = acc[...].astype(BF16)
            store(blk, ob.at[slot]).start()
    for blk in range(n_out - OUT_SLOTS, n_out):
        store(blk, nil).wait()


def table_grad(starts, toks, rows, flags, gain, dy_all, dn_all, picked, vocab_dev):
    smem = pl.BlockSpec(memory_space=pltpu.SMEM)
    dma = pltpu.SemaphoreType.DMA
    return pl.pallas_call(
        table_kernel, out_shape=jax.ShapeDtypeStruct((vocab_dev, 2048), BF16),
        in_specs=[smem] * 4 + [pl.BlockSpec(memory_space=pltpu.VMEM)] + [ANY] * 3, out_specs=ANY,
        scratch_shapes=[pltpu.VMEM((GROUP * TOK, 2048), F32)] + [pltpu.VMEM((IN_SLOTS, IN_BLK, 2048), BF16)] * 3 + [pltpu.VMEM((ROW_BLK, 2048), F32), pltpu.VMEM((OUT_SLOTS, ROW_BLK, 2048), BF16), pltpu.VMEM((ROW_BLK, 2048), BF16), dma((3, IN_SLOTS)), dma((OUT_SLOTS,))],
        compiler_params=pltpu.CompilerParams(vmem_limit_bytes=60 * 1024 * 1024),
        cost_estimate=pl.CostEstimate(flops=10**9, bytes_accessed=80 * 10**6, transcendentals=0), name='table_grad',
    )(starts, toks, rows, flags, gain, dy_all, dn_all, picked)


def small_kernel(src, out, loc_sem, s_sem, r_sem):
    me = lax.axis_index('fsdp')
    meet_all(me)
    own = pltpu.make_async_copy(src, out.at[me], loc_sem)
    own.start()

    def send(step):
        return pltpu.make_async_remote_copy(src, out.at[me], s_sem.at[step], r_sem.at[step],
                                            device_id={'fsdp': (me + step) % GROUP}, device_id_type=MESH)
    for step in range(1, GROUP):
        send(step).start()
    for step in range(1, GROUP):
        send(step).wait()
    own.wait()


def small_gather(tile):
    dma = pltpu.SemaphoreType.DMA
    return pl.pallas_call(
        small_kernel, out_shape=jax.ShapeDtypeStruct((GROUP, 8, 128), F32),
        in_specs=[pl.BlockSpec(memory_space=pltpu.VMEM)], out_specs=pl.BlockSpec(memory_space=pltpu.VMEM),
        scratch_shapes=[dma, dma((GROUP,)), dma((GROUP,))],
        compiler_params=pltpu.CompilerParams(collective_id=0, has_side_effects=True),
        cost_estimate=pl.CostEstimate(flops=10**7, bytes_accessed=10**5, transcendentals=0), name='small_gather',
    )(tile)


def blank(shape, dtype):
    return pl.pallas_call(lambda out: None, out_shape=jax.ShapeDtypeStruct(shape, dtype), out_specs=ANY, name='blank')()


def block_step(rows_f32, grad_rows, full_weights, seq_count):
    gain_vec, w_query, w_kv_down, kv_gain, w_kv_up, w_out = full_weights
    kv_rank = kv_gain.shape[0]
    tok_count = rows_f32.shape[0]
    seq_len = tok_count // seq_count
    normed, norm_pull = jax.vjp(rms_scale, rows_f32, gain_vec)
    q_proj = jnp.dot(normed, w_query, preferred_element_type=jnp.float32).astype(jnp.bfloat16)
    kv_down = jnp.dot(normed, w_kv_down, preferred_element_type=jnp.float32).astype(jnp.bfloat16)
    latent, latent_pull = jax.vjp(rms_scale, kv_down[:, :kv_rank], kv_gain)
    kv_up = jnp.dot(latent, w_kv_up, preferred_element_type=jnp.float32).astype(jnp.bfloat16)
    attn_mix, attn_pull = jax.vjp(attend_local, q_proj.reshape(seq_count, seq_len, -1, NOPE_DIM + ROPE_DIM), kv_down[:, kv_rank:].reshape(seq_count, seq_len, ROPE_DIM), kv_up.reshape(seq_count, seq_len, -1, NOPE_DIM + VALUE_DIM))
    mix_rows = attn_mix.reshape(tok_count, -1)
    out_f32 = rows_f32 + jnp.dot(mix_rows, w_out, preferred_element_type=jnp.float32)
    d_mix = lax.dot_general(grad_rows, w_out, COL_DIMS, preferred_element_type=jnp.float32).astype(jnp.bfloat16)
    d_query, d_pe, d_up = attn_pull(d_mix.reshape(attn_mix.shape))
    d_query = d_query.reshape(tok_count, -1)
    d_up = d_up.reshape(tok_count, -1)
    d_latent = lax.dot_general(d_up, w_kv_up, COL_DIMS, preferred_element_type=jnp.float32).astype(jnp.bfloat16)
    d_ckv, d_kv_gain = latent_pull(d_latent)
    d_down = jnp.concatenate([d_ckv, d_pe.reshape(tok_count, ROPE_DIM)], axis=1)
    d_normed = lax.dot_general(d_query, w_query, COL_DIMS, preferred_element_type=jnp.float32)
    d_normed = d_normed + lax.dot_general(d_down, w_kv_down, COL_DIMS, preferred_element_type=jnp.float32)
    d_normed = d_normed.astype(jnp.bfloat16)
    _, d_gain = norm_pull(d_normed)
    return out_f32.astype(jnp.bfloat16), d_normed, normed, mix_rows, latent, d_query, d_down, d_up, d_gain, d_kv_gain


def solution(mesh):
    tok_spec = P(('dp', 'fsdp'), None)
    seq_spec = P(('dp', 'fsdp'), None, None)
    part_vec = P(('dp', 'fsdp'))
    vec_spec = P('fsdp')
    mat_spec = P('fsdp', None)

    def device_step(tok_ids, grad_out, emb_table, norm_gain, w_query, w_kv_down, kv_gain, w_kv_up, w_out):
        seq_count, seq_len = tok_ids.shape
        vocab_dev, d_model = emb_table.shape
        tok_count = seq_count * seq_len
        me = lax.axis_index('fsdp')
        grad_rows = grad_out.reshape(tok_count, d_model)
        bundle = lax.all_gather(jnp.concatenate([w_query, w_out, w_kv_down], axis=1), 'fsdp', tiled=True)
        fill = lambda rows: jnp.pad(rows, ((0, 0), (0, 128 - rows.shape[1])))
        tile = jnp.concatenate([fill(tok_ids.astype(F32)), norm_gain.astype(F32).reshape(1, 128), fill(kv_gain.astype(F32).reshape(1, 32)), jnp.zeros((3, 128), F32)], axis=0)
        table = small_gather(tile)
        all_ids = table[:, :seq_count, :seq_len].reshape(GROUP, tok_count).astype(jnp.int32)
        gain_full = table[:, 3, :].reshape(-1)
        kv_gain_full = table[:, 4, :32].reshape(-1)

        owner = all_ids // vocab_dev
        mine = (owner == me)
        local = all_ids - me * vocab_dev
        keys = lax.sort(jnp.where(mine, local * 8192 + jnp.arange(GROUP * tok_count).reshape(GROUP, tok_count), 2**30).reshape(-1))
        starts = jnp.sum((mine & (local < ROW_BLK * jnp.arange(vocab_dev // ROW_BLK + 1)[:, None, None])).astype(jnp.int32), axis=(1, 2))
        flags = jnp.sum(mine.reshape(-1, SUB).astype(jnp.int32), axis=1)
        picked = jnp.take(emb_table, jnp.where(mine, local, 0).reshape(-1), axis=0, mode='clip')
        core = me % 2
        near = lax.dynamic_index_in_dim(owner.reshape(RING, 2, tok_count), core, 1, keepdims=False)
        mask = jnp.stack([near == me, near == me + 1 - 2 * core]).astype(BF16)
        mask = jnp.broadcast_to(mask[..., None], (2, RING, tok_count, 128))
        picked, keys, starts, flags = lax.optimization_barrier((picked, keys, starts, flags))
        tok_rows, full_kvb = spread(mask, picked.reshape(GROUP, tok_count, d_model), (w_kv_up,))
        full_wq, full_wo, full_kva = bundle[:, :3072], bundle[:, 3072:5120], bundle[:, 5120:]
        tok_rows, grad_rows = lax.optimization_barrier((tok_rows, grad_rows))
        all_dy = lax.all_gather(grad_rows, 'fsdp', tiled=True)
        block_out, d_normed, normed, mix, latent, d_query, d_down, d_up, d_gain, d_kv_gain = block_step(
            tok_rows.astype(F32), grad_rows, (gain_full, full_wq, full_kva, kv_gain_full, full_kvb, full_wo), seq_count)
        all_dn = lax.all_gather(d_normed, 'fsdp', tiled=True)
        small = jnp.concatenate([d_gain.reshape(GROUP, 1, 128), jnp.pad(d_kv_gain.reshape(GROUP, 1, 32), ((0, 0), (0, 0), (0, 96))), jnp.zeros((GROUP, 6, 128), F32)], axis=1)
        block_out, mix = lax.optimization_barrier((block_out, mix))
        g_out, g_query, g_down, g_up, g_small = grad_shards(mix, all_dy, normed, jnp.pad(d_down, ((0, 0), (0, D_DOWN - d_down.shape[1]))), d_query, latent.T, d_up, small)
        grad_table = table_grad(starts, keys & 8191, (keys >> 13) & (ROW_BLK - 1), flags, gain_full.reshape(1, -1), all_dy, all_dn, picked, vocab_dev)
        return (block_out.reshape(seq_count, seq_len, d_model), grad_table, g_small[0], g_query, g_down[:, :576], g_small[1, :32], g_up, g_out)

    return jax.shard_map(device_step, mesh=mesh, in_specs=(tok_spec, seq_spec, mat_spec, vec_spec, mat_spec, mat_spec, vec_spec, mat_spec, mat_spec), out_specs=(seq_spec, tok_spec, part_vec, tok_spec, tok_spec, part_vec, tok_spec, tok_spec), check_vma=False)
```

```python
import math
import jax
import jax.numpy as jnp
from jax import lax
from jax.sharding import PartitionSpec as P
from jax.experimental import pallas as pl
from jax.experimental.pallas import tpu as pltpu

NOPE_DIM = 128
ROPE_DIM = 64
VALUE_DIM = 128
ROPE_THETA = 50000.0
RMS_EPS = 1e-6
ATTN_SCALE = (NOPE_DIM + ROPE_DIM) ** -0.5 * (0.1 * math.log(32.0) + 1.0) ** 2
ROW_DIMS = (((0,), (0,)), ((), ()))
COL_DIMS = (((1,), (1,)), ((), ()))


def rms_scale(in_vals, gain_vec):
    vals_f32 = in_vals.astype(jnp.float32)
    inv_rms = lax.rsqrt(jnp.mean(vals_f32 * vals_f32, axis=-1, keepdims=True) + RMS_EPS)
    return (vals_f32 * inv_rms * gain_vec).astype(jnp.bfloat16)


def rope_tables(seq_len):
    positions = jnp.arange(seq_len, dtype=jnp.float32)
    inv_freq = ROPE_THETA ** (-2.0 * jnp.arange(ROPE_DIM // 2, dtype=jnp.float32) / ROPE_DIM)
    rot_angle = positions[:, None] * inv_freq[None, :]
    rot_angle = jnp.concatenate([rot_angle, rot_angle], axis=-1)
    return jnp.cos(rot_angle), jnp.sin(rot_angle)


def apply_rope(in_vals, cos_tab, sin_tab):
    half_dim = ROPE_DIM // 2
    vals_f32 = in_vals.astype(jnp.float32)
    turned = jnp.concatenate([-vals_f32[..., half_dim:], vals_f32[..., :half_dim]], axis=-1)
    return (vals_f32 * cos_tab + turned * sin_tab).astype(jnp.bfloat16)


def attend_local(q_proj, pe_raw, kv_up):
    seq_len = q_proj.shape[1]
    cos_tab, sin_tab = rope_tables(seq_len)
    q_rot = apply_rope(q_proj[..., NOPE_DIM:], cos_tab[:, None, :], sin_tab[:, None, :])
    k_rot = apply_rope(pe_raw, cos_tab, sin_tab)
    scores = jnp.einsum('bshd,bthd->bhst', q_proj[..., :NOPE_DIM], kv_up[..., :NOPE_DIM], preferred_element_type=jnp.float32)
    scores = scores + jnp.einsum('bshd,btd->bhst', q_rot, k_rot, preferred_element_type=jnp.float32)
    positions = jnp.arange(seq_len)
    causal = positions[:, None] >= positions[None, :]
    scores = jnp.where(causal, scores * ATTN_SCALE, -1e30)
    attn_probs = jax.nn.softmax(scores, axis=-1).astype(jnp.bfloat16)
    attn_mix = jnp.einsum('bhst,bthd->bshd', attn_probs, kv_up[..., NOPE_DIM:], preferred_element_type=jnp.float32)
    return attn_mix.astype(jnp.bfloat16)


F32, BF16 = jnp.float32, jnp.bfloat16
MESH = pl.DeviceIdType.MESH
ANY = pl.BlockSpec(memory_space=pl.ANY)
RING = 8
GROUP = 16

def chip_at(pos):
    side = pos // 4
    return (pos + side * (7 - 2 * pos)) * 2 + side

def place():
    me = lax.axis_index('fsdp')
    core = me % 2
    chip = me // 2
    side = chip % 2
    zz = chip // 2
    return me, core, zz + side * (7 - 2 * zz)

def at_pos(pos, core):
    return chip_at(pos % RING) * 2 + core

def meet_all(me):
    barrier = pltpu.get_barrier_semaphore()
    for step in range(1, GROUP):
        pl.semaphore_signal(barrier, inc=1, device_id={'fsdp': (me + step) % GROUP}, device_id_type=MESH)
    pl.semaphore_wait(barrier, GROUP - 1)

TOK = 288
D_OUT, D_CAT, D_UP, D_DOWN = 2048, 3712, 4096, 640
WO_COL = 3072
CUT = 1792
PARTS = (('u', 0, 0, 2048), ('u', 1, 2048, 2048), ('n', 0, 0, 896), ('n', 1, 1792, 1024), ('n', 0, 896, 896), ('n', 1, 2816, 896))
N_PARTS = len(PARTS)
ROWS = {'n': 128, 'u': 32}

def col_tiles(width):
    step = 512
    return [(c, min(step, width - c)) for c in range(0, width, step)]

def grad_kernel(mix_h, dy_h, nrm_h, dd_h, dq_h, lat_h, du_h, sm_h, h0_h, wo_h, y_h, go_h, gq_h, gd_h, gu_h, gs_h,
                mix, dy, go, nrm, cat, lat, du, b0, b1, b2, b3, b4, b5, mixf, h0, wo, yv, smr, ssum, loc_sem, xs_sem, xr_sem, s_sem, r_sem, ms_sem, mr_sem, cs_sem, cr_sem, dy_sem, y_sem, out_sem):
    me, core, pos = place()
    partner = me + 1 - 2 * core
    meet_all(me)
    acts = ((lat_h, lat), (du_h, du), (nrm_h, nrm), (dd_h, cat.at[:, :, 0:D_DOWN]), (dq_h, cat.at[:, :, D_DOWN:D_CAT]))
    local, cross = [], []
    for i, (src, dst) in enumerate(acts):
        cp = pltpu.make_async_copy(src, dst.at[core], loc_sem.at[i])
        cp.start()
        local.append(cp)
        rc = pltpu.make_async_remote_copy(src, dst.at[core], xs_sem.at[i], xr_sem.at[i], device_id={'fsdp': partner}, device_id_type=MESH)
        rc.start()
        cross.append(rc)
    own_small = pltpu.make_async_copy(sm_h.at[me], smr.at[0], loc_sem.at[5])
    own_small.start()
    own_mix = pltpu.make_async_copy(mix_h.at[:, pl.ds(pl.multiple_of(me * 128, 128), 128)], mix.at[me], loc_sem.at[6])
    own_mix.start()
    smalls, mixes = [], []
    for i in range(1, GROUP):
        peer = (me + i) % GROUP
        rc = pltpu.make_async_remote_copy(sm_h.at[peer], smr.at[i], ms_sem.at[i], mr_sem.at[i], device_id={'fsdp': peer}, device_id_type=MESH)
        rc.start()
        smalls.append(rc)
    for i, (src, dst) in enumerate(((mix_h, mixf), (h0_h, h0))):
        pltpu.make_async_copy(src, dst, y_sem.at[2 + i]).start()

    def wo_load(t):
        return pltpu.make_async_copy(wo_h.at[:, pl.ds(pl.multiple_of(WO_COL + t * 512, 512), 512)], wo.at[t % 2], y_sem.at[t % 2])
    wo_load(0).start()
    bufs = (b0, b1, b2, b3, b4, b5)
    peers = (at_pos(pos + 1, core), at_pos(pos + 7, core))
    left_ops = {'n': (nrm, cat), 'u': (lat, du)}

    def mix_send(i):
        peer = (me + i) % GROUP
        return pltpu.make_async_remote_copy(mix_h.at[:, pl.ds(pl.multiple_of(peer * 128, 128), 128)], mix.at[me], cs_sem.at[i], cr_sem.at[i],
                                            device_id={'fsdp': peer}, device_id_type=MESH)

    def dy_load(blk):
        return pltpu.make_async_copy(dy_h.at[pl.ds(pl.multiple_of(blk * TOK, TOK), TOK), :], dy.at[blk % 2], dy_sem.at[blk % 2])

    def hop(p, step):
        return pltpu.make_async_remote_copy(bufs[p].at[step], bufs[p].at[step + 1], s_sem.at[p, step], r_sem.at[p, step + 1],
                                            device_id={'fsdp': peers[PARTS[p][1]]}, device_id_type=MESH)

    def work(p, step):
        kind, way, c0, width = PARTS[p]
        chip = chip_at((pos + 7 - step + way * (2 * step + 2)) % RING)
        lhs_ref, rhs_ref = left_ops[kind]
        rows = ROWS[kind]
        row = pl.multiple_of((chip * 2 + core) * rows, rows)
        lhs = [lhs_ref[b, pl.ds(row, rows), :] for b in range(2)]
        for c, w in col_tiles(width):
            part = sum(jnp.dot(lhs[b], rhs_ref[b, :, c0 + c:c0 + c + w], preferred_element_type=F32) for b in range(2))
            bufs[p][step, :, c:c + w] = bufs[p][step, :, c:c + w] + part

    for i in range(1, GROUP):
        mix_send(i).start()
    dy_load(0).start()
    go[...] = jnp.zeros_like(go)
    for p in range(N_PARTS):
        bufs[p][0] = jnp.zeros(bufs[p].shape[1:], F32)
    for i in range(5):
        local[i].wait()
        cross[i].wait_recv()

    @pl.loop(0, RING)
    def _(step):
        for p in range(N_PARTS):
            @pl.when(step > 0)
            def _():
                hop(p, step - 1).wait_recv()
            work(p, step)

            @pl.when(step < RING - 1)
            def _():
                hop(p, step).start()

        @pl.when(step == 0)
        def _():
            own_mix.wait()
            for i in range(1, GROUP):
                mix_send(i).wait()

        @pl.when((step > 0) & (step < 5))
        def _():
            @pl.loop(0, 4)
            def _(j):
                blk = (step - 1) * 4 + j
                dy_load(blk).wait()

                @pl.when(blk < GROUP - 1)
                def _():
                    dy_load(blk + 1).start()
                for c, w in col_tiles(2048):
                    go[:, c:c + w] += lax.dot_general(mix[blk], dy[blk % 2, :, c:c + w], (((0,), (0,)), ((), ())), preferred_element_type=F32)

        @pl.when(step == 5)
        def _():
            for i, (src, dst) in enumerate(((mix_h, mixf), (h0_h, h0))):
                pltpu.make_async_copy(src, dst, y_sem.at[2 + i]).wait()

            @pl.loop(0, 4)
            def _(t):
                wo_load(t).wait()

                @pl.when(t < 3)
                def _():
                    wo_load(t + 1).start()
                here = pl.ds(pl.multiple_of(t * 512, 512), 512)
                yv[:, here] = (h0[:, here].astype(F32) + jnp.dot(mixf[...], wo[t % 2], preferred_element_type=F32)).astype(BF16)

    last = RING - 1
    outs = []
    cp = pltpu.make_async_copy(go, go_h, out_sem.at[6])
    cp.start()
    outs.append(cp)
    cp = pltpu.make_async_copy(yv, y_h, out_sem.at[9])
    cp.start()
    outs.append(cp)
    targets = (((gu_h.at[:, 0:2048], 0, 2048),), ((gu_h.at[:, 2048:4096], 0, 2048),), ((gd_h, 0, 640), (gq_h.at[:, 0:256], 640, 896)),
               ((gq_h.at[:, 1152:2176], 0, 1024),), ((gq_h.at[:, 256:1152], 0, 896),), ((gq_h.at[:, 2176:3072], 0, 896),))
    for p in range(N_PARTS):
        for n, (dst, c0, c1) in enumerate(targets[p]):
            cp = pltpu.make_async_copy(bufs[p].at[last, :, c0:c1], dst, out_sem.at[p + 6 * n])
            cp.start()
            outs.append(cp)
    own_small.wait()
    for rc in smalls:
        rc.wait()
    ssum[...] = jnp.sum(smr[...], axis=0)
    cp = pltpu.make_async_copy(ssum, gs_h, out_sem.at[7])
    cp.start()
    outs.append(cp)
    for rc in cross:
        rc.wait_send()
    for p in range(N_PARTS):
        @pl.loop(0, last)
        def _(step):
            hop(p, step).wait_send()
    for cp in outs:
        cp.wait()


def grad_shards(mix, dy_all, nrm_t, dd, dq, lat_t, du, small, rows, weights):
    shapes = [(ROWS[k], RING, w) for k, _, _, w in PARTS]
    scratch = [pltpu.VMEM((GROUP, TOK, 128), BF16), pltpu.VMEM((2, TOK, 2048), BF16), pltpu.VMEM((128, 2048), F32), pltpu.VMEM((2, 2048, TOK), BF16),
               pltpu.VMEM((2, TOK, D_CAT), BF16), pltpu.VMEM((2, 512, TOK), BF16), pltpu.VMEM((2, TOK, D_UP), BF16)]
    scratch += [pltpu.VMEM((RING, r, w), F32) for r, _, w in shapes]
    scratch += [pltpu.VMEM((TOK, 2048), BF16), pltpu.VMEM((TOK, 2048), BF16), pltpu.VMEM((2, 2048, 512), BF16), pltpu.VMEM((TOK, 2048), BF16)]
    scratch += [pltpu.VMEM((GROUP, 8, 128), F32), pltpu.VMEM((8, 128), F32)]
    dma = pltpu.SemaphoreType.DMA
    scratch += [dma((7,)), dma((5,)), dma((5,)), dma((N_PARTS, RING)), dma((N_PARTS, RING)), dma((GROUP,)), dma((GROUP,)), dma((GROUP,)), dma((GROUP,)), dma((2,)), dma((4,)), dma((10,))]
    return pl.pallas_call(
        grad_kernel,
        out_shape=(jax.ShapeDtypeStruct((TOK, 2048), BF16), jax.ShapeDtypeStruct((128, 2048), F32), jax.ShapeDtypeStruct((128, 3072), F32), jax.ShapeDtypeStruct((128, D_DOWN), F32), jax.ShapeDtypeStruct((32, D_UP), F32), jax.ShapeDtypeStruct((8, 128), F32)),
        in_specs=[ANY] * 10, out_specs=(ANY,) * 6, scratch_shapes=scratch,
        compiler_params=pltpu.CompilerParams(collective_id=1, has_side_effects=True, vmem_limit_bytes=60 * 1024 * 1024),
        cost_estimate=pl.CostEstimate(flops=8 * 10**9, bytes_accessed=20 * 10**6, transcendentals=0), name='grad_shards',
    )(mix, dy_all, nrm_t, dd, dq, lat_t, du, small, rows, weights)


W_SHARDS = ((32, 4096),)
HALF_TOK = TOK // 2


def spread_kernel(n_w, *refs):
    mask, rows_h = refs[0:2]
    srcs = refs[2:2 + n_w]
    got_h = refs[2 + n_w]
    outs = refs[3 + n_w:3 + 2 * n_w]
    stage = refs[3 + 2 * n_w:3 + 3 * n_w]
    own, mate, way0, way1 = refs[3 + 3 * n_w:7 + 3 * n_w]
    in_sem, own_sem, s_sem, r_sem, ps_sem, pr_sem, h_in, m_s, m_r, hs_sem, hr_sem, out_sem = refs[7 + 3 * n_w:]
    me, core, pos = place()
    partner = me + 1 - 2 * core
    barrier = pltpu.get_barrier_semaphore()
    peers = (at_pos(pos + 1, core), at_pos(pos + 7, core))
    for peer in peers + (partner,):
        pl.semaphore_signal(barrier, inc=1, device_id={'fsdp': peer}, device_id_type=MESH)
    pl.semaphore_wait(barrier, 3)
    loads = []
    for i in range(n_w):
        cp = pltpu.make_async_copy(srcs[i], stage[i], in_sem.at[i])
        cp.start()
        loads.append(cp)

    def row_load(q):
        return pltpu.make_async_copy(rows_h.at[at_pos(q, core)], own.at[q], h_in.at[q])

    def row_share(q):
        return pltpu.make_async_remote_copy(rows_h.at[at_pos(q, 1 - core)], mate.at[q], m_s.at[q], m_r.at[q],
                                            device_id={'fsdp': partner}, device_id_type=MESH)
    for j in (7, 1, 6, 2, 5, 3, 4, 0):
        row_share((pos + j) % RING).start()
        row_load((pos + j) % RING).start()

    def where(i, way, source):
        rows = W_SHARDS[i][0]
        half = rows // 2
        return outs[i].at[pl.ds(pl.multiple_of(source * rows + way * half, half), half), :]

    def origin(way, step):
        return at_pos(pos + 8 - step + way * 2 * step, core)

    def hop(i, way, step, src=None):
        spot = where(i, way, origin(way, step))
        return pltpu.make_async_remote_copy(spot if src is None else src, spot, s_sem.at[i, way, step], r_sem.at[i, way, step + 1],
                                            device_id={'fsdp': peers[way]}, device_id_type=MESH)

    def arrive(i, way, step):
        spot = where(i, way, origin(way, step))
        return pltpu.make_async_remote_copy(spot, spot, s_sem.at[i, way, step], r_sem.at[i, way, step],
                                            device_id={'fsdp': peers[way]}, device_id_type=MESH)

    def share(i, way, step, src=None):
        spot = where(i, way, origin(way, step))
        return pltpu.make_async_remote_copy(spot if src is None else src, spot, ps_sem.at[i, way, step], pr_sem.at[i, way, step],
                                            device_id={'fsdp': partner}, device_id_type=MESH)
    ways = (way0, way1)

    def row_hop(way, step):
        return pltpu.make_async_remote_copy(ways[way].at[step], ways[way].at[step + 1], hs_sem.at[way, step], hr_sem.at[way, step + 1],
                                            device_id={'fsdp': peers[way]}, device_id_type=MESH)

    def fill(way, step, first):
        q = (pos + 7 - step + way * (2 * step + 2)) % RING
        chip = chip_at(q)
        for c in range(0, HALF_TOK, 48):
            lo = way * HALF_TOK + c
            mine, theirs = mask[0, chip, lo:lo + 48, :], mask[1, chip, lo:lo + 48, :]
            for w in range(0, 2048, 128):
                part = own[q, lo:lo + 48, w:w + 128] * mine + mate[q, lo:lo + 48, w:w + 128] * theirs
                if not first:
                    part = part + ways[way][step, c:c + 48, w:w + 128]
                ways[way][step, c:c + 48, w:w + 128] = part

    kept = []
    for i in range(n_w):
        loads[i].wait()
        half = W_SHARDS[i][0] // 2
        for way in range(2):
            src = stage[i].at[way * half:(way + 1) * half, :]
            hop(i, way, 0, src).start()
            share(i, way, 0, src).start()
            cp = pltpu.make_async_copy(src, where(i, way, me), own_sem.at[i, way])
            cp.start()
            kept.append(cp)
    for j in (7, 1, 6, 2, 5, 3, 4, 0):
        row_load((pos + j) % RING).wait()
        row_share((pos + j) % RING).wait_recv()
        if j in (7, 1):
            way = 0 if j == 7 else 1
            fill(way, 0, True)
            row_hop(way, 0).start()

    @pl.loop(1, RING)
    def _(step):
        for i in range(n_w):
            for way in range(2):
                arrive(i, way, step).wait_recv()

                @pl.when(step < RING - 1)
                def _():
                    hop(i, way, step).start()
                share(i, way, step).start()
        for way in range(2):
            row_hop(way, step - 1).wait_recv()
            fill(way, step, False)

            @pl.when(step < RING - 1)
            def _():
                row_hop(way, step).start()

    for way in range(2):
        cp = pltpu.make_async_copy(ways[way].at[RING - 1], got_h.at[way * HALF_TOK:(way + 1) * HALF_TOK, :], out_sem.at[way])
        cp.start()
        kept.append(cp)
    for cp in kept:
        cp.wait()

    @pl.loop(0, RING)
    def _(step):
        row_share(step).wait_send()

        @pl.when(step < RING - 1)
        def _():
            for way in range(2):
                row_hop(way, step).wait_send()
        for i in range(n_w):
            for way in range(2):
                @pl.when(step < RING - 1)
                def _():
                    hop(i, way, step).wait_send()
                share(i, way, step).wait()


def spread(mask, rows, shards):
    dma = pltpu.SemaphoreType.DMA
    n_w = len(shards)
    return pl.pallas_call(
        lambda *refs: spread_kernel(n_w, *refs),
        out_shape=(jax.ShapeDtypeStruct((TOK, 2048), BF16),) + tuple(jax.ShapeDtypeStruct((GROUP * r, w), BF16) for r, w in W_SHARDS),
        in_specs=[pl.BlockSpec(memory_space=pltpu.VMEM)] + [ANY] * (n_w + 1), out_specs=(ANY,) * (n_w + 1),
        scratch_shapes=[pltpu.VMEM(s, BF16) for s in W_SHARDS] + [pltpu.VMEM((RING, TOK, 2048), BF16)] * 2 + [pltpu.VMEM((RING, HALF_TOK, 2048), BF16)] * 2
        + [dma((max(n_w, 1),)), dma((max(n_w, 1), 2))] + [dma((max(n_w, 1), 2, RING)) for _ in range(4)] + [dma((RING,)) for _ in range(3)] + [dma((2, RING)) for _ in range(2)] + [dma((2,))],
        compiler_params=pltpu.CompilerParams(collective_id=2, has_side_effects=True, vmem_limit_bytes=60 * 1024 * 1024),
        cost_estimate=pl.CostEstimate(flops=8 * 10**9, bytes_accessed=27 * 10**6, transcendentals=0), name='spread',
    )(mask, rows, *shards)
ROW_BLK = 128
IN_BLK = 144
SUB = 48
PIECE = 16
UNROLL = 4
IN_SLOTS = 4
OUT_SLOTS = 4


def table_kernel(starts, toks, rows, flags, gain, dy_h, dn_h, h_h, out_h, grad, dy, dn, hh, acc, ob, nil, in_sem, out_sem):
    n_in = GROUP * TOK // IN_BLK
    n_out = out_h.shape[0] // ROW_BLK

    def loads(blk):
        span = pl.ds(pl.multiple_of(blk * IN_BLK, IN_BLK), IN_BLK)
        slot = blk % IN_SLOTS
        return [pltpu.make_async_copy(src.at[span, :], dst.at[slot], in_sem.at[i, slot]) for i, (src, dst) in enumerate(((dy_h, dy), (dn_h, dn), (h_h, hh)))]
    for blk in range(IN_SLOTS - 1):
        for cp in loads(blk):
            cp.start()

    @pl.loop(0, n_in)
    def _(blk):
        slot = blk % IN_SLOTS
        for cp in loads(blk):
            cp.wait()

        @pl.when(blk < n_in - IN_SLOTS + 1)
        def _():
            for cp in loads(blk + IN_SLOTS - 1):
                cp.start()

        @pl.loop(0, IN_BLK // SUB)
        def _(g):
            @pl.when(flags[blk * (IN_BLK // SUB) + g] > 0)
            def _():
                r0 = pl.multiple_of(g * SUB, PIECE)
                o0 = pl.multiple_of(blk * IN_BLK + g * SUB, PIECE)
                pieces = range(0, SUB, PIECE)

                def tile(ref, p, c):
                    return ref[slot, pl.ds(r0 + p, PIECE), c:c + 128].astype(F32)
                scale = []
                for p in pieces:
                    sq = jnp.zeros((PIECE, 128), F32)
                    al = jnp.zeros((PIECE, 128), F32)
                    for c in range(0, 2048, 128):
                        h = tile(hh, p, c)
                        sq = sq + h * h
                        al = al + h * (tile(dn, p, c) * gain[:, c:c + 128])
                    scale.append((jnp.sum(sq, axis=1, keepdims=True), jnp.sum(al, axis=1, keepdims=True)))
                for p, (sq, al) in zip(pieces, scale):
                    inv = lax.rsqrt(sq * (1.0 / 2048) + RMS_EPS)
                    coef = inv * inv * inv * (al * (1.0 / 2048))
                    for c in range(0, 2048, 128):
                        s = tile(dn, p, c) * gain[:, c:c + 128]
                        grad[pl.ds(o0 + p, PIECE), c:c + 128] = tile(dy, p, c) + inv * s - coef * tile(hh, p, c)

    def store(blk, src):
        return pltpu.make_async_copy(src, out_h.at[pl.ds(pl.multiple_of(blk * ROW_BLK, ROW_BLK), ROW_BLK), :], out_sem.at[blk % OUT_SLOTS])
    nil[...] = jnp.zeros_like(nil)

    @pl.loop(0, n_out)
    def _(blk):
        first, last = starts[blk], starts[blk + 1]
        slot = blk % OUT_SLOTS

        @pl.when(blk >= OUT_SLOTS)
        def _():
            store(blk - OUT_SLOTS, nil).wait()

        @pl.when(first == last)
        def _():
            store(blk, nil).start()

        @pl.when(first < last)
        def _():
            acc[...] = jnp.zeros_like(acc)

            def add(k):
                acc[pl.ds(rows[k], 1), :] += grad[pl.ds(toks[k], 1), :]
            quads = (last - first) // UNROLL

            @pl.loop(0, quads)
            def _(i):
                for j in range(UNROLL):
                    add(first + i * UNROLL + j)

            @pl.loop(first + quads * UNROLL, last)
            def _(k):
                add(k)
            ob[slot] = acc[...].astype(BF16)
            store(blk, ob.at[slot]).start()
    for blk in range(n_out - OUT_SLOTS, n_out):
        store(blk, nil).wait()


def table_grad(starts, toks, rows, flags, gain, dy_all, dn_all, picked, vocab_dev):
    smem = pl.BlockSpec(memory_space=pltpu.SMEM)
    dma = pltpu.SemaphoreType.DMA
    return pl.pallas_call(
        table_kernel, out_shape=jax.ShapeDtypeStruct((vocab_dev, 2048), BF16),
        in_specs=[smem] * 4 + [pl.BlockSpec(memory_space=pltpu.VMEM)] + [ANY] * 3, out_specs=ANY,
        scratch_shapes=[pltpu.VMEM((GROUP * TOK, 2048), F32)] + [pltpu.VMEM((IN_SLOTS, IN_BLK, 2048), BF16)] * 3 + [pltpu.VMEM((ROW_BLK, 2048), F32), pltpu.VMEM((OUT_SLOTS, ROW_BLK, 2048), BF16), pltpu.VMEM((ROW_BLK, 2048), BF16), dma((3, IN_SLOTS)), dma((OUT_SLOTS,))],
        compiler_params=pltpu.CompilerParams(vmem_limit_bytes=60 * 1024 * 1024),
        cost_estimate=pl.CostEstimate(flops=10**9, bytes_accessed=80 * 10**6, transcendentals=0), name='table_grad',
    )(starts, toks, rows, flags, gain, dy_all, dn_all, picked)


def small_kernel(src, out, loc_sem, s_sem, r_sem):
    me = lax.axis_index('fsdp')
    meet_all(me)
    own = pltpu.make_async_copy(src, out.at[me], loc_sem)
    own.start()

    def send(step):
        return pltpu.make_async_remote_copy(src, out.at[me], s_sem.at[step], r_sem.at[step],
                                            device_id={'fsdp': (me + step) % GROUP}, device_id_type=MESH)
    for step in range(1, GROUP):
        send(step).start()
    for step in range(1, GROUP):
        send(step).wait()
    own.wait()


def small_gather(tile):
    dma = pltpu.SemaphoreType.DMA
    return pl.pallas_call(
        small_kernel, out_shape=jax.ShapeDtypeStruct((GROUP, 8, 128), F32),
        in_specs=[pl.BlockSpec(memory_space=pltpu.VMEM)], out_specs=pl.BlockSpec(memory_space=pltpu.VMEM),
        scratch_shapes=[dma, dma((GROUP,)), dma((GROUP,))],
        compiler_params=pltpu.CompilerParams(collective_id=0, has_side_effects=True),
        cost_estimate=pl.CostEstimate(flops=10**7, bytes_accessed=10**5, transcendentals=0), name='small_gather',
    )(tile)


def blank(shape, dtype):
    return pl.pallas_call(lambda out: None, out_shape=jax.ShapeDtypeStruct(shape, dtype), out_specs=ANY, name='blank')()


def block_step(rows_f32, grad_rows, full_weights, seq_count):
    gain_vec, w_query, w_kv_down, kv_gain, w_kv_up, w_out = full_weights
    kv_rank = kv_gain.shape[0]
    tok_count = rows_f32.shape[0]
    seq_len = tok_count // seq_count
    normed, norm_pull = jax.vjp(rms_scale, rows_f32, gain_vec)
    q_proj = jnp.dot(normed, w_query, preferred_element_type=jnp.float32).astype(jnp.bfloat16)
    kv_down = jnp.dot(normed, w_kv_down, preferred_element_type=jnp.float32).astype(jnp.bfloat16)
    latent, latent_pull = jax.vjp(rms_scale, kv_down[:, :kv_rank], kv_gain)
    kv_up = jnp.dot(latent, w_kv_up, preferred_element_type=jnp.float32).astype(jnp.bfloat16)
    attn_mix, attn_pull = jax.vjp(attend_local, q_proj.reshape(seq_count, seq_len, -1, NOPE_DIM + ROPE_DIM), kv_down[:, kv_rank:].reshape(seq_count, seq_len, ROPE_DIM), kv_up.reshape(seq_count, seq_len, -1, NOPE_DIM + VALUE_DIM))
    mix_rows = attn_mix.reshape(tok_count, -1)
    d_mix = lax.dot_general(grad_rows, w_out, COL_DIMS, preferred_element_type=jnp.float32).astype(jnp.bfloat16)
    d_query, d_pe, d_up = attn_pull(d_mix.reshape(attn_mix.shape))
    d_query = d_query.reshape(tok_count, -1)
    d_up = d_up.reshape(tok_count, -1)
    d_latent = lax.dot_general(d_up, w_kv_up, COL_DIMS, preferred_element_type=jnp.float32).astype(jnp.bfloat16)
    d_ckv, d_kv_gain = latent_pull(d_latent)
    d_down = jnp.concatenate([d_ckv, d_pe.reshape(tok_count, ROPE_DIM)], axis=1)
    d_normed = lax.dot_general(d_query, w_query, COL_DIMS, preferred_element_type=jnp.float32)
    d_normed = d_normed + lax.dot_general(d_down, w_kv_down, COL_DIMS, preferred_element_type=jnp.float32)
    d_normed = d_normed.astype(jnp.bfloat16)
    _, d_gain = norm_pull(d_normed)
    return d_normed, normed, mix_rows, latent, d_query, d_down, d_up, d_gain, d_kv_gain


def solution(mesh):
    tok_spec = P(('dp', 'fsdp'), None)
    seq_spec = P(('dp', 'fsdp'), None, None)
    part_vec = P(('dp', 'fsdp'))
    vec_spec = P('fsdp')
    mat_spec = P('fsdp', None)

    def device_step(tok_ids, grad_out, emb_table, norm_gain, w_query, w_kv_down, kv_gain, w_kv_up, w_out):
        seq_count, seq_len = tok_ids.shape
        vocab_dev, d_model = emb_table.shape
        tok_count = seq_count * seq_len
        me = lax.axis_index('fsdp')
        grad_rows = grad_out.reshape(tok_count, d_model)
        bundle = lax.all_gather(jnp.concatenate([w_query, w_out, w_kv_down], axis=1), 'fsdp', tiled=True)
        fill = lambda rows: jnp.pad(rows, ((0, 0), (0, 128 - rows.shape[1])))
        tile = jnp.concatenate([fill(tok_ids.astype(F32)), norm_gain.astype(F32).reshape(1, 128), fill(kv_gain.astype(F32).reshape(1, 32)), jnp.zeros((3, 128), F32)], axis=0)
        table = small_gather(tile)
        all_ids = table[:, :seq_count, :seq_len].reshape(GROUP, tok_count).astype(jnp.int32)
        gain_full = table[:, 3, :].reshape(-1)
        kv_gain_full = table[:, 4, :32].reshape(-1)

        owner = all_ids // vocab_dev
        mine = (owner == me)
        local = all_ids - me * vocab_dev
        stamp = jnp.arange(GROUP * tok_count).reshape(GROUP, tok_count) * ROW_BLK
        keys = lax.sort(jnp.where(mine, (local // ROW_BLK) * 2**20 + stamp + local % ROW_BLK, 2**30).reshape(-1))
        starts = jnp.sum((mine & (local < ROW_BLK * jnp.arange(vocab_dev // ROW_BLK + 1)[:, None, None])).astype(jnp.int32), axis=(1, 2))
        flags = jnp.sum(mine.reshape(-1, SUB).astype(jnp.int32), axis=1)
        picked = jnp.take(emb_table, jnp.where(mine, local, 0).reshape(-1), axis=0, mode='clip')
        core = me % 2
        near = lax.dynamic_index_in_dim(owner.reshape(RING, 2, tok_count), core, 1, keepdims=False)
        mask = jnp.stack([near == me, near == me + 1 - 2 * core]).astype(BF16)
        mask = jnp.broadcast_to(mask[..., None], (2, RING, tok_count, 128))
        picked, keys, starts, flags = lax.optimization_barrier((picked, keys, starts, flags))
        tok_rows, full_kvb = spread(mask, picked.reshape(GROUP, tok_count, d_model), (w_kv_up,))
        full_wq, full_wo, full_kva = bundle[:, :3072], bundle[:, 3072:5120], bundle[:, 5120:]
        tok_rows, grad_rows = lax.optimization_barrier((tok_rows, grad_rows))
        all_dy = lax.all_gather(grad_rows, 'fsdp', tiled=True)
        d_normed, normed, mix, latent, d_query, d_down, d_up, d_gain, d_kv_gain = block_step(
            tok_rows.astype(F32), grad_rows, (gain_full, full_wq, full_kva, kv_gain_full, full_kvb, full_wo), seq_count)
        all_dn = lax.all_gather(d_normed, 'fsdp', tiled=True)
        small = jnp.concatenate([d_gain.reshape(GROUP, 1, 128), jnp.pad(d_kv_gain.reshape(GROUP, 1, 32), ((0, 0), (0, 0), (0, 96))), jnp.zeros((GROUP, 6, 128), F32)], axis=1)
        block_out, g_out, g_query, g_down, g_up, g_small = grad_shards(mix, all_dy, normed.T, jnp.pad(d_down, ((0, 0), (0, D_DOWN - d_down.shape[1]))), d_query, latent.T, d_up, small, tok_rows, bundle)
        grad_table = table_grad(starts, (keys >> 7) & 8191, keys & (ROW_BLK - 1), flags, gain_full.reshape(1, -1), all_dy, all_dn, picked, vocab_dev)
        return (block_out.reshape(seq_count, seq_len, d_model), grad_table, g_small[0], g_query, g_down[:, :576], g_small[1, :32], g_up, g_out)

    return jax.shard_map(device_step, mesh=mesh, in_specs=(tok_spec, seq_spec, mat_spec, vec_spec, mat_spec, mat_spec, vec_spec, mat_spec, mat_spec), out_specs=(seq_spec, tok_spec, part_vec, tok_spec, tok_spec, part_vec, tok_spec, tok_spec), check_vma=False)
```

```python
import math
import jax
import jax.numpy as jnp
from jax import lax
from jax.sharding import PartitionSpec as P
from jax.experimental import pallas as pl
from jax.experimental.pallas import tpu as pltpu

NOPE_DIM = 128
ROPE_DIM = 64
VALUE_DIM = 128
ROPE_THETA = 50000.0
RMS_EPS = 1e-6
ATTN_SCALE = (NOPE_DIM + ROPE_DIM) ** -0.5 * (0.1 * math.log(32.0) + 1.0) ** 2
ROW_DIMS = (((0,), (0,)), ((), ()))
COL_DIMS = (((1,), (1,)), ((), ()))


def rms_scale(in_vals, gain_vec):
    vals_f32 = in_vals.astype(jnp.float32)
    inv_rms = lax.rsqrt(jnp.mean(vals_f32 * vals_f32, axis=-1, keepdims=True) + RMS_EPS)
    return (vals_f32 * inv_rms * gain_vec).astype(jnp.bfloat16)


def rope_tables(seq_len):
    positions = jnp.arange(seq_len, dtype=jnp.float32)
    inv_freq = ROPE_THETA ** (-2.0 * jnp.arange(ROPE_DIM // 2, dtype=jnp.float32) / ROPE_DIM)
    rot_angle = positions[:, None] * inv_freq[None, :]
    rot_angle = jnp.concatenate([rot_angle, rot_angle], axis=-1)
    return jnp.cos(rot_angle), jnp.sin(rot_angle)


def apply_rope(in_vals, cos_tab, sin_tab):
    half_dim = ROPE_DIM // 2
    vals_f32 = in_vals.astype(jnp.float32)
    turned = jnp.concatenate([-vals_f32[..., half_dim:], vals_f32[..., :half_dim]], axis=-1)
    return (vals_f32 * cos_tab + turned * sin_tab).astype(jnp.bfloat16)


def attend_local(q_proj, pe_raw, kv_up):
    seq_len = q_proj.shape[1]
    cos_tab, sin_tab = rope_tables(seq_len)
    q_rot = apply_rope(q_proj[..., NOPE_DIM:], cos_tab[:, None, :], sin_tab[:, None, :])
    k_rot = apply_rope(pe_raw, cos_tab, sin_tab)
    scores = jnp.einsum('bshd,bthd->bhst', q_proj[..., :NOPE_DIM], kv_up[..., :NOPE_DIM], preferred_element_type=jnp.float32)
    scores = scores + jnp.einsum('bshd,btd->bhst', q_rot, k_rot, preferred_element_type=jnp.float32)
    positions = jnp.arange(seq_len)
    causal = positions[:, None] >= positions[None, :]
    scores = jnp.where(causal, scores * ATTN_SCALE, -1e30)
    attn_probs = jax.nn.softmax(scores, axis=-1).astype(jnp.bfloat16)
    attn_mix = jnp.einsum('bhst,bthd->bshd', attn_probs, kv_up[..., NOPE_DIM:], preferred_element_type=jnp.float32)
    return attn_mix.astype(jnp.bfloat16)


F32, BF16 = jnp.float32, jnp.bfloat16
MESH = pl.DeviceIdType.MESH
ANY = pl.BlockSpec(memory_space=pl.ANY)
RING = 8
GROUP = 16

def chip_at(pos):
    side = pos // 4
    return (pos + side * (7 - 2 * pos)) * 2 + side

def place():
    me = lax.axis_index('fsdp')
    core = me % 2
    chip = me // 2
    side = chip % 2
    zz = chip // 2
    return me, core, zz + side * (7 - 2 * zz)

def at_pos(pos, core):
    return chip_at(pos % RING) * 2 + core

def meet_all(me):
    barrier = pltpu.get_barrier_semaphore()
    for step in range(1, GROUP):
        pl.semaphore_signal(barrier, inc=1, device_id={'fsdp': (me + step) % GROUP}, device_id_type=MESH)
    pl.semaphore_wait(barrier, GROUP - 1)

TOK = 288
D_OUT, D_CAT, D_UP, D_DOWN = 2048, 3712, 4096, 640
WO_COL = 3072
CUT = 1792
PARTS = (('u', 0, 0, 2048), ('u', 1, 2048, 2048), ('n', 0, 0, 896), ('n', 1, 1792, 1024), ('n', 0, 896, 896), ('n', 1, 2816, 896))
N_PARTS = len(PARTS)
ROWS = {'n': 128, 'u': 32}

def col_tiles(width):
    step = 512
    return [(c, min(step, width - c)) for c in range(0, width, step)]

def grad_kernel(mix_h, dy_h, nrm_h, dd_h, dq_h, lat_h, du_h, sm_h, h0_h, wo_h, wl_h, y_h, go_h, gq_h, gd_h, gu_h, gs_h,
                mix, dy, go, nrm, cat, lat, du, b0, b1, b2, b3, b4, b5, mixf, h0, wo, yv, smr, ssum, loc_sem, xs_sem, xr_sem, s_sem, r_sem, ms_sem, mr_sem, cs_sem, cr_sem, dy_sem, y_sem, out_sem):
    me, core, pos = place()
    partner = me + 1 - 2 * core
    meet_all(me)
    acts = ((lat_h, lat), (du_h, du), (nrm_h, nrm), (dd_h, cat.at[:, :, 0:D_DOWN]), (dq_h, cat.at[:, :, D_DOWN:D_CAT]))
    local, cross = [], []
    for i, (src, dst) in enumerate(acts):
        cp = pltpu.make_async_copy(src, dst.at[core], loc_sem.at[i])
        cp.start()
        local.append(cp)
        rc = pltpu.make_async_remote_copy(src, dst.at[core], xs_sem.at[i], xr_sem.at[i], device_id={'fsdp': partner}, device_id_type=MESH)
        rc.start()
        cross.append(rc)
    own_small = pltpu.make_async_copy(sm_h.at[me], smr.at[0], loc_sem.at[5])
    own_small.start()
    own_mix = pltpu.make_async_copy(mix_h.at[:, pl.ds(pl.multiple_of(me * 128, 128), 128)], mix.at[me], loc_sem.at[6])
    own_mix.start()
    smalls, mixes = [], []
    for i in range(1, GROUP):
        peer = (me + i) % GROUP
        rc = pltpu.make_async_remote_copy(sm_h.at[peer], smr.at[i], ms_sem.at[i], mr_sem.at[i], device_id={'fsdp': peer}, device_id_type=MESH)
        rc.start()
        smalls.append(rc)
    for i, (src, dst) in enumerate(((mix_h, mixf), (h0_h, h0))):
        pltpu.make_async_copy(src, dst, y_sem.at[2 + i]).start()

    def wo_load(t):
        return pltpu.make_async_copy(wo_h.at[:, pl.ds(pl.multiple_of(WO_COL + t * 512, 512), 512)], wo.at[t % 2], y_sem.at[t % 2])

    def wo_last():
        return pltpu.make_async_copy(wl_h, wo.at[1], y_sem.at[1])
    wo_load(0).start()
    bufs = (b0, b1, b2, b3, b4, b5)
    peers = (at_pos(pos + 1, core), at_pos(pos + 7, core))
    left_ops = {'n': (nrm, cat), 'u': (lat, du)}

    def mix_send(i):
        peer = (me + i) % GROUP
        return pltpu.make_async_remote_copy(mix_h.at[:, pl.ds(pl.multiple_of(peer * 128, 128), 128)], mix.at[me], cs_sem.at[i], cr_sem.at[i],
                                            device_id={'fsdp': peer}, device_id_type=MESH)

    def dy_load(blk):
        return pltpu.make_async_copy(dy_h.at[pl.ds(pl.multiple_of(blk * TOK, TOK), TOK), :], dy.at[blk % 2], dy_sem.at[blk % 2])

    def hop(p, step):
        return pltpu.make_async_remote_copy(bufs[p].at[step], bufs[p].at[step + 1], s_sem.at[p, step], r_sem.at[p, step + 1],
                                            device_id={'fsdp': peers[PARTS[p][1]]}, device_id_type=MESH)

    def work(p, step):
        kind, way, c0, width = PARTS[p]
        chip = chip_at((pos + 7 - step + way * (2 * step + 2)) % RING)
        lhs_ref, rhs_ref = left_ops[kind]
        rows = ROWS[kind]
        row = pl.multiple_of((chip * 2 + core) * rows, rows)
        lhs = [lhs_ref[b, pl.ds(row, rows), :] for b in range(2)]
        for c, w in col_tiles(width):
            part = sum(jnp.dot(lhs[b], rhs_ref[b, :, c0 + c:c0 + c + w], preferred_element_type=F32) for b in range(2))
            bufs[p][step, :, c:c + w] = bufs[p][step, :, c:c + w] + part

    for i in range(1, GROUP):
        mix_send(i).start()
    dy_load(0).start()
    go[...] = jnp.zeros_like(go)
    for p in range(N_PARTS):
        bufs[p][0] = jnp.zeros(bufs[p].shape[1:], F32)
    for i in range(5):
        local[i].wait()
        cross[i].wait_recv()

    @pl.loop(0, RING)
    def _(step):
        for p in range(N_PARTS):
            @pl.when(step > 0)
            def _():
                hop(p, step - 1).wait_recv()
            work(p, step)

            @pl.when(step < RING - 1)
            def _():
                hop(p, step).start()

        @pl.when(step == 0)
        def _():
            own_mix.wait()
            for i in range(1, GROUP):
                mix_send(i).wait()

        @pl.when((step > 0) & (step < 5))
        def _():
            @pl.loop(0, 4)
            def _(j):
                blk = (step - 1) * 4 + j
                dy_load(blk).wait()

                @pl.when(blk < GROUP - 1)
                def _():
                    dy_load(blk + 1).start()
                for c, w in col_tiles(2048):
                    go[:, c:c + w] += lax.dot_general(mix[blk], dy[blk % 2, :, c:c + w], (((0,), (0,)), ((), ())), preferred_element_type=F32)

        @pl.when(step == 5)
        def _():
            for i, (src, dst) in enumerate(((mix_h, mixf), (h0_h, h0))):
                pltpu.make_async_copy(src, dst, y_sem.at[2 + i]).wait()

            @pl.loop(0, 4)
            def _(t):
                @pl.when(t < 3)
                def _():
                    wo_load(t).wait()

                @pl.when(t == 3)
                def _():
                    wo_last().wait()

                @pl.when(t < 2)
                def _():
                    wo_load(t + 1).start()

                @pl.when(t == 2)
                def _():
                    wo_last().start()
                here = pl.ds(pl.multiple_of(t * 512, 512), 512)
                yv[:, here] = (h0[:, here].astype(F32) + jnp.dot(mixf[...], wo[t % 2], preferred_element_type=F32)).astype(BF16)

    last = RING - 1
    outs = []
    cp = pltpu.make_async_copy(go, go_h, out_sem.at[6])
    cp.start()
    outs.append(cp)
    cp = pltpu.make_async_copy(yv, y_h, out_sem.at[9])
    cp.start()
    outs.append(cp)
    targets = (((gu_h.at[:, 0:2048], 0, 2048),), ((gu_h.at[:, 2048:4096], 0, 2048),), ((gd_h, 0, 640), (gq_h.at[:, 0:256], 640, 896)),
               ((gq_h.at[:, 1152:2176], 0, 1024),), ((gq_h.at[:, 256:1152], 0, 896),), ((gq_h.at[:, 2176:3072], 0, 896),))
    for p in range(N_PARTS):
        for n, (dst, c0, c1) in enumerate(targets[p]):
            cp = pltpu.make_async_copy(bufs[p].at[last, :, c0:c1], dst, out_sem.at[p + 6 * n])
            cp.start()
            outs.append(cp)
    own_small.wait()
    for rc in smalls:
        rc.wait()
    ssum[...] = jnp.sum(smr[...], axis=0)
    cp = pltpu.make_async_copy(ssum, gs_h, out_sem.at[7])
    cp.start()
    outs.append(cp)
    for rc in cross:
        rc.wait_send()
    for p in range(N_PARTS):
        @pl.loop(0, last)
        def _(step):
            hop(p, step).wait_send()
    for cp in outs:
        cp.wait()


def grad_shards(mix, dy_all, nrm_t, dd, dq, lat_t, du, small, rows, weights, last_cols):
    shapes = [(ROWS[k], RING, w) for k, _, _, w in PARTS]
    scratch = [pltpu.VMEM((GROUP, TOK, 128), BF16), pltpu.VMEM((2, TOK, 2048), BF16), pltpu.VMEM((128, 2048), F32), pltpu.VMEM((2, 2048, TOK), BF16),
               pltpu.VMEM((2, TOK, D_CAT), BF16), pltpu.VMEM((2, 512, TOK), BF16), pltpu.VMEM((2, TOK, D_UP), BF16)]
    scratch += [pltpu.VMEM((RING, r, w), F32) for r, _, w in shapes]
    scratch += [pltpu.VMEM((TOK, 2048), BF16), pltpu.VMEM((TOK, 2048), BF16), pltpu.VMEM((2, 2048, 512), BF16), pltpu.VMEM((TOK, 2048), BF16)]
    scratch += [pltpu.VMEM((GROUP, 8, 128), F32), pltpu.VMEM((8, 128), F32)]
    dma = pltpu.SemaphoreType.DMA
    scratch += [dma((7,)), dma((5,)), dma((5,)), dma((N_PARTS, RING)), dma((N_PARTS, RING)), dma((GROUP,)), dma((GROUP,)), dma((GROUP,)), dma((GROUP,)), dma((2,)), dma((4,)), dma((10,))]
    return pl.pallas_call(
        grad_kernel,
        out_shape=(jax.ShapeDtypeStruct((TOK, 2048), BF16), jax.ShapeDtypeStruct((128, 2048), F32), jax.ShapeDtypeStruct((128, 3072), F32), jax.ShapeDtypeStruct((128, D_DOWN), F32), jax.ShapeDtypeStruct((32, D_UP), F32), jax.ShapeDtypeStruct((8, 128), F32)),
        in_specs=[ANY] * 11, out_specs=(ANY,) * 6, scratch_shapes=scratch,
        compiler_params=pltpu.CompilerParams(collective_id=1, has_side_effects=True, vmem_limit_bytes=60 * 1024 * 1024),
        cost_estimate=pl.CostEstimate(flops=8 * 10**9, bytes_accessed=20 * 10**6, transcendentals=0), name='grad_shards',
    )(mix, dy_all, nrm_t, dd, dq, lat_t, du, small, rows, weights, last_cols)


W_SHARDS = ((32, 4096), (128, 576), (128, 512))
HALF_TOK = TOK // 2


def spread_kernel(n_w, *refs):
    mask, rows_h = refs[0:2]
    srcs = refs[2:2 + n_w]
    got_h = refs[2 + n_w]
    outs = refs[3 + n_w:3 + 2 * n_w]
    stage = refs[3 + 2 * n_w:3 + 3 * n_w]
    own, mate, way0, way1 = refs[3 + 3 * n_w:7 + 3 * n_w]
    in_sem, own_sem, s_sem, r_sem, ps_sem, pr_sem, os_sem, or_sem, xs_sem, xr_sem, ts_sem, tr_sem, h_in, m_s, m_r, hs_sem, hr_sem, out_sem = refs[7 + 3 * n_w:]
    me, core, pos = place()
    twin = lax.axis_index('dp')
    partner = me + 1 - 2 * core
    barrier = pltpu.get_barrier_semaphore()
    peers = (at_pos(pos + 1, core), at_pos(pos + 7, core))
    for peer in peers + (partner,):
        pl.semaphore_signal(barrier, inc=1, device_id={'fsdp': peer}, device_id_type=MESH)
    pl.semaphore_signal(barrier, inc=1, device_id={'dp': 1 - twin}, device_id_type=MESH)
    pl.semaphore_wait(barrier, 4)
    loads = []
    for i in range(n_w):
        cp = pltpu.make_async_copy(srcs[i], stage[i], in_sem.at[i])
        cp.start()
        loads.append(cp)

    def row_load(q):
        return pltpu.make_async_copy(rows_h.at[at_pos(q, core)], own.at[q], h_in.at[q])

    def row_share(q):
        return pltpu.make_async_remote_copy(rows_h.at[at_pos(q, 1 - core)], mate.at[q], m_s.at[q], m_r.at[q],
                                            device_id={'fsdp': partner}, device_id_type=MESH)
    for j in (7, 1, 6, 2, 5, 3, 4, 0):
        row_share((pos + j) % RING).start()
        row_load((pos + j) % RING).start()

    def where(i, way, source, side):
        rows = W_SHARDS[i][0]
        part = rows // 4
        return outs[i].at[pl.ds(pl.multiple_of(source * rows + side * 2 * part + way * part, part), part), :]

    def whole(i):
        rows = W_SHARDS[i][0]
        return outs[i].at[pl.ds(pl.multiple_of(me * rows, rows), rows), :]

    def origin(way, step):
        return at_pos(pos + 8 - step + way * 2 * step, core)

    def hop(i, way, step, src=None):
        spot = where(i, way, origin(way, step), twin)
        return pltpu.make_async_remote_copy(spot if src is None else src, spot, s_sem.at[i, way, step], r_sem.at[i, way, step + 1],
                                            device_id={'fsdp': peers[way]}, device_id_type=MESH)

    def arrive(i, way, step):
        spot = where(i, way, origin(way, step), twin)
        return pltpu.make_async_remote_copy(spot, spot, s_sem.at[i, way, step], r_sem.at[i, way, step],
                                            device_id={'fsdp': peers[way]}, device_id_type=MESH)

    def share(i, way, step):
        spot = where(i, way, origin(way, step), twin)
        return pltpu.make_async_remote_copy(spot, spot, ps_sem.at[i, way, step], pr_sem.at[i, way, step],
                                            device_id={'fsdp': partner}, device_id_type=MESH)

    def share_own(i):
        return pltpu.make_async_remote_copy(stage[i], whole(i), os_sem.at[i], or_sem.at[i], device_id={'fsdp': partner}, device_id_type=MESH)

    def to_twin(i, way, step):
        spot = where(i, way, origin(way, step), twin)
        return pltpu.make_async_remote_copy(spot, spot, xs_sem.at[i, way, step], xr_sem.at[i, way, step],
                                            device_id={'dp': 1 - twin}, device_id_type=MESH)

    def share_twin(i, way, step):
        spot = where(i, way, origin(way, step), 1 - twin)
        return pltpu.make_async_remote_copy(spot, spot, ts_sem.at[i, way, step], tr_sem.at[i, way, step],
                                            device_id={'fsdp': partner}, device_id_type=MESH)
    ways = (way0, way1)

    def row_hop(way, step):
        return pltpu.make_async_remote_copy(ways[way].at[step], ways[way].at[step + 1], hs_sem.at[way, step], hr_sem.at[way, step + 1],
                                            device_id={'fsdp': peers[way]}, device_id_type=MESH)

    def fill(way, step, first):
        q = (pos + 7 - step + way * (2 * step + 2)) % RING
        chip = chip_at(q)
        for c in range(0, HALF_TOK, 48):
            lo = way * HALF_TOK + c
            mine, theirs = mask[0, chip, lo:lo + 48, :], mask[1, chip, lo:lo + 48, :]
            for w in range(0, 2048, 128):
                part = own[q, lo:lo + 48, w:w + 128] * mine + mate[q, lo:lo + 48, w:w + 128] * theirs
                if not first:
                    part = part + ways[way][step, c:c + 48, w:w + 128]
                ways[way][step, c:c + 48, w:w + 128] = part

    kept = []
    for i in range(n_w):
        loads[i].wait()
        part = W_SHARDS[i][0] // 4
        for way in range(2):
            hop(i, way, 0, stage[i].at[pl.ds(pl.multiple_of(twin * 2 * part + way * part, part), part), :]).start()
        share_own(i).start()
        cp = pltpu.make_async_copy(stage[i], whole(i), own_sem.at[i])
        cp.start()
        kept.append(cp)
    for j in (7, 1, 6, 2, 5, 3, 4, 0):
        row_load((pos + j) % RING).wait()
        row_share((pos + j) % RING).wait_recv()
        if j in (7, 1):
            way = 0 if j == 7 else 1
            fill(way, 0, True)
            row_hop(way, 0).start()

    @pl.loop(1, RING)
    def _(step):
        for i in range(n_w):
            for way in range(2):
                arrive(i, way, step).wait_recv()

                @pl.when(step < RING - 1)
                def _():
                    hop(i, way, step).start()
                share(i, way, step).start()
                to_twin(i, way, step).start()
        for way in range(2):
            row_hop(way, step - 1).wait_recv()
            fill(way, step, False)

            @pl.when(step < RING - 1)
            def _():
                row_hop(way, step).start()

        @pl.when(step > 1)
        def _():
            for i in range(n_w):
                for way in range(2):
                    to_twin(i, way, step - 1).wait_recv()
                    share_twin(i, way, step - 1).start()

    for i in range(n_w):
        for way in range(2):
            to_twin(i, way, RING - 1).wait_recv()
            share_twin(i, way, RING - 1).start()
    for way in range(2):
        cp = pltpu.make_async_copy(ways[way].at[RING - 1], got_h.at[way * HALF_TOK:(way + 1) * HALF_TOK, :], out_sem.at[way])
        cp.start()
        kept.append(cp)
    for cp in kept:
        cp.wait()

    @pl.loop(0, RING)
    def _(step):
        row_share(step).wait_send()

        @pl.when(step < RING - 1)
        def _():
            for way in range(2):
                row_hop(way, step).wait_send()
        for i in range(n_w):
            for way in range(2):
                @pl.when(step < RING - 1)
                def _():
                    hop(i, way, step).wait_send()

                @pl.when(step > 0)
                def _():
                    share(i, way, step).wait()
                    to_twin(i, way, step).wait_send()
                    share_twin(i, way, step).wait()
    for i in range(n_w):
        share_own(i).wait()


def spread(mask, rows, shards):
    dma = pltpu.SemaphoreType.DMA
    n_w = len(shards)
    return pl.pallas_call(
        lambda *refs: spread_kernel(n_w, *refs),
        out_shape=(jax.ShapeDtypeStruct((TOK, 2048), BF16),) + tuple(jax.ShapeDtypeStruct((GROUP * r, w), BF16) for r, w in W_SHARDS),
        in_specs=[pl.BlockSpec(memory_space=pltpu.VMEM)] + [ANY] * (n_w + 1), out_specs=(ANY,) * (n_w + 1),
        scratch_shapes=[pltpu.VMEM(s, BF16) for s in W_SHARDS] + [pltpu.VMEM((RING, TOK, 2048), BF16)] * 2 + [pltpu.VMEM((RING, HALF_TOK, 2048), BF16)] * 2
        + [dma((n_w,)), dma((n_w,))] + [dma((n_w, 2, RING))] * 4 + [dma((n_w,))] * 2 + [dma((n_w, 2, RING))] * 4 + [dma((RING,)) for _ in range(3)] + [dma((2, RING)) for _ in range(2)] + [dma((2,))],
        compiler_params=pltpu.CompilerParams(collective_id=2, has_side_effects=True, vmem_limit_bytes=60 * 1024 * 1024),
        cost_estimate=pl.CostEstimate(flops=8 * 10**9, bytes_accessed=27 * 10**6, transcendentals=0), name='spread',
    )(mask, rows, *shards)
ROW_BLK = 128
IN_BLK = 144
SUB = 48
PIECE = 16
UNROLL = 4
IN_SLOTS = 4
OUT_SLOTS = 4


def table_kernel(starts, toks, rows, flags, gain, dy_h, dn_h, h_h, out_h, grad, dy, dn, hh, acc, ob, nil, in_sem, out_sem):
    n_in = GROUP * TOK // IN_BLK
    n_out = out_h.shape[0] // ROW_BLK

    def loads(blk):
        span = pl.ds(pl.multiple_of(blk * IN_BLK, IN_BLK), IN_BLK)
        slot = blk % IN_SLOTS
        return [pltpu.make_async_copy(src.at[span, :], dst.at[slot], in_sem.at[i, slot]) for i, (src, dst) in enumerate(((dy_h, dy), (dn_h, dn), (h_h, hh)))]
    for blk in range(IN_SLOTS - 1):
        for cp in loads(blk):
            cp.start()

    @pl.loop(0, n_in)
    def _(blk):
        slot = blk % IN_SLOTS
        for cp in loads(blk):
            cp.wait()

        @pl.when(blk < n_in - IN_SLOTS + 1)
        def _():
            for cp in loads(blk + IN_SLOTS - 1):
                cp.start()

        @pl.loop(0, IN_BLK // SUB)
        def _(g):
            @pl.when(flags[blk * (IN_BLK // SUB) + g] > 0)
            def _():
                r0 = pl.multiple_of(g * SUB, PIECE)
                o0 = pl.multiple_of(blk * IN_BLK + g * SUB, PIECE)
                pieces = range(0, SUB, PIECE)

                def tile(ref, p, c):
                    return ref[slot, pl.ds(r0 + p, PIECE), c:c + 128].astype(F32)
                scale = []
                for p in pieces:
                    sq = jnp.zeros((PIECE, 128), F32)
                    al = jnp.zeros((PIECE, 128), F32)
                    for c in range(0, 2048, 128):
                        h = tile(hh, p, c)
                        sq = sq + h * h
                        al = al + h * (tile(dn, p, c) * gain[:, c:c + 128])
                    scale.append((jnp.sum(sq, axis=1, keepdims=True), jnp.sum(al, axis=1, keepdims=True)))
                for p, (sq, al) in zip(pieces, scale):
                    inv = lax.rsqrt(sq * (1.0 / 2048) + RMS_EPS)
                    coef = inv * inv * inv * (al * (1.0 / 2048))
                    for c in range(0, 2048, 128):
                        s = tile(dn, p, c) * gain[:, c:c + 128]
                        grad[pl.ds(o0 + p, PIECE), c:c + 128] = tile(dy, p, c) + inv * s - coef * tile(hh, p, c)

    def store(blk, src):
        return pltpu.make_async_copy(src, out_h.at[pl.ds(pl.multiple_of(blk * ROW_BLK, ROW_BLK), ROW_BLK), :], out_sem.at[blk % OUT_SLOTS])
    nil[...] = jnp.zeros_like(nil)

    @pl.loop(0, n_out)
    def _(blk):
        first, last = starts[blk], starts[blk + 1]
        slot = blk % OUT_SLOTS

        @pl.when(blk >= OUT_SLOTS)
        def _():
            store(blk - OUT_SLOTS, nil).wait()

        @pl.when(first == last)
        def _():
            store(blk, nil).start()

        @pl.when(first < last)
        def _():
            acc[...] = jnp.zeros_like(acc)

            def add(k):
                acc[pl.ds(rows[k], 1), :] += grad[pl.ds(toks[k], 1), :]
            quads = (last - first) // UNROLL

            @pl.loop(0, quads)
            def _(i):
                for j in range(UNROLL):
                    add(first + i * UNROLL + j)

            @pl.loop(first + quads * UNROLL, last)
            def _(k):
                add(k)
            ob[slot] = acc[...].astype(BF16)
            store(blk, ob.at[slot]).start()
    for blk in range(n_out - OUT_SLOTS, n_out):
        store(blk, nil).wait()


def table_grad(starts, toks, rows, flags, gain, dy_all, dn_all, picked, vocab_dev):
    smem = pl.BlockSpec(memory_space=pltpu.SMEM)
    dma = pltpu.SemaphoreType.DMA
    return pl.pallas_call(
        table_kernel, out_shape=jax.ShapeDtypeStruct((vocab_dev, 2048), BF16),
        in_specs=[smem] * 4 + [pl.BlockSpec(memory_space=pltpu.VMEM)] + [ANY] * 3, out_specs=ANY,
        scratch_shapes=[pltpu.VMEM((GROUP * TOK, 2048), F32)] + [pltpu.VMEM((IN_SLOTS, IN_BLK, 2048), BF16)] * 3 + [pltpu.VMEM((ROW_BLK, 2048), F32), pltpu.VMEM((OUT_SLOTS, ROW_BLK, 2048), BF16), pltpu.VMEM((ROW_BLK, 2048), BF16), dma((3, IN_SLOTS)), dma((OUT_SLOTS,))],
        compiler_params=pltpu.CompilerParams(vmem_limit_bytes=60 * 1024 * 1024),
        cost_estimate=pl.CostEstimate(flops=10**9, bytes_accessed=80 * 10**6, transcendentals=0), name='table_grad',
    )(starts, toks, rows, flags, gain, dy_all, dn_all, picked)


def small_kernel(src, out, loc_sem, s_sem, r_sem):
    me = lax.axis_index('fsdp')
    meet_all(me)
    own = pltpu.make_async_copy(src, out.at[me], loc_sem)
    own.start()

    def send(step):
        return pltpu.make_async_remote_copy(src, out.at[me], s_sem.at[step], r_sem.at[step],
                                            device_id={'fsdp': (me + step) % GROUP}, device_id_type=MESH)
    for step in range(1, GROUP):
        send(step).start()
    for step in range(1, GROUP):
        send(step).wait()
    own.wait()


def small_gather(tile):
    dma = pltpu.SemaphoreType.DMA
    return pl.pallas_call(
        small_kernel, out_shape=jax.ShapeDtypeStruct((GROUP, 8, 128), F32),
        in_specs=[pl.BlockSpec(memory_space=pltpu.VMEM)], out_specs=pl.BlockSpec(memory_space=pltpu.VMEM),
        scratch_shapes=[dma, dma((GROUP,)), dma((GROUP,))],
        compiler_params=pltpu.CompilerParams(collective_id=0, has_side_effects=True),
        cost_estimate=pl.CostEstimate(flops=10**7, bytes_accessed=10**5, transcendentals=0), name='small_gather',
    )(tile)


def blank(shape, dtype):
    return pl.pallas_call(lambda out: None, out_shape=jax.ShapeDtypeStruct(shape, dtype), out_specs=ANY, name='blank')()


def block_step(rows_f32, grad_rows, full_weights, seq_count):
    gain_vec, w_query, w_kv_down, kv_gain, w_kv_up, w_out = full_weights
    kv_rank = kv_gain.shape[0]
    tok_count = rows_f32.shape[0]
    seq_len = tok_count // seq_count
    normed, norm_pull = jax.vjp(rms_scale, rows_f32, gain_vec)
    q_proj = jnp.dot(normed, w_query, preferred_element_type=jnp.float32).astype(jnp.bfloat16)
    kv_down = jnp.dot(normed, w_kv_down, preferred_element_type=jnp.float32).astype(jnp.bfloat16)
    latent, latent_pull = jax.vjp(rms_scale, kv_down[:, :kv_rank], kv_gain)
    kv_up = jnp.dot(latent, w_kv_up, preferred_element_type=jnp.float32).astype(jnp.bfloat16)
    attn_mix, attn_pull = jax.vjp(attend_local, q_proj.reshape(seq_count, seq_len, -1, NOPE_DIM + ROPE_DIM), kv_down[:, kv_rank:].reshape(seq_count, seq_len, ROPE_DIM), kv_up.reshape(seq_count, seq_len, -1, NOPE_DIM + VALUE_DIM))
    mix_rows = attn_mix.reshape(tok_count, -1)
    d_mix = lax.dot_general(grad_rows[:, :1536], w_out[0], COL_DIMS, preferred_element_type=jnp.float32)
    d_mix = (d_mix + lax.dot_general(grad_rows[:, 1536:], w_out[1], COL_DIMS, preferred_element_type=jnp.float32)).astype(jnp.bfloat16)
    d_query, d_pe, d_up = attn_pull(d_mix.reshape(attn_mix.shape))
    d_query = d_query.reshape(tok_count, -1)
    d_up = d_up.reshape(tok_count, -1)
    d_latent = lax.dot_general(d_up, w_kv_up, COL_DIMS, preferred_element_type=jnp.float32).astype(jnp.bfloat16)
    d_ckv, d_kv_gain = latent_pull(d_latent)
    d_down = jnp.concatenate([d_ckv, d_pe.reshape(tok_count, ROPE_DIM)], axis=1)
    d_normed = lax.dot_general(d_query, w_query, COL_DIMS, preferred_element_type=jnp.float32)
    d_normed = d_normed + lax.dot_general(d_down, w_kv_down, COL_DIMS, preferred_element_type=jnp.float32)
    d_normed = d_normed.astype(jnp.bfloat16)
    _, d_gain = norm_pull(d_normed)
    return d_normed, normed, mix_rows, latent, d_query, d_down, d_up, d_gain, d_kv_gain


def solution(mesh):
    tok_spec = P(('dp', 'fsdp'), None)
    seq_spec = P(('dp', 'fsdp'), None, None)
    part_vec = P(('dp', 'fsdp'))
    vec_spec = P('fsdp')
    mat_spec = P('fsdp', None)

    def device_step(tok_ids, grad_out, emb_table, norm_gain, w_query, w_kv_down, kv_gain, w_kv_up, w_out):
        seq_count, seq_len = tok_ids.shape
        vocab_dev, d_model = emb_table.shape
        tok_count = seq_count * seq_len
        me = lax.axis_index('fsdp')
        grad_rows = grad_out.reshape(tok_count, d_model)
        bundle = lax.all_gather(jnp.concatenate([w_query, w_out[:, :1536]], axis=1), 'fsdp', tiled=True)
        fill = lambda rows: jnp.pad(rows, ((0, 0), (0, 128 - rows.shape[1])))
        tile = jnp.concatenate([fill(tok_ids.astype(F32)), norm_gain.astype(F32).reshape(1, 128), fill(kv_gain.astype(F32).reshape(1, 32)), jnp.zeros((3, 128), F32)], axis=0)
        table = small_gather(tile)
        all_ids = table[:, :seq_count, :seq_len].reshape(GROUP, tok_count).astype(jnp.int32)
        gain_full = table[:, 3, :].reshape(-1)
        kv_gain_full = table[:, 4, :32].reshape(-1)

        owner = all_ids // vocab_dev
        mine = (owner == me)
        local = all_ids - me * vocab_dev
        stamp = jnp.arange(GROUP * tok_count).reshape(GROUP, tok_count) * ROW_BLK
        keys = lax.sort(jnp.where(mine, (local // ROW_BLK) * 2**20 + stamp + local % ROW_BLK, 2**30).reshape(-1))
        starts = jnp.sum((mine & (local < ROW_BLK * jnp.arange(vocab_dev // ROW_BLK + 1)[:, None, None])).astype(jnp.int32), axis=(1, 2))
        flags = jnp.sum(mine.reshape(-1, SUB).astype(jnp.int32), axis=1)
        picked = jnp.take(emb_table, jnp.where(mine, local, 0).reshape(-1), axis=0, mode='clip')
        core = me % 2
        near = lax.dynamic_index_in_dim(owner.reshape(RING, 2, tok_count), core, 1, keepdims=False)
        mask = jnp.stack([near == me, near == me + 1 - 2 * core]).astype(BF16)
        mask = jnp.broadcast_to(mask[..., None], (2, RING, tok_count, 128))
        picked, keys, starts, flags = lax.optimization_barrier((picked, keys, starts, flags))
        tok_rows, full_kvb, full_kva, wo_last = spread(mask, picked.reshape(GROUP, tok_count, d_model), (w_kv_up, w_kv_down, w_out[:, 1536:]))
        full_wq, full_wo = bundle[:, :3072], (bundle[:, 3072:], wo_last)
        tok_rows, grad_rows = lax.optimization_barrier((tok_rows, grad_rows))
        all_dy = lax.all_gather(grad_rows, 'fsdp', tiled=True)
        d_normed, normed, mix, latent, d_query, d_down, d_up, d_gain, d_kv_gain = block_step(
            tok_rows.astype(F32), grad_rows, (gain_full, full_wq, full_kva, kv_gain_full, full_kvb, full_wo), seq_count)
        all_dn = lax.all_gather(d_normed, 'fsdp', tiled=True)
        small = jnp.concatenate([d_gain.reshape(GROUP, 1, 128), jnp.pad(d_kv_gain.reshape(GROUP, 1, 32), ((0, 0), (0, 0), (0, 96))), jnp.zeros((GROUP, 6, 128), F32)], axis=1)
        block_out, g_out, g_query, g_down, g_up, g_small = grad_shards(mix, all_dy, normed.T, jnp.pad(d_down, ((0, 0), (0, D_DOWN - d_down.shape[1]))), d_query, latent.T, d_up, small, tok_rows, bundle, wo_last)
        grad_table = table_grad(starts, (keys >> 7) & 8191, keys & (ROW_BLK - 1), flags, gain_full.reshape(1, -1), all_dy, all_dn, picked, vocab_dev)
        return (block_out.reshape(seq_count, seq_len, d_model), grad_table, g_small[0], g_query, g_down[:, :576], g_small[1, :32], g_up, g_out)

    return jax.shard_map(device_step, mesh=mesh, in_specs=(tok_spec, seq_spec, mat_spec, vec_spec, mat_spec, mat_spec, vec_spec, mat_spec, mat_spec), out_specs=(seq_spec, tok_spec, part_vec, tok_spec, tok_spec, part_vec, tok_spec, tok_spec), check_vma=False)
```

```python
import math
import jax
import jax.numpy as jnp
from jax import lax
from jax.sharding import PartitionSpec as P
from jax.experimental import pallas as pl
from jax.experimental.pallas import tpu as pltpu

NOPE_DIM = 128
ROPE_DIM = 64
VALUE_DIM = 128
ROPE_THETA = 50000.0
RMS_EPS = 1e-6
ATTN_SCALE = (NOPE_DIM + ROPE_DIM) ** -0.5 * (0.1 * math.log(32.0) + 1.0) ** 2
ROW_DIMS = (((0,), (0,)), ((), ()))
COL_DIMS = (((1,), (1,)), ((), ()))


def rms_scale(in_vals, gain_vec):
    vals_f32 = in_vals.astype(jnp.float32)
    inv_rms = lax.rsqrt(jnp.mean(vals_f32 * vals_f32, axis=-1, keepdims=True) + RMS_EPS)
    return (vals_f32 * inv_rms * gain_vec).astype(jnp.bfloat16)


def rope_tables(seq_len):
    positions = jnp.arange(seq_len, dtype=jnp.float32)
    inv_freq = ROPE_THETA ** (-2.0 * jnp.arange(ROPE_DIM // 2, dtype=jnp.float32) / ROPE_DIM)
    rot_angle = positions[:, None] * inv_freq[None, :]
    rot_angle = jnp.concatenate([rot_angle, rot_angle], axis=-1)
    return jnp.cos(rot_angle), jnp.sin(rot_angle)


def apply_rope(in_vals, cos_tab, sin_tab):
    half_dim = ROPE_DIM // 2
    vals_f32 = in_vals.astype(jnp.float32)
    turned = jnp.concatenate([-vals_f32[..., half_dim:], vals_f32[..., :half_dim]], axis=-1)
    return (vals_f32 * cos_tab + turned * sin_tab).astype(jnp.bfloat16)


def attend_local(q_proj, pe_raw, kv_up):
    seq_len = q_proj.shape[1]
    cos_tab, sin_tab = rope_tables(seq_len)
    q_rot = apply_rope(q_proj[..., NOPE_DIM:], cos_tab[:, None, :], sin_tab[:, None, :])
    k_rot = apply_rope(pe_raw, cos_tab, sin_tab)
    scores = jnp.einsum('bshd,bthd->bhst', q_proj[..., :NOPE_DIM], kv_up[..., :NOPE_DIM], preferred_element_type=jnp.float32)
    scores = scores + jnp.einsum('bshd,btd->bhst', q_rot, k_rot, preferred_element_type=jnp.float32)
    positions = jnp.arange(seq_len)
    causal = positions[:, None] >= positions[None, :]
    scores = jnp.where(causal, scores * ATTN_SCALE, -1e30)
    attn_probs = jax.nn.softmax(scores, axis=-1).astype(jnp.bfloat16)
    attn_mix = jnp.einsum('bhst,bthd->bshd', attn_probs, kv_up[..., NOPE_DIM:], preferred_element_type=jnp.float32)
    return attn_mix.astype(jnp.bfloat16)


F32, BF16 = jnp.float32, jnp.bfloat16
MESH = pl.DeviceIdType.MESH
ANY = pl.BlockSpec(memory_space=pl.ANY)
RING = 8
GROUP = 16

def chip_at(pos):
    side = pos // 4
    return (pos + side * (7 - 2 * pos)) * 2 + side

def place():
    me = lax.axis_index('fsdp')
    core = me % 2
    chip = me // 2
    side = chip % 2
    zz = chip // 2
    return me, core, zz + side * (7 - 2 * zz)

def at_pos(pos, core):
    return chip_at(pos % RING) * 2 + core

def meet_all(me):
    barrier = pltpu.get_barrier_semaphore()
    for step in range(1, GROUP):
        pl.semaphore_signal(barrier, inc=1, device_id={'fsdp': (me + step) % GROUP}, device_id_type=MESH)
    pl.semaphore_wait(barrier, GROUP - 1)

TOK = 288
D_OUT, D_CAT, D_UP, D_DOWN = 2048, 3712, 4096, 640
WO_COL = 3072
CUT = 1792
PARTS = (('u', 0, 0, 2304), ('u', 1, 2304, 1792), ('n', 0, 0, 896), ('n', 1, 1792, 1024), ('n', 0, 896, 896), ('n', 1, 2816, 896))
N_PARTS = len(PARTS)
ROWS = {'n': 128, 'u': 32}

def col_tiles(width):
    step = 512
    return [(c, min(step, width - c)) for c in range(0, width, step)]

def grad_kernel(mix_h, dy_h, nrm_h, dd_h, dq_h, lat_h, du_h, sm_h, h0_h, wo_h, wl_h, y_h, go_h, gq_h, gd_h, gu_h, gs_h,
                mix, dy, go, nrm, cat, lat, du, b0, b1, b2, b3, b4, b5, mixf, h0, wo, yv, smr, ssum, loc_sem, xs_sem, xr_sem, s_sem, r_sem, ms_sem, mr_sem, cs_sem, cr_sem, dy_sem, y_sem, out_sem):
    me, core, pos = place()
    partner = me + 1 - 2 * core
    meet_all(me)
    acts = ((lat_h, lat), (du_h, du), (nrm_h, nrm), (dd_h, cat.at[:, :, 0:D_DOWN]), (dq_h, cat.at[:, :, D_DOWN:D_CAT]))
    local, cross = [], []
    for i, (src, dst) in enumerate(acts):
        cp = pltpu.make_async_copy(src, dst.at[core], loc_sem.at[i])
        cp.start()
        local.append(cp)
        rc = pltpu.make_async_remote_copy(src, dst.at[core], xs_sem.at[i], xr_sem.at[i], device_id={'fsdp': partner}, device_id_type=MESH)
        rc.start()
        cross.append(rc)
    own_small = pltpu.make_async_copy(sm_h.at[me], smr.at[0], loc_sem.at[5])
    own_small.start()
    own_mix = pltpu.make_async_copy(mix_h.at[:, pl.ds(pl.multiple_of(me * 128, 128), 128)], mix.at[me], loc_sem.at[6])
    own_mix.start()
    smalls, mixes = [], []
    for i in range(1, GROUP):
        peer = (me + i) % GROUP
        rc = pltpu.make_async_remote_copy(sm_h.at[peer], smr.at[i], ms_sem.at[i], mr_sem.at[i], device_id={'fsdp': peer}, device_id_type=MESH)
        rc.start()
        smalls.append(rc)
    for i, (src, dst) in enumerate(((mix_h, mixf), (h0_h, h0))):
        pltpu.make_async_copy(src, dst, y_sem.at[2 + i]).start()

    def wo_load(t):
        return pltpu.make_async_copy(wo_h.at[:, pl.ds(pl.multiple_of(WO_COL + t * 512, 512), 512)], wo.at[t % 2], y_sem.at[t % 2])

    def wo_last():
        return pltpu.make_async_copy(wl_h, wo.at[1], y_sem.at[1])
    wo_load(0).start()
    bufs = (b0, b1, b2, b3, b4, b5)
    peers = (at_pos(pos + 1, core), at_pos(pos + 7, core))
    left_ops = {'n': (nrm, cat), 'u': (lat, du)}

    def mix_send(i):
        peer = (me + i) % GROUP
        return pltpu.make_async_remote_copy(mix_h.at[:, pl.ds(pl.multiple_of(peer * 128, 128), 128)], mix.at[me], cs_sem.at[i], cr_sem.at[i],
                                            device_id={'fsdp': peer}, device_id_type=MESH)

    def dy_load(blk):
        return pltpu.make_async_copy(dy_h.at[pl.ds(pl.multiple_of(blk * TOK, TOK), TOK), :], dy.at[blk % 2], dy_sem.at[blk % 2])

    def hop(p, step):
        return pltpu.make_async_remote_copy(bufs[p].at[step], bufs[p].at[step + 1], s_sem.at[p, step], r_sem.at[p, step + 1],
                                            device_id={'fsdp': peers[PARTS[p][1]]}, device_id_type=MESH)

    def work(p, step):
        kind, way, c0, width = PARTS[p]
        chip = chip_at((pos + 7 - step + way * (2 * step + 2)) % RING)
        lhs_ref, rhs_ref = left_ops[kind]
        rows = ROWS[kind]
        row = pl.multiple_of((chip * 2 + core) * rows, rows)
        lhs = [lhs_ref[b, pl.ds(row, rows), :] for b in range(2)]
        for c, w in col_tiles(width):
            part = sum(jnp.dot(lhs[b], rhs_ref[b, :, c0 + c:c0 + c + w], preferred_element_type=F32) for b in range(2))
            bufs[p][step, :, c:c + w] = bufs[p][step, :, c:c + w] + part

    for i in range(1, GROUP):
        mix_send(i).start()
    dy_load(0).start()
    go[...] = jnp.zeros_like(go)
    for p in range(N_PARTS):
        bufs[p][0] = jnp.zeros(bufs[p].shape[1:], F32)
    first_use = {0: (0, 1), 2: (2, 3, 4)}

    @pl.loop(0, RING)
    def _(step):
        for p in range(N_PARTS):
            if p in first_use:
                @pl.when(step == 0)
                def _():
                    for i in first_use[p]:
                        local[i].wait()
                        cross[i].wait_recv()

            @pl.when(step > 0)
            def _():
                hop(p, step - 1).wait_recv()
            work(p, step)

            @pl.when(step < RING - 1)
            def _():
                hop(p, step).start()

        @pl.when(step == 0)
        def _():
            own_mix.wait()
            for i in range(1, GROUP):
                mix_send(i).wait()

        @pl.when((step > 0) & (step < 5))
        def _():
            @pl.loop(0, 4)
            def _(j):
                blk = (step - 1) * 4 + j
                dy_load(blk).wait()

                @pl.when(blk < GROUP - 1)
                def _():
                    dy_load(blk + 1).start()
                for c, w in col_tiles(2048):
                    go[:, c:c + w] += lax.dot_general(mix[blk], dy[blk % 2, :, c:c + w], (((0,), (0,)), ((), ())), preferred_element_type=F32)

        @pl.when(step == 5)
        def _():
            for i, (src, dst) in enumerate(((mix_h, mixf), (h0_h, h0))):
                pltpu.make_async_copy(src, dst, y_sem.at[2 + i]).wait()

            @pl.loop(0, 4)
            def _(t):
                @pl.when(t < 3)
                def _():
                    wo_load(t).wait()

                @pl.when(t == 3)
                def _():
                    wo_last().wait()

                @pl.when(t < 2)
                def _():
                    wo_load(t + 1).start()

                @pl.when(t == 2)
                def _():
                    wo_last().start()
                here = pl.ds(pl.multiple_of(t * 512, 512), 512)
                yv[:, here] = (h0[:, here].astype(F32) + jnp.dot(mixf[...], wo[t % 2], preferred_element_type=F32)).astype(BF16)

    last = RING - 1
    outs = []
    cp = pltpu.make_async_copy(go, go_h, out_sem.at[6])
    cp.start()
    outs.append(cp)
    cp = pltpu.make_async_copy(yv, y_h, out_sem.at[9])
    cp.start()
    outs.append(cp)
    targets = (((gu_h.at[:, 0:2304], 0, 2304),), ((gu_h.at[:, 2304:4096], 0, 1792),), ((gd_h, 0, 640), (gq_h.at[:, 0:256], 640, 896)),
               ((gq_h.at[:, 1152:2176], 0, 1024),), ((gq_h.at[:, 256:1152], 0, 896),), ((gq_h.at[:, 2176:3072], 0, 896),))
    for p in range(N_PARTS):
        for n, (dst, c0, c1) in enumerate(targets[p]):
            cp = pltpu.make_async_copy(bufs[p].at[last, :, c0:c1], dst, out_sem.at[p + 6 * n])
            cp.start()
            outs.append(cp)
    own_small.wait()
    for rc in smalls:
        rc.wait()
    ssum[...] = jnp.sum(smr[...], axis=0)
    cp = pltpu.make_async_copy(ssum, gs_h, out_sem.at[7])
    cp.start()
    outs.append(cp)
    for rc in cross:
        rc.wait_send()
    for p in range(N_PARTS):
        @pl.loop(0, last)
        def _(step):
            hop(p, step).wait_send()
    for cp in outs:
        cp.wait()


def grad_shards(mix, dy_all, nrm_t, dd, dq, lat_t, du, small, rows, weights, last_cols):
    shapes = [(ROWS[k], RING, w) for k, _, _, w in PARTS]
    scratch = [pltpu.VMEM((GROUP, TOK, 128), BF16), pltpu.VMEM((2, TOK, 2048), BF16), pltpu.VMEM((128, 2048), F32), pltpu.VMEM((2, 2048, TOK), BF16),
               pltpu.VMEM((2, TOK, D_CAT), BF16), pltpu.VMEM((2, 512, TOK), BF16), pltpu.VMEM((2, TOK, D_UP), BF16)]
    scratch += [pltpu.VMEM((RING, r, w), F32) for r, _, w in shapes]
    scratch += [pltpu.VMEM((TOK, 2048), BF16), pltpu.VMEM((TOK, 2048), BF16), pltpu.VMEM((2, 2048, 512), BF16), pltpu.VMEM((TOK, 2048), BF16)]
    scratch += [pltpu.VMEM((GROUP, 8, 128), F32), pltpu.VMEM((8, 128), F32)]
    dma = pltpu.SemaphoreType.DMA
    scratch += [dma((7,)), dma((5,)), dma((5,)), dma((N_PARTS, RING)), dma((N_PARTS, RING)), dma((GROUP,)), dma((GROUP,)), dma((GROUP,)), dma((GROUP,)), dma((2,)), dma((4,)), dma((10,))]
    return pl.pallas_call(
        grad_kernel,
        out_shape=(jax.ShapeDtypeStruct((TOK, 2048), BF16), jax.ShapeDtypeStruct((128, 2048), F32), jax.ShapeDtypeStruct((128, 3072), F32), jax.ShapeDtypeStruct((128, D_DOWN), F32), jax.ShapeDtypeStruct((32, D_UP), F32), jax.ShapeDtypeStruct((8, 128), F32)),
        in_specs=[ANY] * 11, out_specs=(ANY,) * 6, scratch_shapes=scratch,
        compiler_params=pltpu.CompilerParams(collective_id=1, has_side_effects=True, vmem_limit_bytes=60 * 1024 * 1024),
        cost_estimate=pl.CostEstimate(flops=8 * 10**9, bytes_accessed=20 * 10**6, transcendentals=0), name='grad_shards',
    )(mix, dy_all, nrm_t, dd, dq, lat_t, du, small, rows, weights, last_cols)


W_SHARDS = ((32, 4096), (128, 576), (128, 512))
HALF_TOK = TOK // 2


def spread_kernel(n_w, *refs):
    mask, rows_h = refs[0:2]
    srcs = refs[2:2 + n_w]
    got_h = refs[2 + n_w]
    outs = refs[3 + n_w:3 + 2 * n_w]
    stage = refs[3 + 2 * n_w:3 + 3 * n_w]
    own, mate, way0, way1 = refs[3 + 3 * n_w:7 + 3 * n_w]
    in_sem, own_sem, s_sem, r_sem, ps_sem, pr_sem, os_sem, or_sem, xs_sem, xr_sem, ts_sem, tr_sem, h_in, m_s, m_r, hs_sem, hr_sem, out_sem = refs[7 + 3 * n_w:]
    me, core, pos = place()
    twin = lax.axis_index('dp')
    partner = me + 1 - 2 * core
    barrier = pltpu.get_barrier_semaphore()
    peers = (at_pos(pos + 1, core), at_pos(pos + 7, core))
    for peer in peers + (partner,):
        pl.semaphore_signal(barrier, inc=1, device_id={'fsdp': peer}, device_id_type=MESH)
    pl.semaphore_signal(barrier, inc=1, device_id={'dp': 1 - twin}, device_id_type=MESH)
    pl.semaphore_wait(barrier, 4)
    loads = []
    for i in range(n_w):
        cp = pltpu.make_async_copy(srcs[i], stage[i], in_sem.at[i])
        cp.start()
        loads.append(cp)

    def row_load(q):
        return pltpu.make_async_copy(rows_h.at[at_pos(q, core)], own.at[q], h_in.at[q])

    def row_share(q):
        return pltpu.make_async_remote_copy(rows_h.at[at_pos(q, 1 - core)], mate.at[q], m_s.at[q], m_r.at[q],
                                            device_id={'fsdp': partner}, device_id_type=MESH)
    for j in (7, 1, 6, 2, 5, 3, 4, 0):
        row_share((pos + j) % RING).start()
        row_load((pos + j) % RING).start()

    def where(i, way, source, side):
        rows = W_SHARDS[i][0]
        part = rows // 4
        return outs[i].at[pl.ds(pl.multiple_of(source * rows + side * 2 * part + way * part, part), part), :]

    def whole(i):
        rows = W_SHARDS[i][0]
        return outs[i].at[pl.ds(pl.multiple_of(me * rows, rows), rows), :]

    def origin(way, step):
        return at_pos(pos + 8 - step + way * 2 * step, core)

    def hop(i, way, step, src=None):
        spot = where(i, way, origin(way, step), twin)
        return pltpu.make_async_remote_copy(spot if src is None else src, spot, s_sem.at[i, way, step], r_sem.at[i, way, step + 1],
                                            device_id={'fsdp': peers[way]}, device_id_type=MESH)

    def arrive(i, way, step):
        spot = where(i, way, origin(way, step), twin)
        return pltpu.make_async_remote_copy(spot, spot, s_sem.at[i, way, step], r_sem.at[i, way, step],
                                            device_id={'fsdp': peers[way]}, device_id_type=MESH)

    def share(i, way, step):
        spot = where(i, way, origin(way, step), twin)
        return pltpu.make_async_remote_copy(spot, spot, ps_sem.at[i, way, step], pr_sem.at[i, way, step],
                                            device_id={'fsdp': partner}, device_id_type=MESH)

    def share_own(i):
        return pltpu.make_async_remote_copy(stage[i], whole(i), os_sem.at[i], or_sem.at[i], device_id={'fsdp': partner}, device_id_type=MESH)

    def to_twin(i, way, step):
        spot = where(i, way, origin(way, step), twin)
        return pltpu.make_async_remote_copy(spot, spot, xs_sem.at[i, way, step], xr_sem.at[i, way, step],
                                            device_id={'dp': 1 - twin}, device_id_type=MESH)

    def share_twin(i, way, step):
        spot = where(i, way, origin(way, step), 1 - twin)
        return pltpu.make_async_remote_copy(spot, spot, ts_sem.at[i, way, step], tr_sem.at[i, way, step],
                                            device_id={'fsdp': partner}, device_id_type=MESH)
    ways = (way0, way1)

    def row_hop(way, step):
        return pltpu.make_async_remote_copy(ways[way].at[step], ways[way].at[step + 1], hs_sem.at[way, step], hr_sem.at[way, step + 1],
                                            device_id={'fsdp': peers[way]}, device_id_type=MESH)

    def fill(way, step, first):
        q = (pos + 7 - step + way * (2 * step + 2)) % RING
        chip = chip_at(q)
        for c in range(0, HALF_TOK, 48):
            lo = way * HALF_TOK + c
            mine, theirs = mask[0, chip, lo:lo + 48, :], mask[1, chip, lo:lo + 48, :]
            for w in range(0, 2048, 128):
                part = own[q, lo:lo + 48, w:w + 128] * mine + mate[q, lo:lo + 48, w:w + 128] * theirs
                if not first:
                    part = part + ways[way][step, c:c + 48, w:w + 128]
                ways[way][step, c:c + 48, w:w + 128] = part

    kept = []
    for i in range(n_w):
        loads[i].wait()
        part = W_SHARDS[i][0] // 4
        for way in range(2):
            hop(i, way, 0, stage[i].at[pl.ds(pl.multiple_of(twin * 2 * part + way * part, part), part), :]).start()
        share_own(i).start()
        cp = pltpu.make_async_copy(stage[i], whole(i), own_sem.at[i])
        cp.start()
        kept.append(cp)
    for j in (7, 1, 6, 2, 5, 3, 4, 0):
        row_load((pos + j) % RING).wait()
        row_share((pos + j) % RING).wait_recv()
        if j in (7, 1):
            way = 0 if j == 7 else 1
            fill(way, 0, True)
            row_hop(way, 0).start()

    @pl.loop(1, RING)
    def _(step):
        for i in range(n_w):
            for way in range(2):
                arrive(i, way, step).wait_recv()

                @pl.when(step < RING - 1)
                def _():
                    hop(i, way, step).start()
                share(i, way, step).start()
                to_twin(i, way, step).start()
        for way in range(2):
            row_hop(way, step - 1).wait_recv()
            fill(way, step, False)

            @pl.when(step < RING - 1)
            def _():
                row_hop(way, step).start()

        @pl.when(step > 1)
        def _():
            for i in range(n_w):
                for way in range(2):
                    to_twin(i, way, step - 1).wait_recv()
                    share_twin(i, way, step - 1).start()

    for i in range(n_w):
        for way in range(2):
            to_twin(i, way, RING - 1).wait_recv()
            share_twin(i, way, RING - 1).start()
    for way in range(2):
        cp = pltpu.make_async_copy(ways[way].at[RING - 1], got_h.at[way * HALF_TOK:(way + 1) * HALF_TOK, :], out_sem.at[way])
        cp.start()
        kept.append(cp)
    for cp in kept:
        cp.wait()

    @pl.loop(0, RING)
    def _(step):
        row_share(step).wait_send()

        @pl.when(step < RING - 1)
        def _():
            for way in range(2):
                row_hop(way, step).wait_send()
        for i in range(n_w):
            for way in range(2):
                @pl.when(step < RING - 1)
                def _():
                    hop(i, way, step).wait_send()

                @pl.when(step > 0)
                def _():
                    share(i, way, step).wait()
                    to_twin(i, way, step).wait_send()
                    share_twin(i, way, step).wait()
    for i in range(n_w):
        share_own(i).wait()


def spread(mask, rows, shards):
    dma = pltpu.SemaphoreType.DMA
    n_w = len(shards)
    return pl.pallas_call(
        lambda *refs: spread_kernel(n_w, *refs),
        out_shape=(jax.ShapeDtypeStruct((TOK, 2048), BF16),) + tuple(jax.ShapeDtypeStruct((GROUP * r, w), BF16) for r, w in W_SHARDS),
        in_specs=[pl.BlockSpec(memory_space=pltpu.VMEM)] + [ANY] * (n_w + 1), out_specs=(ANY,) * (n_w + 1),
        scratch_shapes=[pltpu.VMEM(s, BF16) for s in W_SHARDS] + [pltpu.VMEM((RING, TOK, 2048), BF16)] * 2 + [pltpu.VMEM((RING, HALF_TOK, 2048), BF16)] * 2
        + [dma((n_w,)), dma((n_w,))] + [dma((n_w, 2, RING))] * 4 + [dma((n_w,))] * 2 + [dma((n_w, 2, RING))] * 4 + [dma((RING,)) for _ in range(3)] + [dma((2, RING)) for _ in range(2)] + [dma((2,))],
        compiler_params=pltpu.CompilerParams(collective_id=2, has_side_effects=True, vmem_limit_bytes=60 * 1024 * 1024),
        cost_estimate=pl.CostEstimate(flops=8 * 10**9, bytes_accessed=27 * 10**6, transcendentals=0), name='spread',
    )(mask, rows, *shards)
ROW_BLK = 128
IN_BLK = 144
SUB = 48
PIECE = 16
UNROLL = 4
IN_SLOTS = 4
OUT_SLOTS = 4


def table_kernel(starts, toks, rows, flags, gain, small, dy_h, dn_h, h_h, *refs):
    passed, out_h, given, gain_out, kv_out = refs[0:5], refs[5], refs[6:11], refs[11], refs[12]
    grad, dy, dn, hh, acc, ob, nil, in_sem, out_sem = refs[13:22]
    hold, cut, ride_in, ride_out = refs[22:27], refs[27], refs[28], refs[29]
    boards = [pltpu.make_async_copy(src, dst, ride_in.at[i]) for i, (src, dst) in enumerate(zip(passed, hold))]
    leaves = [pltpu.make_async_copy(cut if i == 2 else src, dst, ride_out.at[i]) for i, (src, dst) in enumerate(zip(hold, given))]
    for cp in boards:
        cp.start()
    gain_out[...] = small[0:1, :]
    kv_out[...] = small[1:2, 0:32]
    n_in = GROUP * TOK // IN_BLK
    n_out = out_h.shape[0] // ROW_BLK

    def loads(blk):
        span = pl.ds(pl.multiple_of(blk * IN_BLK, IN_BLK), IN_BLK)
        slot = blk % IN_SLOTS
        return [pltpu.make_async_copy(src.at[span, :], dst.at[slot], in_sem.at[i, slot]) for i, (src, dst) in enumerate(((dy_h, dy), (dn_h, dn), (h_h, hh)))]
    for blk in range(IN_SLOTS - 1):
        for cp in loads(blk):
            cp.start()

    @pl.loop(0, n_in)
    def _(blk):
        slot = blk % IN_SLOTS
        for cp in loads(blk):
            cp.wait()

        @pl.when(blk < n_in - IN_SLOTS + 1)
        def _():
            for cp in loads(blk + IN_SLOTS - 1):
                cp.start()

        @pl.loop(0, IN_BLK // SUB)
        def _(g):
            @pl.when(flags[blk * (IN_BLK // SUB) + g] > 0)
            def _():
                r0 = pl.multiple_of(g * SUB, PIECE)
                o0 = pl.multiple_of(blk * IN_BLK + g * SUB, PIECE)
                pieces = range(0, SUB, PIECE)

                def tile(ref, p, c):
                    return ref[slot, pl.ds(r0 + p, PIECE), c:c + 128].astype(F32)
                scale = []
                for p in pieces:
                    sq = jnp.zeros((PIECE, 128), F32)
                    al = jnp.zeros((PIECE, 128), F32)
                    for c in range(0, 2048, 128):
                        h = tile(hh, p, c)
                        sq = sq + h * h
                        al = al + h * (tile(dn, p, c) * gain[:, c:c + 128])
                    scale.append((jnp.sum(sq, axis=1, keepdims=True), jnp.sum(al, axis=1, keepdims=True)))
                for p, (sq, al) in zip(pieces, scale):
                    inv = lax.rsqrt(sq * (1.0 / 2048) + RMS_EPS)
                    coef = inv * inv * inv * (al * (1.0 / 2048))
                    for c in range(0, 2048, 128):
                        s = tile(dn, p, c) * gain[:, c:c + 128]
                        grad[pl.ds(o0 + p, PIECE), c:c + 128] = tile(dy, p, c) + inv * s - coef * tile(hh, p, c)

    for cp in boards:
        cp.wait()
    cut[...] = hold[2][...].T[0:576, :]
    for cp in leaves:
        cp.start()

    def store(blk, src):
        return pltpu.make_async_copy(src, out_h.at[pl.ds(pl.multiple_of(blk * ROW_BLK, ROW_BLK), ROW_BLK), :], out_sem.at[blk % OUT_SLOTS])
    nil[...] = jnp.zeros_like(nil)

    @pl.loop(0, n_out)
    def _(blk):
        first, last = starts[blk], starts[blk + 1]
        slot = blk % OUT_SLOTS

        @pl.when(blk >= OUT_SLOTS)
        def _():
            store(blk - OUT_SLOTS, nil).wait()

        @pl.when(first == last)
        def _():
            store(blk, nil).start()

        @pl.when(first < last)
        def _():
            acc[...] = jnp.zeros_like(acc)

            def add(k):
                acc[pl.ds(rows[k], 1), :] += grad[pl.ds(toks[k], 1), :]
            quads = (last - first) // UNROLL

            @pl.loop(0, quads)
            def _(i):
                for j in range(UNROLL):
                    add(first + i * UNROLL + j)

            @pl.loop(first + quads * UNROLL, last)
            def _(k):
                add(k)
            ob[slot] = acc[...].astype(BF16)
            store(blk, ob.at[slot]).start()
    for blk in range(n_out - OUT_SLOTS, n_out):
        store(blk, nil).wait()
    for cp in leaves:
        cp.wait()


def table_grad(starts, toks, rows, flags, gain, small, dy_all, dn_all, picked, vocab_dev, passed):
    smem = pl.BlockSpec(memory_space=pltpu.SMEM)
    vmem = pl.BlockSpec(memory_space=pltpu.VMEM)
    dma = pltpu.SemaphoreType.DMA
    shapes = [jax.ShapeDtypeStruct((vocab_dev, 2048), BF16)] + [jax.ShapeDtypeStruct((576, 128) if i == 2 else p.shape, p.dtype) for i, p in enumerate(passed)]
    shapes += [jax.ShapeDtypeStruct((1, 128), F32), jax.ShapeDtypeStruct((1, 32), F32)]
    return pl.pallas_call(
        table_kernel, out_shape=tuple(shapes),
        in_specs=[smem] * 4 + [vmem] * 2 + [ANY] * 8, out_specs=(ANY,) * 6 + (vmem,) * 2,
        scratch_shapes=[pltpu.VMEM((GROUP * TOK, 2048), F32)] + [pltpu.VMEM((IN_SLOTS, IN_BLK, 2048), BF16)] * 3
        + [pltpu.VMEM((ROW_BLK, 2048), F32), pltpu.VMEM((OUT_SLOTS, ROW_BLK, 2048), BF16), pltpu.VMEM((ROW_BLK, 2048), BF16), dma((3, IN_SLOTS)), dma((OUT_SLOTS,))]
        + [pltpu.VMEM(p.shape, p.dtype) for p in passed] + [pltpu.VMEM((576, 128), F32), dma((5,)), dma((5,))],
        compiler_params=pltpu.CompilerParams(vmem_limit_bytes=63 * 1024 * 1024),
        cost_estimate=pl.CostEstimate(flops=10**9, bytes_accessed=90 * 10**6, transcendentals=0), name='table_grad',
    )(starts, toks, rows, flags, gain, small, dy_all, dn_all, picked, *passed)


def small_kernel(src, out, loc_sem, s_sem, r_sem):
    me = lax.axis_index('fsdp')
    meet_all(me)
    own = pltpu.make_async_copy(src, out.at[me], loc_sem)
    own.start()

    def send(step):
        return pltpu.make_async_remote_copy(src, out.at[me], s_sem.at[step], r_sem.at[step],
                                            device_id={'fsdp': (me + step) % GROUP}, device_id_type=MESH)
    for step in range(1, GROUP):
        send(step).start()
    for step in range(1, GROUP):
        send(step).wait()
    own.wait()


def small_gather(tile):
    dma = pltpu.SemaphoreType.DMA
    return pl.pallas_call(
        small_kernel, out_shape=jax.ShapeDtypeStruct((GROUP, 8, 128), F32),
        in_specs=[pl.BlockSpec(memory_space=pltpu.VMEM)], out_specs=pl.BlockSpec(memory_space=pltpu.VMEM),
        scratch_shapes=[dma, dma((GROUP,)), dma((GROUP,))],
        compiler_params=pltpu.CompilerParams(collective_id=0, has_side_effects=True),
        cost_estimate=pl.CostEstimate(flops=10**7, bytes_accessed=10**5, transcendentals=0), name='small_gather',
    )(tile)


def blank(shape, dtype):
    return pl.pallas_call(lambda out: None, out_shape=jax.ShapeDtypeStruct(shape, dtype), out_specs=ANY, name='blank')()


def block_step(rows_f32, grad_rows, full_weights, seq_count):
    gain_vec, w_query, w_kv_down, kv_gain, w_kv_up, w_out = full_weights
    kv_rank = kv_gain.shape[0]
    tok_count = rows_f32.shape[0]
    seq_len = tok_count // seq_count
    normed, norm_pull = jax.vjp(rms_scale, rows_f32, gain_vec)
    q_proj = jnp.dot(normed, w_query, preferred_element_type=jnp.float32).astype(jnp.bfloat16)
    kv_down = jnp.dot(normed, w_kv_down, preferred_element_type=jnp.float32).astype(jnp.bfloat16)
    latent, latent_pull = jax.vjp(rms_scale, kv_down[:, :kv_rank], kv_gain)
    kv_up = jnp.dot(latent, w_kv_up, preferred_element_type=jnp.float32).astype(jnp.bfloat16)
    attn_mix, attn_pull = jax.vjp(attend_local, q_proj.reshape(seq_count, seq_len, -1, NOPE_DIM + ROPE_DIM), kv_down[:, kv_rank:].reshape(seq_count, seq_len, ROPE_DIM), kv_up.reshape(seq_count, seq_len, -1, NOPE_DIM + VALUE_DIM))
    mix_rows = attn_mix.reshape(tok_count, -1)
    d_mix = lax.dot_general(grad_rows[:, :1536], w_out[0], COL_DIMS, preferred_element_type=jnp.float32)
    d_mix = (d_mix + lax.dot_general(grad_rows[:, 1536:], w_out[1], COL_DIMS, preferred_element_type=jnp.float32)).astype(jnp.bfloat16)
    d_query, d_pe, d_up = attn_pull(d_mix.reshape(attn_mix.shape))
    d_query = d_query.reshape(tok_count, -1)
    d_up = d_up.reshape(tok_count, -1)
    d_latent = lax.dot_general(d_up, w_kv_up, COL_DIMS, preferred_element_type=jnp.float32).astype(jnp.bfloat16)
    d_ckv, d_kv_gain = latent_pull(d_latent)
    d_down = jnp.concatenate([d_ckv, d_pe.reshape(tok_count, ROPE_DIM)], axis=1)
    d_normed = lax.dot_general(d_query, w_query, COL_DIMS, preferred_element_type=jnp.float32)
    d_normed = d_normed + lax.dot_general(d_down, w_kv_down, COL_DIMS, preferred_element_type=jnp.float32)
    d_normed = d_normed.astype(jnp.bfloat16)
    _, d_gain = norm_pull(d_normed)
    return d_normed, normed, mix_rows, latent, d_query, d_down, d_up, d_gain, d_kv_gain


def solution(mesh):
    tok_spec = P(('dp', 'fsdp'), None)
    seq_spec = P(('dp', 'fsdp'), None, None)
    part_vec = P(('dp', 'fsdp'))
    vec_spec = P('fsdp')
    mat_spec = P('fsdp', None)

    def device_step(tok_ids, grad_out, emb_table, norm_gain, w_query, w_kv_down, kv_gain, w_kv_up, w_out):
        seq_count, seq_len = tok_ids.shape
        vocab_dev, d_model = emb_table.shape
        tok_count = seq_count * seq_len
        me = lax.axis_index('fsdp')
        grad_rows = grad_out.reshape(tok_count, d_model)
        bundle = lax.all_gather(jnp.concatenate([w_query, w_out[:, :1536]], axis=1), 'fsdp', tiled=True)
        fill = lambda rows: jnp.pad(rows, ((0, 0), (0, 128 - rows.shape[1])))
        tile = jnp.concatenate([fill(tok_ids.astype(F32)), norm_gain.astype(F32).reshape(1, 128), fill(kv_gain.astype(F32).reshape(1, 32)), jnp.zeros((3, 128), F32)], axis=0)
        table = small_gather(tile)
        all_ids = table[:, :seq_count, :seq_len].reshape(GROUP, tok_count).astype(jnp.int32)
        gain_full = table[:, 3, :].reshape(-1)
        kv_gain_full = table[:, 4, :32].reshape(-1)

        owner = all_ids // vocab_dev
        mine = (owner == me)
        local = all_ids - me * vocab_dev
        stamp = jnp.arange(GROUP * tok_count).reshape(GROUP, tok_count) * ROW_BLK
        keys = lax.sort(jnp.where(mine, (local // ROW_BLK) * 2**20 + stamp + local % ROW_BLK, 2**30).reshape(-1))
        starts = jnp.sum((mine & (local < ROW_BLK * jnp.arange(vocab_dev // ROW_BLK + 1)[:, None, None])).astype(jnp.int32), axis=(1, 2))
        flags = jnp.sum(mine.reshape(-1, SUB).astype(jnp.int32), axis=1)
        picked = jnp.take(emb_table, jnp.where(mine, local, 0).reshape(-1), axis=0, mode='clip')
        core = me % 2
        near = lax.dynamic_index_in_dim(owner.reshape(RING, 2, tok_count), core, 1, keepdims=False)
        mask = jnp.stack([near == me, near == me + 1 - 2 * core]).astype(BF16)
        mask = jnp.broadcast_to(mask[..., None], (2, RING, tok_count, 128))
        picked, keys, starts, flags, w_kv_down = lax.optimization_barrier((picked, keys, starts, flags, w_kv_down))
        tok_rows, full_kvb, full_kva, wo_last = spread(mask, picked.reshape(GROUP, tok_count, d_model), (w_kv_up, w_kv_down, w_out[:, 1536:]))
        full_wq, full_wo = bundle[:, :3072], (bundle[:, 3072:], wo_last)
        tok_rows, grad_rows = lax.optimization_barrier((tok_rows, grad_rows))
        all_dy = lax.all_gather(grad_rows, 'fsdp', tiled=True)
        d_normed, normed, mix, latent, d_query, d_down, d_up, d_gain, d_kv_gain = block_step(
            tok_rows.astype(F32), grad_rows, (gain_full, full_wq, full_kva, kv_gain_full, full_kvb, full_wo), seq_count)
        all_dn = lax.all_gather(d_normed, 'fsdp', tiled=True)
        small = jnp.concatenate([d_gain.reshape(GROUP, 1, 128), jnp.pad(d_kv_gain.reshape(GROUP, 1, 32), ((0, 0), (0, 0), (0, 96))), jnp.zeros((GROUP, 6, 128), F32)], axis=1)
        block_out, g_out, g_query, g_down, g_up, g_small = grad_shards(mix, all_dy, normed.T, jnp.pad(d_down, ((0, 0), (0, D_DOWN - d_down.shape[1]))), d_query, latent.T, d_up, small, tok_rows, bundle, wo_last)
        grad_table, block_out, g_query, g_down, g_up, g_out, g_gain, g_kv_gain = table_grad(
            starts, (keys >> 7) & 8191, keys & (ROW_BLK - 1), flags, gain_full.reshape(1, -1), g_small, all_dy, all_dn, picked, vocab_dev,
            (block_out, g_query, g_down, g_up, g_out))
        return (block_out.reshape(seq_count, seq_len, d_model), grad_table, g_gain.reshape(-1), g_query, g_down.T, g_kv_gain.reshape(-1), g_up, g_out)

    return jax.shard_map(device_step, mesh=mesh, in_specs=(tok_spec, seq_spec, mat_spec, vec_spec, mat_spec, mat_spec, vec_spec, mat_spec, mat_spec), out_specs=(seq_spec, tok_spec, part_vec, tok_spec, tok_spec, part_vec, tok_spec, tok_spec), check_vma=False)
```

```python
import math
import jax
import jax.numpy as jnp
from jax import lax
from jax.sharding import PartitionSpec as P
from jax.experimental import pallas as pl
from jax.experimental.pallas import tpu as pltpu

NOPE_DIM = 128
ROPE_DIM = 64
VALUE_DIM = 128
ROPE_THETA = 50000.0
RMS_EPS = 1e-6
ATTN_SCALE = (NOPE_DIM + ROPE_DIM) ** -0.5 * (0.1 * math.log(32.0) + 1.0) ** 2
ROW_DIMS = (((0,), (0,)), ((), ()))
COL_DIMS = (((1,), (1,)), ((), ()))


def rms_scale(in_vals, gain_vec):
    vals_f32 = in_vals.astype(jnp.float32)
    inv_rms = lax.rsqrt(jnp.mean(vals_f32 * vals_f32, axis=-1, keepdims=True) + RMS_EPS)
    return (vals_f32 * inv_rms * gain_vec).astype(jnp.bfloat16)


def rope_tables(seq_len):
    positions = jnp.arange(seq_len, dtype=jnp.float32)
    inv_freq = ROPE_THETA ** (-2.0 * jnp.arange(ROPE_DIM // 2, dtype=jnp.float32) / ROPE_DIM)
    rot_angle = positions[:, None] * inv_freq[None, :]
    rot_angle = jnp.concatenate([rot_angle, rot_angle], axis=-1)
    return jnp.cos(rot_angle), jnp.sin(rot_angle)


def apply_rope(in_vals, cos_tab, sin_tab):
    half_dim = ROPE_DIM // 2
    vals_f32 = in_vals.astype(jnp.float32)
    turned = jnp.concatenate([-vals_f32[..., half_dim:], vals_f32[..., :half_dim]], axis=-1)
    return (vals_f32 * cos_tab + turned * sin_tab).astype(jnp.bfloat16)


def attend_local(q_proj, pe_raw, kv_up):
    seq_len = q_proj.shape[1]
    cos_tab, sin_tab = rope_tables(seq_len)
    q_rot = apply_rope(q_proj[..., NOPE_DIM:], cos_tab[:, None, :], sin_tab[:, None, :])
    k_rot = apply_rope(pe_raw, cos_tab, sin_tab)
    scores = jnp.einsum('bshd,bthd->bhst', q_proj[..., :NOPE_DIM], kv_up[..., :NOPE_DIM], preferred_element_type=jnp.float32)
    scores = scores + jnp.einsum('bshd,btd->bhst', q_rot, k_rot, preferred_element_type=jnp.float32)
    positions = jnp.arange(seq_len)
    causal = positions[:, None] >= positions[None, :]
    scores = jnp.where(causal, scores * ATTN_SCALE, -1e30)
    attn_probs = jax.nn.softmax(scores, axis=-1).astype(jnp.bfloat16)
    attn_mix = jnp.einsum('bhst,bthd->bshd', attn_probs, kv_up[..., NOPE_DIM:], preferred_element_type=jnp.float32)
    return attn_mix.astype(jnp.bfloat16)


F32, BF16 = jnp.float32, jnp.bfloat16
MESH = pl.DeviceIdType.MESH
ANY = pl.BlockSpec(memory_space=pl.ANY)
RING = 8
GROUP = 16

def chip_at(pos):
    side = pos // 4
    return (pos + side * (7 - 2 * pos)) * 2 + side

def place():
    me = lax.axis_index('fsdp')
    core = me % 2
    chip = me // 2
    side = chip % 2
    zz = chip // 2
    return me, core, zz + side * (7 - 2 * zz)

def at_pos(pos, core):
    return chip_at(pos % RING) * 2 + core

def meet_all(me):
    barrier = pltpu.get_barrier_semaphore()
    for step in range(1, GROUP):
        pl.semaphore_signal(barrier, inc=1, device_id={'fsdp': (me + step) % GROUP}, device_id_type=MESH)
    pl.semaphore_wait(barrier, GROUP - 1)

TOK = 288
IN_BLK = 144
PIECE = 16
D_OUT, D_CAT, D_UP, D_DOWN = 2048, 3712, 4096, 640
WO_COL = 3072
CUT = 1792
PARTS = (('u', 0, 0, 2304), ('u', 1, 2304, 1792), ('n', 0, 0, 896), ('n', 1, 1792, 1024), ('n', 0, 896, 896), ('n', 1, 2816, 896))
N_PARTS = len(PARTS)
ROWS = {'n': 128, 'u': 32}

def col_tiles(width):
    step = 512
    return [(c, min(step, width - c)) for c in range(0, width, step)]

def grad_kernel(mix_h, dy_h, nrm_h, dd_h, dq_h, lat_h, du_h, sm_h, h0_h, wo_h, wl_h, dn_h, h_h, gain, y_h, dn_all, grad_h, go_h, gq_h, gd_h, gu_h, gs_h,
                mix, dy, go, nrm, cat, lat, du, b0, b1, b2, b3, b4, b5, mixf, h0, wo, yv, own_dn, fdn, fdy, fh, fo, smr, ssum, loc_sem, xs_sem, xr_sem, s_sem, r_sem, ms_sem, mr_sem, cs_sem, cr_sem, dy_sem, y_sem, ns_sem, nr_sem, np_sem, nq_sem, f_sem, fo_sem, out_sem):
    me, core, pos = place()
    partner = me + 1 - 2 * core
    meet_all(me)
    acts = ((lat_h, lat), (du_h, du), (nrm_h, nrm), (dd_h, cat.at[:, :, 0:D_DOWN]), (dq_h, cat.at[:, :, D_DOWN:D_CAT]))
    local, cross = [], []
    for i, (src, dst) in enumerate(acts):
        cp = pltpu.make_async_copy(src, dst.at[core], loc_sem.at[i])
        cp.start()
        local.append(cp)
        rc = pltpu.make_async_remote_copy(src, dst.at[core], xs_sem.at[i], xr_sem.at[i], device_id={'fsdp': partner}, device_id_type=MESH)
        rc.start()
        cross.append(rc)
    peers = (at_pos(pos + 1, core), at_pos(pos + 7, core))

    def unit(dev, way):
        return pl.ds(pl.multiple_of(dev * TOK + way * IN_BLK, PIECE), IN_BLK)

    def origin(way, step):
        return at_pos(pos + 8 - step + way * 2 * step, core)

    def dn_hop(way, step, src=None):
        spot = dn_all.at[unit(origin(way, step), way), :]
        return pltpu.make_async_remote_copy(spot if src is None else src, spot, ns_sem.at[way, step], nr_sem.at[way, step + 1],
                                            device_id={'fsdp': peers[way]}, device_id_type=MESH)

    def dn_arrive(way, step):
        spot = dn_all.at[unit(origin(way, step), way), :]
        return pltpu.make_async_remote_copy(spot, spot, ns_sem.at[way, step], nr_sem.at[way, step],
                                            device_id={'fsdp': peers[way]}, device_id_type=MESH)

    def dn_share(way, step, src=None):
        spot = dn_all.at[unit(origin(way, step), way), :]
        return pltpu.make_async_remote_copy(spot if src is None else src, spot, np_sem.at[way, step], nq_sem.at[way, step],
                                            device_id={'fsdp': partner}, device_id_type=MESH)
    own_load = pltpu.make_async_copy(dn_h, own_dn, f_sem.at[0, 0])
    own_load.start()
    own_load.wait()
    for way in range(2):
        src = own_dn.at[way * IN_BLK:(way + 1) * IN_BLK, :]
        dn_hop(way, 0, src).start()
        dn_share(way, 0, src).start()
        pltpu.make_async_copy(src, dn_all.at[unit(me, way), :], fo_sem.at[way]).start()

    def row_grads(step):
        jobs = [(at_pos(pos + 8 - step + way * 2 * step, c), way) for way in range(2) for c in (core, 1 - core)]

        def fetch(slot):
            dev, way = jobs[slot]
            return [pltpu.make_async_copy(src.at[unit(dev, way), :], dst.at[slot], f_sem.at[i, slot])
                    for i, (src, dst) in enumerate(((dn_all, fdn), (dy_h, fdy), (h_h, fh)))]

        def put(slot):
            dev, way = jobs[slot]
            return pltpu.make_async_copy(fo.at[slot % 2], grad_h.at[unit(dev, way), :], fo_sem.at[slot % 2])
        for way in range(2):
            dn_share(way, step).wait_recv()
        for slot in range(4):
            for cp in fetch(slot):
                cp.start()

        for slot in range(4):
            for cp in fetch(slot):
                cp.wait()
            if slot >= 2:
                put(slot - 2).wait()

            @pl.loop(0, IN_BLK // 48)
            def _(g):
                r0 = pl.multiple_of(g * 48, PIECE)

                def tile(ref, p, c):
                    return ref[slot, pl.ds(r0 + p, PIECE), c:c + 128].astype(F32)
                scale = []
                for p in range(0, 48, PIECE):
                    sq = jnp.zeros((PIECE, 128), F32)
                    al = jnp.zeros((PIECE, 128), F32)
                    for c in range(0, 2048, 128):
                        h = tile(fh, p, c)
                        sq = sq + h * h
                        al = al + h * (tile(fdn, p, c) * gain[:, c:c + 128])
                    scale.append((jnp.sum(sq, axis=1, keepdims=True), jnp.sum(al, axis=1, keepdims=True)))
                for p, (sq, al) in zip(range(0, 48, PIECE), scale):
                    inv = lax.rsqrt(sq * (1.0 / 2048) + RMS_EPS)
                    coef = inv * inv * inv * (al * (1.0 / 2048))
                    for c in range(0, 2048, 128):
                        s = tile(fdn, p, c) * gain[:, c:c + 128]
                        fo[slot % 2, pl.ds(r0 + p, PIECE), c:c + 128] = tile(fdy, p, c) + inv * s - coef * tile(fh, p, c)
            put(slot).start()
        put(2).wait()
        put(3).wait()

    own_small = pltpu.make_async_copy(sm_h.at[me], smr.at[0], loc_sem.at[5])
    own_small.start()
    own_mix = pltpu.make_async_copy(mix_h.at[:, pl.ds(pl.multiple_of(me * 128, 128), 128)], mix.at[me], loc_sem.at[6])
    own_mix.start()
    smalls, mixes = [], []
    for i in range(1, GROUP):
        peer = (me + i) % GROUP
        rc = pltpu.make_async_remote_copy(sm_h.at[peer], smr.at[i], ms_sem.at[i], mr_sem.at[i], device_id={'fsdp': peer}, device_id_type=MESH)
        rc.start()
        smalls.append(rc)
    for i, (src, dst) in enumerate(((mix_h, mixf), (h0_h, h0))):
        pltpu.make_async_copy(src, dst, y_sem.at[2 + i]).start()

    def wo_load(t):
        return pltpu.make_async_copy(wo_h.at[:, pl.ds(pl.multiple_of(WO_COL + t * 512, 512), 512)], wo.at[t % 2], y_sem.at[t % 2])

    def wo_last():
        return pltpu.make_async_copy(wl_h, wo.at[1], y_sem.at[1])
    wo_load(0).start()
    bufs = (b0, b1, b2, b3, b4, b5)
    left_ops = {'n': (nrm, cat), 'u': (lat, du)}

    def mix_send(i):
        peer = (me + i) % GROUP
        return pltpu.make_async_remote_copy(mix_h.at[:, pl.ds(pl.multiple_of(peer * 128, 128), 128)], mix.at[me], cs_sem.at[i], cr_sem.at[i],
                                            device_id={'fsdp': peer}, device_id_type=MESH)

    def dy_load(blk):
        return pltpu.make_async_copy(dy_h.at[pl.ds(pl.multiple_of(blk * TOK, TOK), TOK), :], dy.at[blk % 2], dy_sem.at[blk % 2])

    def hop(p, step):
        return pltpu.make_async_remote_copy(bufs[p].at[step], bufs[p].at[step + 1], s_sem.at[p, step], r_sem.at[p, step + 1],
                                            device_id={'fsdp': peers[PARTS[p][1]]}, device_id_type=MESH)

    def work(p, step):
        kind, way, c0, width = PARTS[p]
        chip = chip_at((pos + 7 - step + way * (2 * step + 2)) % RING)
        lhs_ref, rhs_ref = left_ops[kind]
        rows = ROWS[kind]
        row = pl.multiple_of((chip * 2 + core) * rows, rows)
        lhs = [lhs_ref[b, pl.ds(row, rows), :] for b in range(2)]
        for c, w in col_tiles(width):
            part = sum(jnp.dot(lhs[b], rhs_ref[b, :, c0 + c:c0 + c + w], preferred_element_type=F32) for b in range(2))
            bufs[p][step, :, c:c + w] = bufs[p][step, :, c:c + w] + part

    for i in range(1, GROUP):
        mix_send(i).start()
    dy_load(0).start()
    go[...] = jnp.zeros_like(go)
    for p in range(N_PARTS):
        bufs[p][0] = jnp.zeros(bufs[p].shape[1:], F32)
    first_use = {0: (0, 1), 2: (2, 3, 4)}

    for way in range(2):
        pltpu.make_async_copy(own_dn.at[way * IN_BLK:(way + 1) * IN_BLK, :], dn_all.at[unit(me, way), :], fo_sem.at[way]).wait()

    @pl.loop(0, RING)
    def _(step):
        @pl.when(step > 0)
        def _():
            for way in range(2):
                dn_arrive(way, step).wait_recv()

                @pl.when(step < RING - 1)
                def _():
                    dn_hop(way, step).start()
                dn_share(way, step).start()

            @pl.loop(step - 1, step + step // (RING - 1))
            def _(done):
                row_grads(done)

        for p in range(N_PARTS):
            if p in first_use:
                @pl.when(step == 0)
                def _():
                    for i in first_use[p]:
                        local[i].wait()
                        cross[i].wait_recv()

            @pl.when(step > 0)
            def _():
                hop(p, step - 1).wait_recv()
            work(p, step)

            @pl.when(step < RING - 1)
            def _():
                hop(p, step).start()

        @pl.when(step == 0)
        def _():
            own_mix.wait()
            for i in range(1, GROUP):
                mix_send(i).wait()

        @pl.when((step > 0) & (step < 5))
        def _():
            @pl.loop(0, 4)
            def _(j):
                blk = (step - 1) * 4 + j
                dy_load(blk).wait()

                @pl.when(blk < GROUP - 1)
                def _():
                    dy_load(blk + 1).start()
                for c, w in col_tiles(2048):
                    go[:, c:c + w] += lax.dot_general(mix[blk], dy[blk % 2, :, c:c + w], (((0,), (0,)), ((), ())), preferred_element_type=F32)

        @pl.when(step == 5)
        def _():
            for i, (src, dst) in enumerate(((mix_h, mixf), (h0_h, h0))):
                pltpu.make_async_copy(src, dst, y_sem.at[2 + i]).wait()

            @pl.loop(0, 4)
            def _(t):
                @pl.when(t < 3)
                def _():
                    wo_load(t).wait()

                @pl.when(t == 3)
                def _():
                    wo_last().wait()

                @pl.when(t < 2)
                def _():
                    wo_load(t + 1).start()

                @pl.when(t == 2)
                def _():
                    wo_last().start()
                here = pl.ds(pl.multiple_of(t * 512, 512), 512)
                yv[:, here] = (h0[:, here].astype(F32) + jnp.dot(mixf[...], wo[t % 2], preferred_element_type=F32)).astype(BF16)

    last = RING - 1
    outs = []
    cp = pltpu.make_async_copy(go, go_h, out_sem.at[6])
    cp.start()
    outs.append(cp)
    cp = pltpu.make_async_copy(yv, y_h, out_sem.at[9])
    cp.start()
    outs.append(cp)
    targets = (((gu_h.at[:, 0:2304], 0, 2304),), ((gu_h.at[:, 2304:4096], 0, 1792),), ((gd_h, 0, 640), (gq_h.at[:, 0:256], 640, 896)),
               ((gq_h.at[:, 1152:2176], 0, 1024),), ((gq_h.at[:, 256:1152], 0, 896),), ((gq_h.at[:, 2176:3072], 0, 896),))
    for p in range(N_PARTS):
        for n, (dst, c0, c1) in enumerate(targets[p]):
            cp = pltpu.make_async_copy(bufs[p].at[last, :, c0:c1], dst, out_sem.at[p + 6 * n])
            cp.start()
            outs.append(cp)
    own_small.wait()
    for rc in smalls:
        rc.wait()
    ssum[...] = jnp.sum(smr[...], axis=0)
    cp = pltpu.make_async_copy(ssum, gs_h, out_sem.at[7])
    cp.start()
    outs.append(cp)
    for rc in cross:
        rc.wait_send()
    for p in range(N_PARTS):
        @pl.loop(0, last)
        def _(step):
            hop(p, step).wait_send()

    @pl.loop(0, RING)
    def _(step):
        for way in range(2):
            dn_share(way, step).wait_send()

            @pl.when(step < last)
            def _():
                dn_hop(way, step).wait_send()
    for cp in outs:
        cp.wait()


def grad_shards(mix, dy_all, nrm_t, dd, dq, lat_t, du, small, rows, weights, last_cols, dn, picked, gain):
    shapes = [(ROWS[k], RING, w) for k, _, _, w in PARTS]
    scratch = [pltpu.VMEM((GROUP, TOK, 128), BF16), pltpu.VMEM((2, TOK, 2048), BF16), pltpu.VMEM((128, 2048), F32), pltpu.VMEM((2, 2048, TOK), BF16),
               pltpu.VMEM((2, TOK, D_CAT), BF16), pltpu.VMEM((2, 512, TOK), BF16), pltpu.VMEM((2, TOK, D_UP), BF16)]
    scratch += [pltpu.VMEM((RING, r, w), F32) for r, _, w in shapes]
    scratch += [pltpu.VMEM((TOK, 2048), BF16), pltpu.VMEM((TOK, 2048), BF16), pltpu.VMEM((2, 2048, 512), BF16), pltpu.VMEM((TOK, 2048), BF16)]
    scratch += [pltpu.VMEM((TOK, 2048), BF16)] + [pltpu.VMEM((4, IN_BLK, 2048), BF16)] * 3 + [pltpu.VMEM((2, IN_BLK, 2048), F32)]
    scratch += [pltpu.VMEM((GROUP, 8, 128), F32), pltpu.VMEM((8, 128), F32)]
    dma = pltpu.SemaphoreType.DMA
    scratch += [dma((7,)), dma((5,)), dma((5,)), dma((N_PARTS, RING)), dma((N_PARTS, RING)), dma((GROUP,)), dma((GROUP,)), dma((GROUP,)), dma((GROUP,)), dma((2,)), dma((4,)), dma((2, RING)), dma((2, RING)), dma((2, RING)), dma((2, RING)), dma((3, 4)), dma((2,)), dma((10,))]
    return pl.pallas_call(
        grad_kernel,
        out_shape=(jax.ShapeDtypeStruct((TOK, 2048), BF16), jax.ShapeDtypeStruct((GROUP * TOK, 2048), BF16), jax.ShapeDtypeStruct((GROUP * TOK, 2048), F32), jax.ShapeDtypeStruct((128, 2048), F32), jax.ShapeDtypeStruct((128, 3072), F32), jax.ShapeDtypeStruct((128, D_DOWN), F32), jax.ShapeDtypeStruct((32, D_UP), F32), jax.ShapeDtypeStruct((8, 128), F32)),
        in_specs=[ANY] * 13 + [pl.BlockSpec(memory_space=pltpu.VMEM)], out_specs=(ANY,) * 8, scratch_shapes=scratch,
        compiler_params=pltpu.CompilerParams(collective_id=1, has_side_effects=True, vmem_limit_bytes=63 * 1024 * 1024),
        cost_estimate=pl.CostEstimate(flops=8 * 10**9, bytes_accessed=20 * 10**6, transcendentals=0), name='grad_shards',
    )(mix, dy_all, nrm_t, dd, dq, lat_t, du, small, rows, weights, last_cols, dn, picked, gain)


W_SHARDS = ((32, 4096), (128, 576), (128, 512))
HALF_TOK = TOK // 2


def spread_kernel(n_w, *refs):
    mask, rows_h = refs[0:2]
    srcs = refs[2:2 + n_w]
    got_h = refs[2 + n_w]
    outs = refs[3 + n_w:3 + 2 * n_w]
    stage = refs[3 + 2 * n_w:3 + 3 * n_w]
    own, mate, way0, way1 = refs[3 + 3 * n_w:7 + 3 * n_w]
    in_sem, own_sem, s_sem, r_sem, ps_sem, pr_sem, os_sem, or_sem, xs_sem, xr_sem, ts_sem, tr_sem, h_in, m_s, m_r, hs_sem, hr_sem, out_sem = refs[7 + 3 * n_w:]
    me, core, pos = place()
    twin = lax.axis_index('dp')
    partner = me + 1 - 2 * core
    barrier = pltpu.get_barrier_semaphore()
    peers = (at_pos(pos + 1, core), at_pos(pos + 7, core))
    for peer in peers + (partner,):
        pl.semaphore_signal(barrier, inc=1, device_id={'fsdp': peer}, device_id_type=MESH)
    pl.semaphore_signal(barrier, inc=1, device_id={'dp': 1 - twin}, device_id_type=MESH)
    pl.semaphore_wait(barrier, 4)
    loads = []
    for i in range(n_w):
        cp = pltpu.make_async_copy(srcs[i], stage[i], in_sem.at[i])
        cp.start()
        loads.append(cp)

    def row_load(q):
        return pltpu.make_async_copy(rows_h.at[at_pos(q, core)], own.at[q], h_in.at[q])

    def row_share(q):
        return pltpu.make_async_remote_copy(rows_h.at[at_pos(q, 1 - core)], mate.at[q], m_s.at[q], m_r.at[q],
                                            device_id={'fsdp': partner}, device_id_type=MESH)
    for j in (7, 1, 6, 2, 5, 3, 4, 0):
        row_share((pos + j) % RING).start()
        row_load((pos + j) % RING).start()

    def where(i, way, source, side):
        rows = W_SHARDS[i][0]
        part = rows // 4
        return outs[i].at[pl.ds(pl.multiple_of(source * rows + side * 2 * part + way * part, part), part), :]

    def whole(i):
        rows = W_SHARDS[i][0]
        return outs[i].at[pl.ds(pl.multiple_of(me * rows, rows), rows), :]

    def origin(way, step):
        return at_pos(pos + 8 - step + way * 2 * step, core)

    def hop(i, way, step, src=None):
        spot = where(i, way, origin(way, step), twin)
        return pltpu.make_async_remote_copy(spot if src is None else src, spot, s_sem.at[i, way, step], r_sem.at[i, way, step + 1],
                                            device_id={'fsdp': peers[way]}, device_id_type=MESH)

    def arrive(i, way, step):
        spot = where(i, way, origin(way, step), twin)
        return pltpu.make_async_remote_copy(spot, spot, s_sem.at[i, way, step], r_sem.at[i, way, step],
                                            device_id={'fsdp': peers[way]}, device_id_type=MESH)

    def share(i, way, step):
        spot = where(i, way, origin(way, step), twin)
        return pltpu.make_async_remote_copy(spot, spot, ps_sem.at[i, way, step], pr_sem.at[i, way, step],
                                            device_id={'fsdp': partner}, device_id_type=MESH)

    def share_own(i):
        return pltpu.make_async_remote_copy(stage[i], whole(i), os_sem.at[i], or_sem.at[i], device_id={'fsdp': partner}, device_id_type=MESH)

    def to_twin(i, way, step):
        spot = where(i, way, origin(way, step), twin)
        return pltpu.make_async_remote_copy(spot, spot, xs_sem.at[i, way, step], xr_sem.at[i, way, step],
                                            device_id={'dp': 1 - twin}, device_id_type=MESH)

    def share_twin(i, way, step):
        spot = where(i, way, origin(way, step), 1 - twin)
        return pltpu.make_async_remote_copy(spot, spot, ts_sem.at[i, way, step], tr_sem.at[i, way, step],
                                            device_id={'fsdp': partner}, device_id_type=MESH)
    ways = (way0, way1)

    def row_hop(way, step):
        return pltpu.make_async_remote_copy(ways[way].at[step], ways[way].at[step + 1], hs_sem.at[way, step], hr_sem.at[way, step + 1],
                                            device_id={'fsdp': peers[way]}, device_id_type=MESH)

    def fill(way, step, first):
        q = (pos + 7 - step + way * (2 * step + 2)) % RING
        chip = chip_at(q)
        for c in range(0, HALF_TOK, 48):
            lo = way * HALF_TOK + c
            mine, theirs = mask[0, chip, lo:lo + 48, :], mask[1, chip, lo:lo + 48, :]
            for w in range(0, 2048, 128):
                part = own[q, lo:lo + 48, w:w + 128] * mine + mate[q, lo:lo + 48, w:w + 128] * theirs
                if not first:
                    part = part + ways[way][step, c:c + 48, w:w + 128]
                ways[way][step, c:c + 48, w:w + 128] = part

    kept = []
    for i in range(n_w):
        loads[i].wait()
        part = W_SHARDS[i][0] // 4
        for way in range(2):
            hop(i, way, 0, stage[i].at[pl.ds(pl.multiple_of(twin * 2 * part + way * part, part), part), :]).start()
        share_own(i).start()
        cp = pltpu.make_async_copy(stage[i], whole(i), own_sem.at[i])
        cp.start()
        kept.append(cp)
    for j in (7, 1, 6, 2, 5, 3, 4, 0):
        row_load((pos + j) % RING).wait()
        row_share((pos + j) % RING).wait_recv()
        if j in (7, 1):
            way = 0 if j == 7 else 1
            fill(way, 0, True)
            row_hop(way, 0).start()

    @pl.loop(1, RING)
    def _(step):
        for i in range(n_w):
            for way in range(2):
                arrive(i, way, step).wait_recv()

                @pl.when(step < RING - 1)
                def _():
                    hop(i, way, step).start()
                share(i, way, step).start()
                to_twin(i, way, step).start()
        for way in range(2):
            row_hop(way, step - 1).wait_recv()
            fill(way, step, False)

            @pl.when(step < RING - 1)
            def _():
                row_hop(way, step).start()

        @pl.when(step > 1)
        def _():
            for i in range(n_w):
                for way in range(2):
                    to_twin(i, way, step - 1).wait_recv()
                    share_twin(i, way, step - 1).start()

    for i in range(n_w):
        for way in range(2):
            to_twin(i, way, RING - 1).wait_recv()
            share_twin(i, way, RING - 1).start()
    for way in range(2):
        cp = pltpu.make_async_copy(ways[way].at[RING - 1], got_h.at[way * HALF_TOK:(way + 1) * HALF_TOK, :], out_sem.at[way])
        cp.start()
        kept.append(cp)
    for cp in kept:
        cp.wait()

    @pl.loop(0, RING)
    def _(step):
        row_share(step).wait_send()

        @pl.when(step < RING - 1)
        def _():
            for way in range(2):
                row_hop(way, step).wait_send()
        for i in range(n_w):
            for way in range(2):
                @pl.when(step < RING - 1)
                def _():
                    hop(i, way, step).wait_send()

                @pl.when(step > 0)
                def _():
                    share(i, way, step).wait()
                    to_twin(i, way, step).wait_send()
                    share_twin(i, way, step).wait()
    for i in range(n_w):
        share_own(i).wait()


def spread(mask, rows, shards):
    dma = pltpu.SemaphoreType.DMA
    n_w = len(shards)
    return pl.pallas_call(
        lambda *refs: spread_kernel(n_w, *refs),
        out_shape=(jax.ShapeDtypeStruct((TOK, 2048), BF16),) + tuple(jax.ShapeDtypeStruct((GROUP * r, w), BF16) for r, w in W_SHARDS),
        in_specs=[pl.BlockSpec(memory_space=pltpu.VMEM)] + [ANY] * (n_w + 1), out_specs=(ANY,) * (n_w + 1),
        scratch_shapes=[pltpu.VMEM(s, BF16) for s in W_SHARDS] + [pltpu.VMEM((RING, TOK, 2048), BF16)] * 2 + [pltpu.VMEM((RING, HALF_TOK, 2048), BF16)] * 2
        + [dma((n_w,)), dma((n_w,))] + [dma((n_w, 2, RING))] * 4 + [dma((n_w,))] * 2 + [dma((n_w, 2, RING))] * 4 + [dma((RING,)) for _ in range(3)] + [dma((2, RING)) for _ in range(2)] + [dma((2,))],
        compiler_params=pltpu.CompilerParams(collective_id=2, has_side_effects=True, vmem_limit_bytes=60 * 1024 * 1024),
        cost_estimate=pl.CostEstimate(flops=8 * 10**9, bytes_accessed=27 * 10**6, transcendentals=0), name='spread',
    )(mask, rows, *shards)
ROW_BLK = 128
SUB = 144
UNROLL = 4
OUT_SLOTS = 4


def table_kernel(starts, toks, rows, flags, small, grad_h, *refs):
    passed, out_h, given, gain_out, kv_out = refs[0:5], refs[5], refs[6:11], refs[11], refs[12]
    grad, acc, ob, nil, in_sem, out_sem = refs[13:19]
    hold, cut, ride_in, ride_out = refs[19:24], refs[24], refs[25], refs[26]
    boards = [pltpu.make_async_copy(src, dst, ride_in.at[i]) for i, (src, dst) in enumerate(zip(passed, hold))]
    leaves = [pltpu.make_async_copy(cut if i == 2 else src, dst, ride_out.at[i]) for i, (src, dst) in enumerate(zip(hold, given))]
    for cp in boards:
        cp.start()
    gain_out[...] = small[0:1, :]
    kv_out[...] = small[1:2, 0:32]
    n_in = GROUP * TOK // SUB
    n_out = out_h.shape[0] // ROW_BLK

    def load(blk):
        span = pl.ds(pl.multiple_of(blk * SUB, SUB), SUB)
        return pltpu.make_async_copy(grad_h.at[span, :], grad.at[span, :], in_sem)

    @pl.loop(0, n_in)
    def _(blk):
        @pl.when(flags[blk] > 0)
        def _():
            load(blk).start()
    nil[...] = jnp.zeros_like(nil)

    @pl.loop(0, n_in)
    def _(blk):
        @pl.when(flags[blk] > 0)
        def _():
            load(blk).wait()
    for cp in boards:
        cp.wait()
    cut[...] = hold[2][...].T[0:576, :]
    for cp in leaves:
        cp.start()

    def store(blk, src):
        return pltpu.make_async_copy(src, out_h.at[pl.ds(pl.multiple_of(blk * ROW_BLK, ROW_BLK), ROW_BLK), :], out_sem.at[blk % OUT_SLOTS])
    @pl.loop(0, n_out)
    def _(blk):
        first, last = starts[blk], starts[blk + 1]
        slot = blk % OUT_SLOTS

        @pl.when(blk >= OUT_SLOTS)
        def _():
            store(blk - OUT_SLOTS, nil).wait()

        @pl.when(first == last)
        def _():
            store(blk, nil).start()

        @pl.when(first < last)
        def _():
            acc[...] = jnp.zeros_like(acc)

            def add(k):
                acc[pl.ds(rows[k], 1), :] += grad[pl.ds(toks[k], 1), :]
            quads = (last - first) // UNROLL

            @pl.loop(0, quads)
            def _(i):
                for j in range(UNROLL):
                    add(first + i * UNROLL + j)

            @pl.loop(first + quads * UNROLL, last)
            def _(k):
                add(k)
            ob[slot] = acc[...].astype(BF16)
            store(blk, ob.at[slot]).start()
    for blk in range(n_out - OUT_SLOTS, n_out):
        store(blk, nil).wait()
    for cp in leaves:
        cp.wait()


def table_grad(starts, toks, rows, flags, small, row_grads, vocab_dev, passed):
    smem = pl.BlockSpec(memory_space=pltpu.SMEM)
    vmem = pl.BlockSpec(memory_space=pltpu.VMEM)
    dma = pltpu.SemaphoreType.DMA
    shapes = [jax.ShapeDtypeStruct((vocab_dev, 2048), BF16)] + [jax.ShapeDtypeStruct((576, 128) if i == 2 else p.shape, p.dtype) for i, p in enumerate(passed)]
    shapes += [jax.ShapeDtypeStruct((1, 128), F32), jax.ShapeDtypeStruct((1, 32), F32)]
    return pl.pallas_call(
        table_kernel, out_shape=tuple(shapes),
        in_specs=[smem] * 4 + [vmem] + [ANY] * 6, out_specs=(ANY,) * 6 + (vmem,) * 2,
        scratch_shapes=[pltpu.VMEM((GROUP * TOK, 2048), F32)]
        + [pltpu.VMEM((ROW_BLK, 2048), F32), pltpu.VMEM((OUT_SLOTS, ROW_BLK, 2048), BF16), pltpu.VMEM((ROW_BLK, 2048), BF16), dma, dma((OUT_SLOTS,))]
        + [pltpu.VMEM(p.shape, p.dtype) for p in passed] + [pltpu.VMEM((576, 128), F32), dma((5,)), dma((5,))],
        compiler_params=pltpu.CompilerParams(vmem_limit_bytes=63 * 1024 * 1024),
        cost_estimate=pl.CostEstimate(flops=10**9, bytes_accessed=90 * 10**6, transcendentals=0), name='table_grad',
    )(starts, toks, rows, flags, small, row_grads, *passed)


def small_kernel(src, out, loc_sem, s_sem, r_sem):
    me = lax.axis_index('fsdp')
    meet_all(me)
    own = pltpu.make_async_copy(src, out.at[me], loc_sem)
    own.start()

    def send(step):
        return pltpu.make_async_remote_copy(src, out.at[me], s_sem.at[step], r_sem.at[step],
                                            device_id={'fsdp': (me + step) % GROUP}, device_id_type=MESH)
    for step in range(1, GROUP):
        send(step).start()
    for step in range(1, GROUP):
        send(step).wait()
    own.wait()


def small_gather(tile):
    dma = pltpu.SemaphoreType.DMA
    return pl.pallas_call(
        small_kernel, out_shape=jax.ShapeDtypeStruct((GROUP, 8, 128), F32),
        in_specs=[pl.BlockSpec(memory_space=pltpu.VMEM)], out_specs=pl.BlockSpec(memory_space=pltpu.VMEM),
        scratch_shapes=[dma, dma((GROUP,)), dma((GROUP,))],
        compiler_params=pltpu.CompilerParams(collective_id=0, has_side_effects=True),
        cost_estimate=pl.CostEstimate(flops=10**7, bytes_accessed=10**5, transcendentals=0), name='small_gather',
    )(tile)


def blank(shape, dtype):
    return pl.pallas_call(lambda out: None, out_shape=jax.ShapeDtypeStruct(shape, dtype), out_specs=ANY, name='blank')()


def block_step(rows_f32, grad_rows, full_weights, seq_count):
    gain_vec, w_query, w_kv_down, kv_gain, w_kv_up, w_out = full_weights
    kv_rank = kv_gain.shape[0]
    tok_count = rows_f32.shape[0]
    seq_len = tok_count // seq_count
    normed, norm_pull = jax.vjp(rms_scale, rows_f32, gain_vec)
    q_proj = jnp.dot(normed, w_query, preferred_element_type=jnp.float32).astype(jnp.bfloat16)
    kv_down = jnp.dot(normed, w_kv_down, preferred_element_type=jnp.float32).astype(jnp.bfloat16)
    latent, latent_pull = jax.vjp(rms_scale, kv_down[:, :kv_rank], kv_gain)
    kv_up = jnp.dot(latent, w_kv_up, preferred_element_type=jnp.float32).astype(jnp.bfloat16)
    attn_mix, attn_pull = jax.vjp(attend_local, q_proj.reshape(seq_count, seq_len, -1, NOPE_DIM + ROPE_DIM), kv_down[:, kv_rank:].reshape(seq_count, seq_len, ROPE_DIM), kv_up.reshape(seq_count, seq_len, -1, NOPE_DIM + VALUE_DIM))
    mix_rows = attn_mix.reshape(tok_count, -1)
    d_mix = lax.dot_general(grad_rows[:, :1536], w_out[0], COL_DIMS, preferred_element_type=jnp.float32)
    d_mix = (d_mix + lax.dot_general(grad_rows[:, 1536:], w_out[1], COL_DIMS, preferred_element_type=jnp.float32)).astype(jnp.bfloat16)
    d_query, d_pe, d_up = attn_pull(d_mix.reshape(attn_mix.shape))
    d_query = d_query.reshape(tok_count, -1)
    d_up = d_up.reshape(tok_count, -1)
    d_latent = lax.dot_general(d_up, w_kv_up, COL_DIMS, preferred_element_type=jnp.float32).astype(jnp.bfloat16)
    d_ckv, d_kv_gain = latent_pull(d_latent)
    d_down = jnp.concatenate([d_ckv, d_pe.reshape(tok_count, ROPE_DIM)], axis=1)
    d_normed = lax.dot_general(d_query, w_query, COL_DIMS, preferred_element_type=jnp.float32)
    d_normed = d_normed + lax.dot_general(d_down, w_kv_down, COL_DIMS, preferred_element_type=jnp.float32)
    d_normed = d_normed.astype(jnp.bfloat16)
    _, d_gain = norm_pull(d_normed)
    return d_normed, normed, mix_rows, latent, d_query, d_down, d_up, d_gain, d_kv_gain


def solution(mesh):
    tok_spec = P(('dp', 'fsdp'), None)
    seq_spec = P(('dp', 'fsdp'), None, None)
    part_vec = P(('dp', 'fsdp'))
    vec_spec = P('fsdp')
    mat_spec = P('fsdp', None)

    def device_step(tok_ids, grad_out, emb_table, norm_gain, w_query, w_kv_down, kv_gain, w_kv_up, w_out):
        seq_count, seq_len = tok_ids.shape
        vocab_dev, d_model = emb_table.shape
        tok_count = seq_count * seq_len
        me = lax.axis_index('fsdp')
        grad_rows = grad_out.reshape(tok_count, d_model)
        bundle = lax.all_gather(jnp.concatenate([w_query, w_out[:, :1536]], axis=1), 'fsdp', tiled=True)
        fill = lambda rows: jnp.pad(rows, ((0, 0), (0, 128 - rows.shape[1])))
        tile = jnp.concatenate([fill(tok_ids.astype(F32)), norm_gain.astype(F32).reshape(1, 128), fill(kv_gain.astype(F32).reshape(1, 32)), jnp.zeros((3, 128), F32)], axis=0)
        table = small_gather(tile)
        all_ids = table[:, :seq_count, :seq_len].reshape(GROUP, tok_count).astype(jnp.int32)
        gain_full = table[:, 3, :].reshape(-1)
        kv_gain_full = table[:, 4, :32].reshape(-1)

        owner = all_ids // vocab_dev
        mine = (owner == me)
        local = all_ids - me * vocab_dev
        stamp = jnp.arange(GROUP * tok_count).reshape(GROUP, tok_count) * ROW_BLK
        keys = lax.sort(jnp.where(mine, (local // ROW_BLK) * 2**20 + stamp + local % ROW_BLK, 2**30).reshape(-1))
        starts = jnp.sum((mine & (local < ROW_BLK * jnp.arange(vocab_dev // ROW_BLK + 1)[:, None, None])).astype(jnp.int32), axis=(1, 2))
        flags = jnp.sum(mine.reshape(-1, SUB).astype(jnp.int32), axis=1)
        picked = jnp.take(emb_table, jnp.where(mine, local, 0).reshape(-1), axis=0, mode='clip')
        core = me % 2
        near = lax.dynamic_index_in_dim(owner.reshape(RING, 2, tok_count), core, 1, keepdims=False)
        mask = jnp.stack([near == me, near == me + 1 - 2 * core]).astype(BF16)
        mask = jnp.broadcast_to(mask[..., None], (2, RING, tok_count, 128))
        picked, keys, starts, flags, w_kv_down = lax.optimization_barrier((picked, keys, starts, flags, w_kv_down))
        tok_rows, full_kvb, full_kva, wo_last = spread(mask, picked.reshape(GROUP, tok_count, d_model), (w_kv_up, w_kv_down, w_out[:, 1536:]))
        full_wq, full_wo = bundle[:, :3072], (bundle[:, 3072:], wo_last)
        tok_rows, grad_rows = lax.optimization_barrier((tok_rows, grad_rows))
        all_dy = lax.all_gather(grad_rows, 'fsdp', tiled=True)
        d_normed, normed, mix, latent, d_query, d_down, d_up, d_gain, d_kv_gain = block_step(
            tok_rows.astype(F32), grad_rows, (gain_full, full_wq, full_kva, kv_gain_full, full_kvb, full_wo), seq_count)
        small = jnp.concatenate([d_gain.reshape(GROUP, 1, 128), jnp.pad(d_kv_gain.reshape(GROUP, 1, 32), ((0, 0), (0, 0), (0, 96))), jnp.zeros((GROUP, 6, 128), F32)], axis=1)
        block_out, _, row_grads, g_out, g_query, g_down, g_up, g_small = grad_shards(mix, all_dy, normed.T, jnp.pad(d_down, ((0, 0), (0, D_DOWN - d_down.shape[1]))), d_query, latent.T, d_up, small, tok_rows, bundle, wo_last, d_normed, picked, gain_full.reshape(1, -1))
        grad_table, block_out, g_query, g_down, g_up, g_out, g_gain, g_kv_gain = table_grad(
            starts, (keys >> 7) & 8191, keys & (ROW_BLK - 1), flags, g_small, row_grads, vocab_dev,
            (block_out, g_query, g_down, g_up, g_out))
        return (block_out.reshape(seq_count, seq_len, d_model), grad_table, g_gain.reshape(-1), g_query, g_down.T, g_kv_gain.reshape(-1), g_up, g_out)

    return jax.shard_map(device_step, mesh=mesh, in_specs=(tok_spec, seq_spec, mat_spec, vec_spec, mat_spec, mat_spec, vec_spec, mat_spec, mat_spec), out_specs=(seq_spec, tok_spec, part_vec, tok_spec, tok_spec, part_vec, tok_spec, tok_spec), check_vma=False)
```

```python
import math
import jax
import jax.numpy as jnp
from jax import lax
from jax.sharding import PartitionSpec as P
from jax.experimental import pallas as pl
from jax.experimental.pallas import tpu as pltpu

NOPE_DIM = 128
ROPE_DIM = 64
VALUE_DIM = 128
ROPE_THETA = 50000.0
RMS_EPS = 1e-6
ATTN_SCALE = (NOPE_DIM + ROPE_DIM) ** -0.5 * (0.1 * math.log(32.0) + 1.0) ** 2
ROW_DIMS = (((0,), (0,)), ((), ()))
COL_DIMS = (((1,), (1,)), ((), ()))


def rms_scale(in_vals, gain_vec):
    vals_f32 = in_vals.astype(jnp.float32)
    inv_rms = lax.rsqrt(jnp.mean(vals_f32 * vals_f32, axis=-1, keepdims=True) + RMS_EPS)
    return (vals_f32 * inv_rms * gain_vec).astype(jnp.bfloat16)


def rope_tables(seq_len):
    positions = jnp.arange(seq_len, dtype=jnp.float32)
    inv_freq = ROPE_THETA ** (-2.0 * jnp.arange(ROPE_DIM // 2, dtype=jnp.float32) / ROPE_DIM)
    rot_angle = positions[:, None] * inv_freq[None, :]
    rot_angle = jnp.concatenate([rot_angle, rot_angle], axis=-1)
    return jnp.cos(rot_angle), jnp.sin(rot_angle)


def apply_rope(in_vals, cos_tab, sin_tab):
    half_dim = ROPE_DIM // 2
    vals_f32 = in_vals.astype(jnp.float32)
    turned = jnp.concatenate([-vals_f32[..., half_dim:], vals_f32[..., :half_dim]], axis=-1)
    return (vals_f32 * cos_tab + turned * sin_tab).astype(jnp.bfloat16)


def attend_local(q_proj, pe_raw, kv_up):
    seq_len = q_proj.shape[1]
    cos_tab, sin_tab = rope_tables(seq_len)
    q_rot = apply_rope(q_proj[..., NOPE_DIM:], cos_tab[:, None, :], sin_tab[:, None, :])
    k_rot = apply_rope(pe_raw, cos_tab, sin_tab)
    scores = jnp.einsum('bshd,bthd->bhst', q_proj[..., :NOPE_DIM], kv_up[..., :NOPE_DIM], preferred_element_type=jnp.float32)
    scores = scores + jnp.einsum('bshd,btd->bhst', q_rot, k_rot, preferred_element_type=jnp.float32)
    positions = jnp.arange(seq_len)
    causal = positions[:, None] >= positions[None, :]
    scores = jnp.where(causal, scores * ATTN_SCALE, -1e30)
    attn_probs = jax.nn.softmax(scores, axis=-1).astype(jnp.bfloat16)
    attn_mix = jnp.einsum('bhst,bthd->bshd', attn_probs, kv_up[..., NOPE_DIM:], preferred_element_type=jnp.float32)
    return attn_mix.astype(jnp.bfloat16)


F32, BF16 = jnp.float32, jnp.bfloat16
MESH = pl.DeviceIdType.MESH
ANY = pl.BlockSpec(memory_space=pl.ANY)
RING = 8
GROUP = 16

def chip_at(pos):
    side = pos // 4
    return (pos + side * (7 - 2 * pos)) * 2 + side

def place():
    me = lax.axis_index('fsdp')
    core = me % 2
    chip = me // 2
    side = chip % 2
    zz = chip // 2
    return me, core, zz + side * (7 - 2 * zz)

def at_pos(pos, core):
    return chip_at(pos % RING) * 2 + core

def meet_all(me):
    barrier = pltpu.get_barrier_semaphore()
    for step in range(1, GROUP):
        pl.semaphore_signal(barrier, inc=1, device_id={'fsdp': (me + step) % GROUP}, device_id_type=MESH)
    pl.semaphore_wait(barrier, GROUP - 1)

TOK = 288
IN_BLK = 144
PIECE = 16
D_OUT, D_CAT, D_UP, D_DOWN = 2048, 3712, 4096, 640
WO_COL = 3072
WO_CUT = 1152
CUT = 1792
PARTS = (('u', 0, 0, 2304), ('u', 1, 2304, 1792), ('n', 0, 0, 896), ('n', 1, 1792, 1024), ('n', 0, 896, 896), ('n', 1, 2816, 896))
N_PARTS = len(PARTS)
ROWS = {'n': 128, 'u': 32}

def col_tiles(width):
    step = 512
    return [(c, min(step, width - c)) for c in range(0, width, step)]

def grad_kernel(mix_h, dy_h, nrm_h, dd_h, dq_h, lat_h, du_h, sm_h, h0_h, wo_h, wl_h, dn_h, h_h, gain, y_h, dn_all, grad_h, go_h, gq_h, gd_h, gu_h, gs_h,
                mix, dy, go, nrm, cat, lat, du, b0, b1, b2, b3, b4, b5, mixf, h0, wo, yacc, yv, own_dn, fdn, fdy, fh, fo, smr, ssum, loc_sem, xs_sem, xr_sem, s_sem, r_sem, ms_sem, mr_sem, cs_sem, cr_sem, dy_sem, y_sem, ns_sem, nr_sem, np_sem, nq_sem, f_sem, fo_sem, out_sem):
    me, core, pos = place()
    partner = me + 1 - 2 * core
    meet_all(me)
    acts = ((lat_h, lat), (du_h, du), (nrm_h, nrm), (dd_h, cat.at[:, :, 0:D_DOWN]), (dq_h, cat.at[:, :, D_DOWN:D_CAT]))
    local, cross = [], []
    for i, (src, dst) in enumerate(acts):
        cp = pltpu.make_async_copy(src, dst.at[core], loc_sem.at[i])
        cp.start()
        local.append(cp)
        rc = pltpu.make_async_remote_copy(src, dst.at[core], xs_sem.at[i], xr_sem.at[i], device_id={'fsdp': partner}, device_id_type=MESH)
        rc.start()
        cross.append(rc)
    peers = (at_pos(pos + 1, core), at_pos(pos + 7, core))

    def unit(dev, way):
        return pl.ds(pl.multiple_of(dev * TOK + way * IN_BLK, PIECE), IN_BLK)

    def origin(way, step):
        return at_pos(pos + 8 - step + way * 2 * step, core)

    def dn_hop(way, step, src=None):
        spot = dn_all.at[unit(origin(way, step), way), :]
        return pltpu.make_async_remote_copy(spot if src is None else src, spot, ns_sem.at[way, step], nr_sem.at[way, step + 1],
                                            device_id={'fsdp': peers[way]}, device_id_type=MESH)

    def dn_arrive(way, step):
        spot = dn_all.at[unit(origin(way, step), way), :]
        return pltpu.make_async_remote_copy(spot, spot, ns_sem.at[way, step], nr_sem.at[way, step],
                                            device_id={'fsdp': peers[way]}, device_id_type=MESH)

    def dn_share(way, step, src=None):
        spot = dn_all.at[unit(origin(way, step), way), :]
        return pltpu.make_async_remote_copy(spot if src is None else src, spot, np_sem.at[way, step], nq_sem.at[way, step],
                                            device_id={'fsdp': partner}, device_id_type=MESH)
    own_load = pltpu.make_async_copy(dn_h, own_dn, f_sem.at[0, 0])
    own_load.start()
    own_load.wait()
    for way in range(2):
        src = own_dn.at[way * IN_BLK:(way + 1) * IN_BLK, :]
        dn_hop(way, 0, src).start()
        dn_share(way, 0, src).start()
        pltpu.make_async_copy(src, dn_all.at[unit(me, way), :], fo_sem.at[way]).start()

    def row_grads(step):
        jobs = [(at_pos(pos + 8 - step + way * 2 * step, c), way) for way in range(2) for c in (core, 1 - core)]

        def fetch(slot):
            dev, way = jobs[slot]
            return [pltpu.make_async_copy(src.at[unit(dev, way), :], dst.at[slot], f_sem.at[i, slot])
                    for i, (src, dst) in enumerate(((dn_all, fdn), (dy_h, fdy), (h_h, fh)))]

        def put(slot):
            dev, way = jobs[slot]
            return pltpu.make_async_copy(fo.at[slot % 2], grad_h.at[unit(dev, way), :], fo_sem.at[slot % 2])
        for way in range(2):
            dn_share(way, step).wait_recv()
        for slot in range(4):
            for cp in fetch(slot):
                cp.start()

        for slot in range(4):
            for cp in fetch(slot):
                cp.wait()
            if slot >= 2:
                put(slot - 2).wait()

            @pl.loop(0, IN_BLK // 48)
            def _(g):
                r0 = pl.multiple_of(g * 48, PIECE)

                def tile(ref, p, c):
                    return ref[slot, pl.ds(r0 + p, PIECE), c:c + 128].astype(F32)
                scale = []
                for p in range(0, 48, PIECE):
                    sq = jnp.zeros((PIECE, 128), F32)
                    al = jnp.zeros((PIECE, 128), F32)
                    for c in range(0, 2048, 128):
                        h = tile(fh, p, c)
                        sq = sq + h * h
                        al = al + h * (tile(fdn, p, c) * gain[:, c:c + 128])
                    scale.append((jnp.sum(sq, axis=1, keepdims=True), jnp.sum(al, axis=1, keepdims=True)))
                for p, (sq, al) in zip(range(0, 48, PIECE), scale):
                    inv = lax.rsqrt(sq * (1.0 / 2048) + RMS_EPS)
                    coef = inv * inv * inv * (al * (1.0 / 2048))
                    for c in range(0, 2048, 128):
                        s = tile(fdn, p, c) * gain[:, c:c + 128]
                        fo[slot % 2, pl.ds(r0 + p, PIECE), c:c + 128] = tile(fdy, p, c) + inv * s - coef * tile(fh, p, c)
            put(slot).start()
        put(2).wait()
        put(3).wait()

    own_small = pltpu.make_async_copy(sm_h.at[me], smr.at[0], loc_sem.at[5])
    own_small.start()
    own_mix = pltpu.make_async_copy(mix_h.at[:, pl.ds(pl.multiple_of(me * 128, 128), 128)], mix.at[me], loc_sem.at[6])
    own_mix.start()
    smalls, mixes = [], []
    for i in range(1, GROUP):
        peer = (me + i) % GROUP
        rc = pltpu.make_async_remote_copy(sm_h.at[peer], smr.at[i], ms_sem.at[i], mr_sem.at[i], device_id={'fsdp': peer}, device_id_type=MESH)
        rc.start()
        smalls.append(rc)
    for i, (src, dst) in enumerate(((mix_h, mixf), (h0_h, h0))):
        pltpu.make_async_copy(src, dst, y_sem.at[2, i]).start()

    def wo_load(t):
        span = pl.ds(pl.multiple_of(t * 256, 256), 256)
        return [pltpu.make_async_copy(src, dst, y_sem.at[i, t % 2]) for i, (src, dst) in enumerate((
            (wo_h.at[span, WO_COL:WO_COL + WO_CUT], wo.at[t % 2, :, 0:WO_CUT]), (wl_h.at[span, :], wo.at[t % 2, :, WO_CUT:2048])))]
    for cp in wo_load(0):
        cp.start()
    bufs = (b0, b1, b2, b3, b4, b5)
    left_ops = {'n': (nrm, cat), 'u': (lat, du)}

    def mix_send(i):
        peer = (me + i) % GROUP
        return pltpu.make_async_remote_copy(mix_h.at[:, pl.ds(pl.multiple_of(peer * 128, 128), 128)], mix.at[me], cs_sem.at[i], cr_sem.at[i],
                                            device_id={'fsdp': peer}, device_id_type=MESH)

    def dy_load(blk):
        return pltpu.make_async_copy(dy_h.at[pl.ds(pl.multiple_of(blk * TOK, TOK), TOK), :], dy.at[blk % 2], dy_sem.at[blk % 2])

    def hop(p, step):
        return pltpu.make_async_remote_copy(bufs[p].at[step], bufs[p].at[step + 1], s_sem.at[p, step], r_sem.at[p, step + 1],
                                            device_id={'fsdp': peers[PARTS[p][1]]}, device_id_type=MESH)

    def work(p, step):
        kind, way, c0, width = PARTS[p]
        chip = chip_at((pos + 7 - step + way * (2 * step + 2)) % RING)
        lhs_ref, rhs_ref = left_ops[kind]
        rows = ROWS[kind]
        row = pl.multiple_of((chip * 2 + core) * rows, rows)
        lhs = [lhs_ref[b, pl.ds(row, rows), :] for b in range(2)]
        for c, w in col_tiles(width):
            part = sum(jnp.dot(lhs[b], rhs_ref[b, :, c0 + c:c0 + c + w], preferred_element_type=F32) for b in range(2))
            bufs[p][step, :, c:c + w] = bufs[p][step, :, c:c + w] + part

    for i in range(1, GROUP):
        mix_send(i).start()
    dy_load(0).start()
    go[...] = jnp.zeros_like(go)
    for p in range(N_PARTS):
        bufs[p][0] = jnp.zeros(bufs[p].shape[1:], F32)
    first_use = {0: (0, 1), 2: (2, 3, 4)}

    for way in range(2):
        pltpu.make_async_copy(own_dn.at[way * IN_BLK:(way + 1) * IN_BLK, :], dn_all.at[unit(me, way), :], fo_sem.at[way]).wait()

    @pl.loop(0, RING)
    def _(step):
        @pl.when(step > 0)
        def _():
            for way in range(2):
                dn_arrive(way, step).wait_recv()

                @pl.when(step < RING - 1)
                def _():
                    dn_hop(way, step).start()
                dn_share(way, step).start()

            @pl.loop(step - 1, step + step // (RING - 1))
            def _(done):
                row_grads(done)

        for p in range(N_PARTS):
            if p in first_use:
                @pl.when(step == 0)
                def _():
                    for i in first_use[p]:
                        local[i].wait()
                        cross[i].wait_recv()

            @pl.when(step > 0)
            def _():
                hop(p, step - 1).wait_recv()
            work(p, step)

            @pl.when(step < RING - 1)
            def _():
                hop(p, step).start()

        @pl.when(step == 0)
        def _():
            own_mix.wait()
            for i in range(1, GROUP):
                mix_send(i).wait()

        @pl.when((step > 0) & (step < 5))
        def _():
            @pl.loop(0, 4)
            def _(j):
                blk = (step - 1) * 4 + j
                dy_load(blk).wait()

                @pl.when(blk < GROUP - 1)
                def _():
                    dy_load(blk + 1).start()
                for c, w in col_tiles(2048):
                    go[:, c:c + w] += lax.dot_general(mix[blk], dy[blk % 2, :, c:c + w], (((0,), (0,)), ((), ())), preferred_element_type=F32)

        @pl.when(step == 5)
        def _():
            for i, (src, dst) in enumerate(((mix_h, mixf), (h0_h, h0))):
                pltpu.make_async_copy(src, dst, y_sem.at[2, i]).wait()

            yacc[...] = h0[...].astype(F32)

            @pl.loop(0, 8)
            def _(t):
                for cp in wo_load(t):
                    cp.wait()

                @pl.when(t < 7)
                def _():
                    for cp in wo_load(t + 1):
                        cp.start()

                @pl.loop(0, 4)
                def _(j):
                    here = pl.ds(pl.multiple_of(j * 512, 512), 512)
                    yacc[:, here] += jnp.dot(mixf[:, pl.ds(pl.multiple_of(t * 256, 256), 256)], wo[t % 2, :, here], preferred_element_type=F32)
            yv[...] = yacc[...].astype(BF16)

    last = RING - 1
    outs = []
    cp = pltpu.make_async_copy(go, go_h, out_sem.at[6])
    cp.start()
    outs.append(cp)
    cp = pltpu.make_async_copy(yv, y_h, out_sem.at[9])
    cp.start()
    outs.append(cp)
    targets = (((gu_h.at[:, 0:2304], 0, 2304),), ((gu_h.at[:, 2304:4096], 0, 1792),), ((gd_h, 0, 640), (gq_h.at[:, 0:256], 640, 896)),
               ((gq_h.at[:, 1152:2176], 0, 1024),), ((gq_h.at[:, 256:1152], 0, 896),), ((gq_h.at[:, 2176:3072], 0, 896),))
    for p in range(N_PARTS):
        for n, (dst, c0, c1) in enumerate(targets[p]):
            cp = pltpu.make_async_copy(bufs[p].at[last, :, c0:c1], dst, out_sem.at[p + 6 * n])
            cp.start()
            outs.append(cp)
    own_small.wait()
    for rc in smalls:
        rc.wait()
    ssum[...] = jnp.sum(smr[...], axis=0)
    cp = pltpu.make_async_copy(ssum, gs_h, out_sem.at[7])
    cp.start()
    outs.append(cp)
    for rc in cross:
        rc.wait_send()
    for p in range(N_PARTS):
        @pl.loop(0, last)
        def _(step):
            hop(p, step).wait_send()

    @pl.loop(0, RING)
    def _(step):
        for way in range(2):
            dn_share(way, step).wait_send()

            @pl.when(step < last)
            def _():
                dn_hop(way, step).wait_send()
    for cp in outs:
        cp.wait()


def grad_shards(mix, dy_all, nrm_t, dd, dq, lat_t, du, small, rows, weights, last_cols, dn, picked, gain):
    shapes = [(ROWS[k], RING, w) for k, _, _, w in PARTS]
    scratch = [pltpu.VMEM((GROUP, TOK, 128), BF16), pltpu.VMEM((2, TOK, 2048), BF16), pltpu.VMEM((128, 2048), F32), pltpu.VMEM((2, 2048, TOK), BF16),
               pltpu.VMEM((2, TOK, D_CAT), BF16), pltpu.VMEM((2, 512, TOK), BF16), pltpu.VMEM((2, TOK, D_UP), BF16)]
    scratch += [pltpu.VMEM((RING, r, w), F32) for r, _, w in shapes]
    scratch += [pltpu.VMEM((TOK, 2048), BF16), pltpu.VMEM((TOK, 2048), BF16), pltpu.VMEM((2, 256, 2048), BF16), pltpu.VMEM((TOK, 2048), F32), pltpu.VMEM((TOK, 2048), BF16)]
    scratch += [pltpu.VMEM((TOK, 2048), BF16)] + [pltpu.VMEM((4, IN_BLK, 2048), BF16)] * 3 + [pltpu.VMEM((2, IN_BLK, 2048), F32)]
    scratch += [pltpu.VMEM((GROUP, 8, 128), F32), pltpu.VMEM((8, 128), F32)]
    dma = pltpu.SemaphoreType.DMA
    scratch += [dma((7,)), dma((5,)), dma((5,)), dma((N_PARTS, RING)), dma((N_PARTS, RING)), dma((GROUP,)), dma((GROUP,)), dma((GROUP,)), dma((GROUP,)), dma((2,)), dma((3, 2)), dma((2, RING)), dma((2, RING)), dma((2, RING)), dma((2, RING)), dma((3, 4)), dma((2,)), dma((10,))]
    return pl.pallas_call(
        grad_kernel,
        out_shape=(jax.ShapeDtypeStruct((TOK, 2048), BF16), jax.ShapeDtypeStruct((GROUP * TOK, 2048), BF16), jax.ShapeDtypeStruct((GROUP * TOK, 2048), F32), jax.ShapeDtypeStruct((128, 2048), F32), jax.ShapeDtypeStruct((128, 3072), F32), jax.ShapeDtypeStruct((128, D_DOWN), F32), jax.ShapeDtypeStruct((32, D_UP), F32), jax.ShapeDtypeStruct((8, 128), F32)),
        in_specs=[ANY] * 13 + [pl.BlockSpec(memory_space=pltpu.VMEM)], out_specs=(ANY,) * 8, scratch_shapes=scratch,
        compiler_params=pltpu.CompilerParams(collective_id=1, has_side_effects=True, vmem_limit_bytes=63 * 1024 * 1024),
        cost_estimate=pl.CostEstimate(flops=8 * 10**9, bytes_accessed=20 * 10**6, transcendentals=0), name='grad_shards',
    )(mix, dy_all, nrm_t, dd, dq, lat_t, du, small, rows, weights, last_cols, dn, picked, gain)


W_SHARDS = ((32, 4096), (128, 576), (128, 896))
HALF_TOK = TOK // 2


def spread_kernel(n_w, *refs):
    mask, rows_h = refs[0:2]
    srcs = refs[2:2 + n_w]
    got_h = refs[2 + n_w]
    outs = refs[3 + n_w:3 + 2 * n_w]
    stage = refs[3 + 2 * n_w:3 + 3 * n_w]
    own, mate, way0, way1 = refs[3 + 3 * n_w:7 + 3 * n_w]
    in_sem, own_sem, s_sem, r_sem, ps_sem, pr_sem, os_sem, or_sem, xs_sem, xr_sem, ts_sem, tr_sem, h_in, m_s, m_r, hs_sem, hr_sem, out_sem = refs[7 + 3 * n_w:]
    me, core, pos = place()
    twin = lax.axis_index('dp')
    partner = me + 1 - 2 * core
    barrier = pltpu.get_barrier_semaphore()
    peers = (at_pos(pos + 1, core), at_pos(pos + 7, core))
    for peer in peers + (partner,):
        pl.semaphore_signal(barrier, inc=1, device_id={'fsdp': peer}, device_id_type=MESH)
    pl.semaphore_signal(barrier, inc=1, device_id={'dp': 1 - twin}, device_id_type=MESH)
    pl.semaphore_wait(barrier, 4)
    loads = []
    for i in range(n_w):
        cp = pltpu.make_async_copy(srcs[i], stage[i], in_sem.at[i])
        cp.start()
        loads.append(cp)

    def row_load(q):
        return pltpu.make_async_copy(rows_h.at[at_pos(q, core)], own.at[q], h_in.at[q])

    def row_share(q):
        return pltpu.make_async_remote_copy(rows_h.at[at_pos(q, 1 - core)], mate.at[q], m_s.at[q], m_r.at[q],
                                            device_id={'fsdp': partner}, device_id_type=MESH)
    for j in (7, 1, 6, 2, 5, 3, 4, 0):
        row_share((pos + j) % RING).start()
        row_load((pos + j) % RING).start()

    def where(i, way, source, side):
        rows = W_SHARDS[i][0]
        part = rows // 4
        return outs[i].at[pl.ds(pl.multiple_of(source * rows + side * 2 * part + way * part, part), part), :]

    def whole(i):
        rows = W_SHARDS[i][0]
        return outs[i].at[pl.ds(pl.multiple_of(me * rows, rows), rows), :]

    def origin(way, step):
        return at_pos(pos + 8 - step + way * 2 * step, core)

    def hop(i, way, step, src=None):
        spot = where(i, way, origin(way, step), twin)
        return pltpu.make_async_remote_copy(spot if src is None else src, spot, s_sem.at[i, way, step], r_sem.at[i, way, step + 1],
                                            device_id={'fsdp': peers[way]}, device_id_type=MESH)

    def arrive(i, way, step):
        spot = where(i, way, origin(way, step), twin)
        return pltpu.make_async_remote_copy(spot, spot, s_sem.at[i, way, step], r_sem.at[i, way, step],
                                            device_id={'fsdp': peers[way]}, device_id_type=MESH)

    def share(i, way, step):
        spot = where(i, way, origin(way, step), twin)
        return pltpu.make_async_remote_copy(spot, spot, ps_sem.at[i, way, step], pr_sem.at[i, way, step],
                                            device_id={'fsdp': partner}, device_id_type=MESH)

    def share_own(i):
        return pltpu.make_async_remote_copy(stage[i], whole(i), os_sem.at[i], or_sem.at[i], device_id={'fsdp': partner}, device_id_type=MESH)

    def to_twin(i, way, step):
        spot = where(i, way, origin(way, step), twin)
        return pltpu.make_async_remote_copy(spot, spot, xs_sem.at[i, way, step], xr_sem.at[i, way, step],
                                            device_id={'dp': 1 - twin}, device_id_type=MESH)

    def share_twin(i, way, step):
        spot = where(i, way, origin(way, step), 1 - twin)
        return pltpu.make_async_remote_copy(spot, spot, ts_sem.at[i, way, step], tr_sem.at[i, way, step],
                                            device_id={'fsdp': partner}, device_id_type=MESH)
    ways = (way0, way1)

    def row_hop(way, step):
        return pltpu.make_async_remote_copy(ways[way].at[step], ways[way].at[step + 1], hs_sem.at[way, step], hr_sem.at[way, step + 1],
                                            device_id={'fsdp': peers[way]}, device_id_type=MESH)

    def fill(way, step, first):
        q = (pos + 7 - step + way * (2 * step + 2)) % RING
        chip = chip_at(q)
        for c in range(0, HALF_TOK, 48):
            lo = way * HALF_TOK + c
            mine, theirs = mask[0, chip, lo:lo + 48, :], mask[1, chip, lo:lo + 48, :]
            for w in range(0, 2048, 128):
                part = own[q, lo:lo + 48, w:w + 128] * mine + mate[q, lo:lo + 48, w:w + 128] * theirs
                if not first:
                    part = part + ways[way][step, c:c + 48, w:w + 128]
                ways[way][step, c:c + 48, w:w + 128] = part

    kept = []
    for i in range(n_w):
        loads[i].wait()
        part = W_SHARDS[i][0] // 4
        for way in range(2):
            hop(i, way, 0, stage[i].at[pl.ds(pl.multiple_of(twin * 2 * part + way * part, part), part), :]).start()
        share_own(i).start()
        cp = pltpu.make_async_copy(stage[i], whole(i), own_sem.at[i])
        cp.start()
        kept.append(cp)
    for j in (7, 1, 6, 2, 5, 3, 4, 0):
        row_load((pos + j) % RING).wait()
        row_share((pos + j) % RING).wait_recv()
        if j in (7, 1):
            way = 0 if j == 7 else 1
            fill(way, 0, True)
            row_hop(way, 0).start()

    @pl.loop(1, RING)
    def _(step):
        for i in range(n_w):
            for way in range(2):
                arrive(i, way, step).wait_recv()

                @pl.when(step < RING - 1)
                def _():
                    hop(i, way, step).start()
                share(i, way, step).start()
                to_twin(i, way, step).start()
        for way in range(2):
            row_hop(way, step - 1).wait_recv()
            fill(way, step, False)

            @pl.when(step < RING - 1)
            def _():
                row_hop(way, step).start()

        @pl.when(step > 1)
        def _():
            for i in range(n_w):
                for way in range(2):
                    to_twin(i, way, step - 1).wait_recv()
                    share_twin(i, way, step - 1).start()

    for i in range(n_w):
        for way in range(2):
            to_twin(i, way, RING - 1).wait_recv()
            share_twin(i, way, RING - 1).start()
    for way in range(2):
        cp = pltpu.make_async_copy(ways[way].at[RING - 1], got_h.at[way * HALF_TOK:(way + 1) * HALF_TOK, :], out_sem.at[way])
        cp.start()
        kept.append(cp)
    for cp in kept:
        cp.wait()

    @pl.loop(0, RING)
    def _(step):
        row_share(step).wait_send()

        @pl.when(step < RING - 1)
        def _():
            for way in range(2):
                row_hop(way, step).wait_send()
        for i in range(n_w):
            for way in range(2):
                @pl.when(step < RING - 1)
                def _():
                    hop(i, way, step).wait_send()

                @pl.when(step > 0)
                def _():
                    share(i, way, step).wait()
                    to_twin(i, way, step).wait_send()
                    share_twin(i, way, step).wait()
    for i in range(n_w):
        share_own(i).wait()


def spread(mask, rows, shards):
    dma = pltpu.SemaphoreType.DMA
    n_w = len(shards)
    return pl.pallas_call(
        lambda *refs: spread_kernel(n_w, *refs),
        out_shape=(jax.ShapeDtypeStruct((TOK, 2048), BF16),) + tuple(jax.ShapeDtypeStruct((GROUP * r, w), BF16) for r, w in W_SHARDS),
        in_specs=[pl.BlockSpec(memory_space=pltpu.VMEM)] + [ANY] * (n_w + 1), out_specs=(ANY,) * (n_w + 1),
        scratch_shapes=[pltpu.VMEM(s, BF16) for s in W_SHARDS] + [pltpu.VMEM((RING, TOK, 2048), BF16)] * 2 + [pltpu.VMEM((RING, HALF_TOK, 2048), BF16)] * 2
        + [dma((n_w,)), dma((n_w,))] + [dma((n_w, 2, RING))] * 4 + [dma((n_w,))] * 2 + [dma((n_w, 2, RING))] * 4 + [dma((RING,)) for _ in range(3)] + [dma((2, RING)) for _ in range(2)] + [dma((2,))],
        compiler_params=pltpu.CompilerParams(collective_id=2, has_side_effects=True, vmem_limit_bytes=60 * 1024 * 1024),
        cost_estimate=pl.CostEstimate(flops=8 * 10**9, bytes_accessed=27 * 10**6, transcendentals=0), name='spread',
    )(mask, rows, *shards)
ROW_BLK = 256
SUB = 144
UNROLL = 4
OUT_SLOTS = 4


def table_kernel(starts, toks, rows, flags, small, grad_h, *refs):
    passed, out_h, given, gain_out, kv_out = refs[0:5], refs[5], refs[6:11], refs[11], refs[12]
    grad, acc, ob, nil, in_sem, out_sem = refs[13:19]
    hold, cut, ride_in, ride_out = refs[19:24], refs[24], refs[25], refs[26]
    boards = [pltpu.make_async_copy(src, dst, ride_in.at[i]) for i, (src, dst) in enumerate(zip(passed, hold))]
    leaves = [pltpu.make_async_copy(cut if i == 2 else src, dst, ride_out.at[i]) for i, (src, dst) in enumerate(zip(hold, given))]
    for cp in boards:
        cp.start()
    gain_out[...] = small[0:1, :]
    kv_out[...] = small[1:2, 0:32]
    n_in = GROUP * TOK // SUB
    n_out = out_h.shape[0] // ROW_BLK

    def load(blk):
        span = pl.ds(pl.multiple_of(blk * SUB, SUB), SUB)
        return pltpu.make_async_copy(grad_h.at[span, :], grad.at[span, :], in_sem)

    @pl.loop(0, n_in)
    def _(blk):
        @pl.when(flags[blk] > 0)
        def _():
            load(blk).start()
    nil[...] = jnp.zeros_like(nil)
    acc[...] = jnp.zeros_like(acc)

    @pl.loop(0, n_in)
    def _(blk):
        @pl.when(flags[blk] > 0)
        def _():
            load(blk).wait()
    for cp in boards:
        cp.wait()
    cut[...] = hold[2][...].T[0:576, :]
    for cp in leaves:
        cp.start()

    def store(blk, src):
        return pltpu.make_async_copy(src, out_h.at[pl.ds(pl.multiple_of(blk * ROW_BLK, ROW_BLK), ROW_BLK), :], out_sem.at[blk % OUT_SLOTS])
    @pl.loop(0, n_out)
    def _(blk):
        first, last = starts[blk], starts[blk + 1]
        slot = blk % OUT_SLOTS

        @pl.when(blk >= OUT_SLOTS)
        def _():
            store(blk - OUT_SLOTS, nil).wait()

        @pl.when(first == last)
        def _():
            store(blk, nil).start()

        @pl.when(first < last)
        def _():
            def add(k):
                acc[pl.ds(rows[k], 1), :] += grad[pl.ds(toks[k], 1), :]
            quads = (last - first) // UNROLL

            @pl.loop(0, quads)
            def _(i):
                for j in range(UNROLL):
                    add(first + i * UNROLL + j)

            @pl.loop(first + quads * UNROLL, last)
            def _(k):
                add(k)
            @pl.loop(0, ROW_BLK // 32)
            def _(r):
                here = pl.ds(pl.multiple_of(r * 32, 32), 32)
                ob[slot, here, :] = acc[here, :].astype(BF16)
                acc[here, :] = jnp.zeros((32, 2048), F32)
            store(blk, ob.at[slot]).start()
    for blk in range(n_out - OUT_SLOTS, n_out):
        store(blk, nil).wait()
    for cp in leaves:
        cp.wait()


def table_grad(starts, toks, rows, flags, small, row_grads, vocab_dev, passed):
    smem = pl.BlockSpec(memory_space=pltpu.SMEM)
    vmem = pl.BlockSpec(memory_space=pltpu.VMEM)
    dma = pltpu.SemaphoreType.DMA
    shapes = [jax.ShapeDtypeStruct((vocab_dev, 2048), BF16)] + [jax.ShapeDtypeStruct((576, 128) if i == 2 else p.shape, p.dtype) for i, p in enumerate(passed)]
    shapes += [jax.ShapeDtypeStruct((1, 128), F32), jax.ShapeDtypeStruct((1, 32), F32)]
    return pl.pallas_call(
        table_kernel, out_shape=tuple(shapes),
        in_specs=[smem] * 4 + [vmem] + [ANY] * 6, out_specs=(ANY,) * 6 + (vmem,) * 2,
        scratch_shapes=[pltpu.VMEM((GROUP * TOK, 2048), F32)]
        + [pltpu.VMEM((ROW_BLK, 2048), F32), pltpu.VMEM((OUT_SLOTS, ROW_BLK, 2048), BF16), pltpu.VMEM((ROW_BLK, 2048), BF16), dma, dma((OUT_SLOTS,))]
        + [pltpu.VMEM(p.shape, p.dtype) for p in passed] + [pltpu.VMEM((576, 128), F32), dma((5,)), dma((5,))],
        compiler_params=pltpu.CompilerParams(vmem_limit_bytes=63 * 1024 * 1024),
        cost_estimate=pl.CostEstimate(flops=10**9, bytes_accessed=90 * 10**6, transcendentals=0), name='table_grad',
    )(starts, toks, rows, flags, small, row_grads, *passed)


def small_kernel(src, out, loc_sem, s_sem, r_sem):
    me = lax.axis_index('fsdp')
    meet_all(me)
    own = pltpu.make_async_copy(src, out.at[me], loc_sem)
    own.start()

    def send(step):
        return pltpu.make_async_remote_copy(src, out.at[me], s_sem.at[step], r_sem.at[step],
                                            device_id={'fsdp': (me + step) % GROUP}, device_id_type=MESH)
    for step in range(1, GROUP):
        send(step).start()
    for step in range(1, GROUP):
        send(step).wait()
    own.wait()


def small_gather(tile):
    dma = pltpu.SemaphoreType.DMA
    return pl.pallas_call(
        small_kernel, out_shape=jax.ShapeDtypeStruct((GROUP, 8, 128), F32),
        in_specs=[pl.BlockSpec(memory_space=pltpu.VMEM)], out_specs=pl.BlockSpec(memory_space=pltpu.VMEM),
        scratch_shapes=[dma, dma((GROUP,)), dma((GROUP,))],
        compiler_params=pltpu.CompilerParams(collective_id=0, has_side_effects=True),
        cost_estimate=pl.CostEstimate(flops=10**7, bytes_accessed=10**5, transcendentals=0), name='small_gather',
    )(tile)


def blank(shape, dtype):
    return pl.pallas_call(lambda out: None, out_shape=jax.ShapeDtypeStruct(shape, dtype), out_specs=ANY, name='blank')()


def block_step(rows_f32, grad_rows, full_weights, seq_count):
    gain_vec, w_query, w_kv_down, kv_gain, w_kv_up, w_out = full_weights
    kv_rank = kv_gain.shape[0]
    tok_count = rows_f32.shape[0]
    seq_len = tok_count // seq_count
    normed, norm_pull = jax.vjp(rms_scale, rows_f32, gain_vec)
    q_proj = jnp.dot(normed, w_query, preferred_element_type=jnp.float32).astype(jnp.bfloat16)
    kv_down = jnp.dot(normed, w_kv_down, preferred_element_type=jnp.float32).astype(jnp.bfloat16)
    latent, latent_pull = jax.vjp(rms_scale, kv_down[:, :kv_rank], kv_gain)
    kv_up = jnp.dot(latent, w_kv_up, preferred_element_type=jnp.float32).astype(jnp.bfloat16)
    attn_mix, attn_pull = jax.vjp(attend_local, q_proj.reshape(seq_count, seq_len, -1, NOPE_DIM + ROPE_DIM), kv_down[:, kv_rank:].reshape(seq_count, seq_len, ROPE_DIM), kv_up.reshape(seq_count, seq_len, -1, NOPE_DIM + VALUE_DIM))
    mix_rows = attn_mix.reshape(tok_count, -1)
    d_mix = lax.dot_general(grad_rows[:, :WO_CUT], w_out[0], COL_DIMS, preferred_element_type=jnp.float32)
    d_mix = (d_mix + lax.dot_general(grad_rows[:, WO_CUT:], w_out[1], COL_DIMS, preferred_element_type=jnp.float32)).astype(jnp.bfloat16)
    d_query, d_pe, d_up = attn_pull(d_mix.reshape(attn_mix.shape))
    d_query = d_query.reshape(tok_count, -1)
    d_up = d_up.reshape(tok_count, -1)
    d_latent = lax.dot_general(d_up, w_kv_up, COL_DIMS, preferred_element_type=jnp.float32).astype(jnp.bfloat16)
    d_ckv, d_kv_gain = latent_pull(d_latent)
    d_down = jnp.concatenate([d_ckv, d_pe.reshape(tok_count, ROPE_DIM)], axis=1)
    d_normed = lax.dot_general(d_query, w_query, COL_DIMS, preferred_element_type=jnp.float32)
    d_normed = d_normed + lax.dot_general(d_down, w_kv_down, COL_DIMS, preferred_element_type=jnp.float32)
    d_normed = d_normed.astype(jnp.bfloat16)
    _, d_gain = norm_pull(d_normed)
    return d_normed, normed, mix_rows, latent, d_query, d_down, d_up, d_gain, d_kv_gain


def solution(mesh):
    tok_spec = P(('dp', 'fsdp'), None)
    seq_spec = P(('dp', 'fsdp'), None, None)
    part_vec = P(('dp', 'fsdp'))
    vec_spec = P('fsdp')
    mat_spec = P('fsdp', None)

    def device_step(tok_ids, grad_out, emb_table, norm_gain, w_query, w_kv_down, kv_gain, w_kv_up, w_out):
        seq_count, seq_len = tok_ids.shape
        vocab_dev, d_model = emb_table.shape
        tok_count = seq_count * seq_len
        me = lax.axis_index('fsdp')
        grad_rows = grad_out.reshape(tok_count, d_model)
        bundle = lax.all_gather(jnp.concatenate([w_query, w_out[:, :WO_CUT]], axis=1), 'fsdp', tiled=True)
        fill = lambda rows: jnp.pad(rows, ((0, 0), (0, 128 - rows.shape[1])))
        tile = jnp.concatenate([fill(tok_ids.astype(F32)), norm_gain.astype(F32).reshape(1, 128), fill(kv_gain.astype(F32).reshape(1, 32)), jnp.zeros((3, 128), F32)], axis=0)
        table = small_gather(tile)
        all_ids = table[:, :seq_count, :seq_len].reshape(GROUP, tok_count).astype(jnp.int32)
        gain_full = table[:, 3, :].reshape(-1)
        kv_gain_full = table[:, 4, :32].reshape(-1)

        owner = all_ids // vocab_dev
        mine = (owner == me)
        local = all_ids - me * vocab_dev
        stamp = jnp.arange(GROUP * tok_count).reshape(GROUP, tok_count) * ROW_BLK
        keys = lax.sort(jnp.where(mine, (local // ROW_BLK) * (8192 * ROW_BLK) + stamp + local % ROW_BLK, 2**30).reshape(-1))
        starts = jnp.sum((mine & (local < ROW_BLK * jnp.arange(vocab_dev // ROW_BLK + 1)[:, None, None])).astype(jnp.int32), axis=(1, 2))
        flags = jnp.sum(mine.reshape(-1, SUB).astype(jnp.int32), axis=1)
        picked = jnp.take(emb_table, jnp.where(mine, local, 0).reshape(-1), axis=0, mode='clip')
        core = me % 2
        near = lax.dynamic_index_in_dim(owner.reshape(RING, 2, tok_count), core, 1, keepdims=False)
        mask = jnp.stack([near == me, near == me + 1 - 2 * core]).astype(BF16)
        mask = jnp.broadcast_to(mask[..., None], (2, RING, tok_count, 128))
        picked, keys, starts, flags, w_kv_down = lax.optimization_barrier((picked, keys, starts, flags, w_kv_down))
        tok_rows, full_kvb, full_kva, wo_last = spread(mask, picked.reshape(GROUP, tok_count, d_model), (w_kv_up, w_kv_down, w_out[:, WO_CUT:]))
        full_wq, full_wo = bundle[:, :3072], (bundle[:, 3072:], wo_last)
        tok_rows, grad_rows = lax.optimization_barrier((tok_rows, grad_rows))
        all_dy = lax.all_gather(grad_rows, 'fsdp', tiled=True)
        d_normed, normed, mix, latent, d_query, d_down, d_up, d_gain, d_kv_gain = block_step(
            tok_rows.astype(F32), grad_rows, (gain_full, full_wq, full_kva, kv_gain_full, full_kvb, full_wo), seq_count)
        small = jnp.concatenate([d_gain.reshape(GROUP, 1, 128), jnp.pad(d_kv_gain.reshape(GROUP, 1, 32), ((0, 0), (0, 0), (0, 96))), jnp.zeros((GROUP, 6, 128), F32)], axis=1)
        block_out, _, row_grads, g_out, g_query, g_down, g_up, g_small = grad_shards(mix, all_dy, normed.T, jnp.pad(d_down, ((0, 0), (0, D_DOWN - d_down.shape[1]))), d_query, latent.T, d_up, small, tok_rows, bundle, wo_last, d_normed, picked, gain_full.reshape(1, -1))
        grad_table, block_out, g_query, g_down, g_up, g_out, g_gain, g_kv_gain = table_grad(
            starts, (keys // ROW_BLK) & 8191, keys & (ROW_BLK - 1), flags, g_small, row_grads, vocab_dev,
            (block_out, g_query, g_down, g_up, g_out))
        return (block_out.reshape(seq_count, seq_len, d_model), grad_table, g_gain.reshape(-1), g_query, g_down.T, g_kv_gain.reshape(-1), g_up, g_out)

    return jax.shard_map(device_step, mesh=mesh, in_specs=(tok_spec, seq_spec, mat_spec, vec_spec, mat_spec, mat_spec, vec_spec, mat_spec, mat_spec), out_specs=(seq_spec, tok_spec, part_vec, tok_spec, tok_spec, part_vec, tok_spec, tok_spec), check_vma=False)
```

```python
import math
import jax
import jax.numpy as jnp
from jax import lax
from jax.sharding import PartitionSpec as P
from jax.experimental import pallas as pl
from jax.experimental.pallas import tpu as pltpu

NOPE_DIM = 128
ROPE_DIM = 64
VALUE_DIM = 128
ROPE_THETA = 50000.0
RMS_EPS = 1e-6
ATTN_SCALE = (NOPE_DIM + ROPE_DIM) ** -0.5 * (0.1 * math.log(32.0) + 1.0) ** 2
ROW_DIMS = (((0,), (0,)), ((), ()))
COL_DIMS = (((1,), (1,)), ((), ()))


def rms_scale(in_vals, gain_vec):
    vals_f32 = in_vals.astype(jnp.float32)
    inv_rms = lax.rsqrt(jnp.mean(vals_f32 * vals_f32, axis=-1, keepdims=True) + RMS_EPS)
    return (vals_f32 * inv_rms * gain_vec).astype(jnp.bfloat16)


def rope_tables(seq_len):
    positions = jnp.arange(seq_len, dtype=jnp.float32)
    inv_freq = ROPE_THETA ** (-2.0 * jnp.arange(ROPE_DIM // 2, dtype=jnp.float32) / ROPE_DIM)
    rot_angle = positions[:, None] * inv_freq[None, :]
    rot_angle = jnp.concatenate([rot_angle, rot_angle], axis=-1)
    return jnp.cos(rot_angle), jnp.sin(rot_angle)


def apply_rope(in_vals, cos_tab, sin_tab):
    half_dim = ROPE_DIM // 2
    vals_f32 = in_vals.astype(jnp.float32)
    turned = jnp.concatenate([-vals_f32[..., half_dim:], vals_f32[..., :half_dim]], axis=-1)
    return (vals_f32 * cos_tab + turned * sin_tab).astype(jnp.bfloat16)


def attend_local(q_proj, pe_raw, kv_up):
    seq_len = q_proj.shape[1]
    cos_tab, sin_tab = rope_tables(seq_len)
    q_rot = apply_rope(q_proj[..., NOPE_DIM:], cos_tab[:, None, :], sin_tab[:, None, :])
    k_rot = apply_rope(pe_raw, cos_tab, sin_tab)
    scores = jnp.einsum('bshd,bthd->bhst', q_proj[..., :NOPE_DIM], kv_up[..., :NOPE_DIM], preferred_element_type=jnp.float32)
    scores = scores + jnp.einsum('bshd,btd->bhst', q_rot, k_rot, preferred_element_type=jnp.float32)
    positions = jnp.arange(seq_len)
    causal = positions[:, None] >= positions[None, :]
    scores = jnp.where(causal, scores * ATTN_SCALE, -1e30)
    attn_probs = jax.nn.softmax(scores, axis=-1).astype(jnp.bfloat16)
    attn_mix = jnp.einsum('bhst,bthd->bshd', attn_probs, kv_up[..., NOPE_DIM:], preferred_element_type=jnp.float32)
    return attn_mix.astype(jnp.bfloat16)


F32, BF16 = jnp.float32, jnp.bfloat16
MESH = pl.DeviceIdType.MESH
ANY = pl.BlockSpec(memory_space=pl.ANY)
RING = 8
GROUP = 16

def chip_at(pos):
    side = pos // 4
    return (pos + side * (7 - 2 * pos)) * 2 + side

def place():
    me = lax.axis_index('fsdp')
    core = me % 2
    chip = me // 2
    side = chip % 2
    zz = chip // 2
    return me, core, zz + side * (7 - 2 * zz)

def at_pos(pos, core):
    return chip_at(pos % RING) * 2 + core

def meet_all(me):
    barrier = pltpu.get_barrier_semaphore()
    for step in range(1, GROUP):
        pl.semaphore_signal(barrier, inc=1, device_id={'fsdp': (me + step) % GROUP}, device_id_type=MESH)
    pl.semaphore_wait(barrier, GROUP - 1)

TOK = 288
IN_BLK = 144
PIECE = 16
D_OUT, D_CAT, D_UP, D_DOWN = 2048, 3712, 4096, 640
WO_COL = 3072
WO_CUT = 1152
CUT = 1792
PARTS = (('u', 0, 0, 2304), ('u', 1, 2304, 1792), ('n', 0, 0, 896), ('n', 1, 1792, 1024), ('n', 0, 896, 896), ('n', 1, 2816, 896))
N_PARTS = len(PARTS)
ROWS = {'n': 128, 'u': 32}

def col_tiles(width):
    step = 512
    return [(c, min(step, width - c)) for c in range(0, width, step)]

def grad_kernel(mix_h, dy_h, nrm_h, dd_h, dq_h, lat_h, du_h, sm_h, h0_h, wo_h, wl_h, dn_h, h_h, gain, y_h, dn_all, grad_h, go_h, gq_h, gd_h, gu_h, gs_h,
                mix, dy, go, nrm, cat, lat, du, b0, b1, b2, b3, b4, b5, mixf, h0, wo, yacc, yv, own_dn, fdn, fdy, fh, fo, smr, ssum, loc_sem, xs_sem, xr_sem, s_sem, r_sem, ms_sem, mr_sem, cs_sem, cr_sem, dy_sem, y_sem, ns_sem, nr_sem, np_sem, nq_sem, f_sem, fo_sem, out_sem):
    me, core, pos = place()
    partner = me + 1 - 2 * core
    meet_all(me)
    acts = ((lat_h, lat), (du_h, du), (nrm_h, nrm), (dd_h, cat.at[:, :, 0:D_DOWN]), (dq_h, cat.at[:, :, D_DOWN:D_CAT]))
    local, cross = [], []
    for i, (src, dst) in enumerate(acts):
        cp = pltpu.make_async_copy(src, dst.at[core], loc_sem.at[i])
        cp.start()
        local.append(cp)
        rc = pltpu.make_async_remote_copy(src, dst.at[core], xs_sem.at[i], xr_sem.at[i], device_id={'fsdp': partner}, device_id_type=MESH)
        rc.start()
        cross.append(rc)
    peers = (at_pos(pos + 1, core), at_pos(pos + 7, core))

    def unit(dev, way):
        return pl.ds(pl.multiple_of(dev * TOK + way * IN_BLK, PIECE), IN_BLK)

    def origin(way, step):
        return at_pos(pos + 8 - step + way * 2 * step, core)

    def dn_hop(way, step, src=None):
        spot = dn_all.at[unit(origin(way, step), way), :]
        return pltpu.make_async_remote_copy(spot if src is None else src, spot, ns_sem.at[way, step], nr_sem.at[way, step + 1],
                                            device_id={'fsdp': peers[way]}, device_id_type=MESH)

    def dn_arrive(way, step):
        spot = dn_all.at[unit(origin(way, step), way), :]
        return pltpu.make_async_remote_copy(spot, spot, ns_sem.at[way, step], nr_sem.at[way, step],
                                            device_id={'fsdp': peers[way]}, device_id_type=MESH)

    def dn_share(way, step, src=None):
        spot = dn_all.at[unit(origin(way, step), way), :]
        return pltpu.make_async_remote_copy(spot if src is None else src, spot, np_sem.at[way, step], nq_sem.at[way, step],
                                            device_id={'fsdp': partner}, device_id_type=MESH)
    own_load = pltpu.make_async_copy(dn_h, own_dn, f_sem.at[0, 0])
    own_load.start()
    own_load.wait()
    for way in range(2):
        src = own_dn.at[way * IN_BLK:(way + 1) * IN_BLK, :]
        dn_hop(way, 0, src).start()
        dn_share(way, 0, src).start()
        pltpu.make_async_copy(src, dn_all.at[unit(me, way), :], fo_sem.at[way]).start()

    def row_grads(step):
        jobs = [(at_pos(pos + 8 - step + way * 2 * step, c), way) for way in range(2) for c in (core, 1 - core)]

        def fetch(slot):
            dev, way = jobs[slot]
            return [pltpu.make_async_copy(src.at[unit(dev, way), :], dst.at[slot], f_sem.at[i, slot])
                    for i, (src, dst) in enumerate(((dn_all, fdn), (dy_h, fdy), (h_h, fh)))]

        def put(slot):
            dev, way = jobs[slot]
            return pltpu.make_async_copy(fo.at[slot % 2], grad_h.at[unit(dev, way), :], fo_sem.at[slot % 2])
        for way in range(2):
            dn_share(way, step).wait_recv()
        for slot in range(4):
            for cp in fetch(slot):
                cp.start()

        for slot in range(4):
            for cp in fetch(slot):
                cp.wait()
            if slot >= 2:
                put(slot - 2).wait()

            @pl.loop(0, IN_BLK // 48)
            def _(g):
                r0 = pl.multiple_of(g * 48, PIECE)

                def tile(ref, p, c):
                    return ref[slot, pl.ds(r0 + p, PIECE), c:c + 128].astype(F32)
                scale = []
                for p in range(0, 48, PIECE):
                    sq = jnp.zeros((PIECE, 128), F32)
                    al = jnp.zeros((PIECE, 128), F32)
                    for c in range(0, 2048, 128):
                        h = tile(fh, p, c)
                        sq = sq + h * h
                        al = al + h * (tile(fdn, p, c) * gain[:, c:c + 128])
                    scale.append((jnp.sum(sq, axis=1, keepdims=True), jnp.sum(al, axis=1, keepdims=True)))
                for p, (sq, al) in zip(range(0, 48, PIECE), scale):
                    inv = lax.rsqrt(sq * (1.0 / 2048) + RMS_EPS)
                    coef = inv * inv * inv * (al * (1.0 / 2048))
                    for c in range(0, 2048, 128):
                        s = tile(fdn, p, c) * gain[:, c:c + 128]
                        fo[slot % 2, pl.ds(r0 + p, PIECE), c:c + 128] = tile(fdy, p, c) + inv * s - coef * tile(fh, p, c)
            put(slot).start()
        put(2).wait()
        put(3).wait()

    own_small = pltpu.make_async_copy(sm_h.at[me], smr.at[0], loc_sem.at[5])
    own_small.start()
    own_mix = pltpu.make_async_copy(mix_h.at[:, pl.ds(pl.multiple_of(me * 128, 128), 128)], mix.at[me], loc_sem.at[6])
    own_mix.start()
    smalls, mixes = [], []
    for i in range(1, GROUP):
        peer = (me + i) % GROUP
        rc = pltpu.make_async_remote_copy(sm_h.at[peer], smr.at[i], ms_sem.at[i], mr_sem.at[i], device_id={'fsdp': peer}, device_id_type=MESH)
        rc.start()
        smalls.append(rc)
    for i, (src, dst) in enumerate(((mix_h, mixf), (h0_h, h0))):
        pltpu.make_async_copy(src, dst, y_sem.at[2, i]).start()

    def wo_load(t):
        span = pl.ds(pl.multiple_of(t * 256, 256), 256)
        return [pltpu.make_async_copy(src, dst, y_sem.at[i, t % 2]) for i, (src, dst) in enumerate((
            (wo_h.at[span, WO_COL:WO_COL + WO_CUT], wo.at[t % 2, :, 0:WO_CUT]), (wl_h.at[span, :], wo.at[t % 2, :, WO_CUT:2048])))]
    for cp in wo_load(0):
        cp.start()
    bufs = (b0, b1, b2, b3, b4, b5)
    left_ops = {'n': (nrm, cat), 'u': (lat, du)}

    def mix_send(i):
        peer = (me + i) % GROUP
        return pltpu.make_async_remote_copy(mix_h.at[:, pl.ds(pl.multiple_of(peer * 128, 128), 128)], mix.at[me], cs_sem.at[i], cr_sem.at[i],
                                            device_id={'fsdp': peer}, device_id_type=MESH)

    def dy_load(blk):
        return pltpu.make_async_copy(dy_h.at[pl.ds(pl.multiple_of(blk * TOK, TOK), TOK), :], dy.at[blk % 2], dy_sem.at[blk % 2])

    def hop(p, step):
        return pltpu.make_async_remote_copy(bufs[p].at[step], bufs[p].at[step + 1], s_sem.at[p, step], r_sem.at[p, step + 1],
                                            device_id={'fsdp': peers[PARTS[p][1]]}, device_id_type=MESH)

    def work(p, step):
        kind, way, c0, width = PARTS[p]
        chip = chip_at((pos + 7 - step + way * (2 * step + 2)) % RING)
        lhs_ref, rhs_ref = left_ops[kind]
        rows = ROWS[kind]
        row = pl.multiple_of((chip * 2 + core) * rows, rows)
        lhs = [lhs_ref[b, pl.ds(row, rows), :] for b in range(2)]
        for c, w in col_tiles(width):
            part = sum(jnp.dot(lhs[b], rhs_ref[b, :, c0 + c:c0 + c + w], preferred_element_type=F32) for b in range(2))
            bufs[p][step, :, c:c + w] = bufs[p][step, :, c:c + w] + part

    for i in range(1, GROUP):
        mix_send(i).start()
    dy_load(0).start()
    go[...] = jnp.zeros_like(go)
    for p in range(N_PARTS):
        bufs[p][0] = jnp.zeros(bufs[p].shape[1:], F32)
    first_use = {0: (0, 1), 2: (2, 3, 4)}

    for way in range(2):
        pltpu.make_async_copy(own_dn.at[way * IN_BLK:(way + 1) * IN_BLK, :], dn_all.at[unit(me, way), :], fo_sem.at[way]).wait()

    @pl.loop(0, RING)
    def _(step):
        @pl.when(step > 0)
        def _():
            for way in range(2):
                dn_arrive(way, step).wait_recv()

                @pl.when(step < RING - 1)
                def _():
                    dn_hop(way, step).start()
                dn_share(way, step).start()

            @pl.loop(step - 1, step + step // (RING - 1))
            def _(done):
                row_grads(done)

        for p in range(N_PARTS):
            if p in first_use:
                @pl.when(step == 0)
                def _():
                    for i in first_use[p]:
                        local[i].wait()
                        cross[i].wait_recv()

            @pl.when(step > 0)
            def _():
                hop(p, step - 1).wait_recv()
            work(p, step)

            @pl.when(step < RING - 1)
            def _():
                hop(p, step).start()

        @pl.when(step == 0)
        def _():
            own_mix.wait()
            for i in range(1, GROUP):
                mix_send(i).wait()

        @pl.when((step > 0) & (step < 5))
        def _():
            @pl.loop(0, 4)
            def _(j):
                blk = (step - 1) * 4 + j
                dy_load(blk).wait()

                @pl.when(blk < GROUP - 1)
                def _():
                    dy_load(blk + 1).start()
                for c, w in col_tiles(2048):
                    go[:, c:c + w] += lax.dot_general(mix[blk], dy[blk % 2, :, c:c + w], (((0,), (0,)), ((), ())), preferred_element_type=F32)

        @pl.when(step == 5)
        def _():
            for i, (src, dst) in enumerate(((mix_h, mixf), (h0_h, h0))):
                pltpu.make_async_copy(src, dst, y_sem.at[2, i]).wait()

            yacc[...] = h0[...].astype(F32)

            @pl.loop(0, 8)
            def _(t):
                for cp in wo_load(t):
                    cp.wait()

                @pl.when(t < 7)
                def _():
                    for cp in wo_load(t + 1):
                        cp.start()

                @pl.loop(0, 4)
                def _(j):
                    here = pl.ds(pl.multiple_of(j * 512, 512), 512)
                    yacc[:, here] += jnp.dot(mixf[:, pl.ds(pl.multiple_of(t * 256, 256), 256)], wo[t % 2, :, here], preferred_element_type=F32)
            yv[...] = yacc[...].astype(BF16)

    last = RING - 1
    outs = []
    cp = pltpu.make_async_copy(go, go_h, out_sem.at[6])
    cp.start()
    outs.append(cp)
    cp = pltpu.make_async_copy(yv, y_h, out_sem.at[9])
    cp.start()
    outs.append(cp)
    targets = (((gu_h.at[:, 0:2304], 0, 2304),), ((gu_h.at[:, 2304:4096], 0, 1792),), ((gd_h, 0, 640), (gq_h.at[:, 0:256], 640, 896)),
               ((gq_h.at[:, 1152:2176], 0, 1024),), ((gq_h.at[:, 256:1152], 0, 896),), ((gq_h.at[:, 2176:3072], 0, 896),))
    for p in range(N_PARTS):
        for n, (dst, c0, c1) in enumerate(targets[p]):
            cp = pltpu.make_async_copy(bufs[p].at[last, :, c0:c1], dst, out_sem.at[p + 6 * n])
            cp.start()
            outs.append(cp)
    own_small.wait()
    for rc in smalls:
        rc.wait()
    ssum[...] = jnp.sum(smr[...], axis=0)
    cp = pltpu.make_async_copy(ssum, gs_h, out_sem.at[7])
    cp.start()
    outs.append(cp)
    for rc in cross:
        rc.wait_send()
    for p in range(N_PARTS):
        @pl.loop(0, last)
        def _(step):
            hop(p, step).wait_send()

    @pl.loop(0, RING)
    def _(step):
        for way in range(2):
            dn_share(way, step).wait_send()

            @pl.when(step < last)
            def _():
                dn_hop(way, step).wait_send()
    for cp in outs:
        cp.wait()


def grad_shards(mix, dy_all, nrm_t, dd, dq, lat_t, du, small, rows, weights, last_cols, dn, picked, gain):
    shapes = [(ROWS[k], RING, w) for k, _, _, w in PARTS]
    scratch = [pltpu.VMEM((GROUP, TOK, 128), BF16), pltpu.VMEM((2, TOK, 2048), BF16), pltpu.VMEM((128, 2048), F32), pltpu.VMEM((2, 2048, TOK), BF16),
               pltpu.VMEM((2, TOK, D_CAT), BF16), pltpu.VMEM((2, 512, TOK), BF16), pltpu.VMEM((2, TOK, D_UP), BF16)]
    scratch += [pltpu.VMEM((RING, r, w), F32) for r, _, w in shapes]
    scratch += [pltpu.VMEM((TOK, 2048), BF16), pltpu.VMEM((TOK, 2048), BF16), pltpu.VMEM((2, 256, 2048), BF16), pltpu.VMEM((TOK, 2048), F32), pltpu.VMEM((TOK, 2048), BF16)]
    scratch += [pltpu.VMEM((TOK, 2048), BF16)] + [pltpu.VMEM((4, IN_BLK, 2048), BF16)] * 3 + [pltpu.VMEM((2, IN_BLK, 2048), F32)]
    scratch += [pltpu.VMEM((GROUP, 8, 128), F32), pltpu.VMEM((8, 128), F32)]
    dma = pltpu.SemaphoreType.DMA
    scratch += [dma((7,)), dma((5,)), dma((5,)), dma((N_PARTS, RING)), dma((N_PARTS, RING)), dma((GROUP,)), dma((GROUP,)), dma((GROUP,)), dma((GROUP,)), dma((2,)), dma((3, 2)), dma((2, RING)), dma((2, RING)), dma((2, RING)), dma((2, RING)), dma((3, 4)), dma((2,)), dma((10,))]
    return pl.pallas_call(
        grad_kernel,
        out_shape=(jax.ShapeDtypeStruct((TOK, 2048), BF16), jax.ShapeDtypeStruct((GROUP * TOK, 2048), BF16), jax.ShapeDtypeStruct((GROUP * TOK, 2048), F32), jax.ShapeDtypeStruct((128, 2048), F32), jax.ShapeDtypeStruct((128, 3072), F32), jax.ShapeDtypeStruct((128, D_DOWN), F32), jax.ShapeDtypeStruct((32, D_UP), F32), jax.ShapeDtypeStruct((8, 128), F32)),
        in_specs=[ANY] * 13 + [pl.BlockSpec(memory_space=pltpu.VMEM)], out_specs=(ANY,) * 8, scratch_shapes=scratch,
        compiler_params=pltpu.CompilerParams(collective_id=1, has_side_effects=True, vmem_limit_bytes=63 * 1024 * 1024),
        cost_estimate=pl.CostEstimate(flops=8 * 10**9, bytes_accessed=20 * 10**6, transcendentals=0), name='grad_shards',
    )(mix, dy_all, nrm_t, dd, dq, lat_t, du, small, rows, weights, last_cols, dn, picked, gain)


W_SHARDS = ((32, 4096), (128, 576), (128, 896))
HALF_TOK = TOK // 2


def spread_kernel(n_w, *refs):
    mask, rows_h = refs[0:2]
    srcs = refs[2:2 + n_w]
    got_h = refs[2 + n_w]
    outs = refs[3 + n_w:3 + 2 * n_w]
    stage = refs[3 + 2 * n_w:3 + 3 * n_w]
    own, mate, way0, way1 = refs[3 + 3 * n_w:7 + 3 * n_w]
    in_sem, own_sem, s_sem, r_sem, ps_sem, pr_sem, os_sem, or_sem, xs_sem, xr_sem, ts_sem, tr_sem, h_in, m_s, m_r, hs_sem, hr_sem, out_sem = refs[7 + 3 * n_w:]
    me, core, pos = place()
    twin = lax.axis_index('dp')
    partner = me + 1 - 2 * core
    barrier = pltpu.get_barrier_semaphore()
    peers = (at_pos(pos + 1, core), at_pos(pos + 7, core))
    for peer in peers + (partner,):
        pl.semaphore_signal(barrier, inc=1, device_id={'fsdp': peer}, device_id_type=MESH)
    pl.semaphore_signal(barrier, inc=1, device_id={'dp': 1 - twin}, device_id_type=MESH)
    pl.semaphore_wait(barrier, 4)
    loads = []
    for i in range(n_w):
        cp = pltpu.make_async_copy(srcs[i], stage[i], in_sem.at[i])
        cp.start()
        loads.append(cp)

    def row_load(q):
        return pltpu.make_async_copy(rows_h.at[at_pos(q, core)], own.at[q], h_in.at[q])

    def row_share(q):
        return pltpu.make_async_remote_copy(rows_h.at[at_pos(q, 1 - core)], mate.at[q], m_s.at[q], m_r.at[q],
                                            device_id={'fsdp': partner}, device_id_type=MESH)
    for j in (7, 1, 6, 2, 5, 3, 4, 0):
        row_share((pos + j) % RING).start()
        row_load((pos + j) % RING).start()

    def where(i, way, source, side):
        rows = W_SHARDS[i][0]
        part = rows // 4
        return outs[i].at[pl.ds(pl.multiple_of(source * rows + side * 2 * part + way * part, part), part), :]

    def whole(i):
        rows = W_SHARDS[i][0]
        return outs[i].at[pl.ds(pl.multiple_of(me * rows, rows), rows), :]

    def origin(way, step):
        return at_pos(pos + 8 - step + way * 2 * step, core)

    def hop(i, way, step, src=None):
        spot = where(i, way, origin(way, step), twin)
        return pltpu.make_async_remote_copy(spot if src is None else src, spot, s_sem.at[i, way, step], r_sem.at[i, way, step + 1],
                                            device_id={'fsdp': peers[way]}, device_id_type=MESH)

    def arrive(i, way, step):
        spot = where(i, way, origin(way, step), twin)
        return pltpu.make_async_remote_copy(spot, spot, s_sem.at[i, way, step], r_sem.at[i, way, step],
                                            device_id={'fsdp': peers[way]}, device_id_type=MESH)

    def share(i, way, step):
        spot = where(i, way, origin(way, step), twin)
        return pltpu.make_async_remote_copy(spot, spot, ps_sem.at[i, way, step], pr_sem.at[i, way, step],
                                            device_id={'fsdp': partner}, device_id_type=MESH)

    def share_own(i):
        return pltpu.make_async_remote_copy(stage[i], whole(i), os_sem.at[i], or_sem.at[i], device_id={'fsdp': partner}, device_id_type=MESH)

    def to_twin(i, way, step):
        spot = where(i, way, origin(way, step), twin)
        return pltpu.make_async_remote_copy(spot, spot, xs_sem.at[i, way, step], xr_sem.at[i, way, step],
                                            device_id={'dp': 1 - twin}, device_id_type=MESH)

    def share_twin(i, way, step):
        spot = where(i, way, origin(way, step), 1 - twin)
        return pltpu.make_async_remote_copy(spot, spot, ts_sem.at[i, way, step], tr_sem.at[i, way, step],
                                            device_id={'fsdp': partner}, device_id_type=MESH)
    ways = (way0, way1)

    def row_hop(way, step):
        return pltpu.make_async_remote_copy(ways[way].at[step], ways[way].at[step + 1], hs_sem.at[way, step], hr_sem.at[way, step + 1],
                                            device_id={'fsdp': peers[way]}, device_id_type=MESH)

    def fill(way, step, first):
        q = (pos + 7 - step + way * (2 * step + 2)) % RING
        chip = chip_at(q)
        for c in range(0, HALF_TOK, 48):
            lo = way * HALF_TOK + c
            mine, theirs = mask[0, chip, lo:lo + 48, :], mask[1, chip, lo:lo + 48, :]
            for w in range(0, 2048, 128):
                part = own[q, lo:lo + 48, w:w + 128] * mine + mate[q, lo:lo + 48, w:w + 128] * theirs
                if not first:
                    part = part + ways[way][step, c:c + 48, w:w + 128]
                ways[way][step, c:c + 48, w:w + 128] = part

    kept = []
    for i in range(n_w):
        loads[i].wait()
        part = W_SHARDS[i][0] // 4
        for way in range(2):
            hop(i, way, 0, stage[i].at[pl.ds(pl.multiple_of(twin * 2 * part + way * part, part), part), :]).start()
        share_own(i).start()
        cp = pltpu.make_async_copy(stage[i], whole(i), own_sem.at[i])
        cp.start()
        kept.append(cp)
    for j in (7, 1, 6, 2, 5, 3, 4, 0):
        row_load((pos + j) % RING).wait()
        row_share((pos + j) % RING).wait_recv()
        if j in (7, 1):
            way = 0 if j == 7 else 1
            fill(way, 0, True)
            row_hop(way, 0).start()

    @pl.loop(1, RING)
    def _(step):
        for i in range(n_w):
            for way in range(2):
                arrive(i, way, step).wait_recv()

                @pl.when(step < RING - 1)
                def _():
                    hop(i, way, step).start()
                share(i, way, step).start()
                to_twin(i, way, step).start()
        for way in range(2):
            row_hop(way, step - 1).wait_recv()
            fill(way, step, False)

            @pl.when(step < RING - 1)
            def _():
                row_hop(way, step).start()

        @pl.when(step > 1)
        def _():
            for i in range(n_w):
                for way in range(2):
                    to_twin(i, way, step - 1).wait_recv()
                    share_twin(i, way, step - 1).start()

    for i in range(n_w):
        for way in range(2):
            to_twin(i, way, RING - 1).wait_recv()
            share_twin(i, way, RING - 1).start()
    for way in range(2):
        cp = pltpu.make_async_copy(ways[way].at[RING - 1], got_h.at[way * HALF_TOK:(way + 1) * HALF_TOK, :], out_sem.at[way])
        cp.start()
        kept.append(cp)
    for cp in kept:
        cp.wait()

    @pl.loop(0, RING)
    def _(step):
        row_share(step).wait_send()

        @pl.when(step < RING - 1)
        def _():
            for way in range(2):
                row_hop(way, step).wait_send()
        for i in range(n_w):
            for way in range(2):
                @pl.when(step < RING - 1)
                def _():
                    hop(i, way, step).wait_send()

                @pl.when(step > 0)
                def _():
                    share(i, way, step).wait()
                    to_twin(i, way, step).wait_send()
                    share_twin(i, way, step).wait()
    for i in range(n_w):
        share_own(i).wait()


def spread(mask, rows, shards):
    dma = pltpu.SemaphoreType.DMA
    n_w = len(shards)
    return pl.pallas_call(
        lambda *refs: spread_kernel(n_w, *refs),
        out_shape=(jax.ShapeDtypeStruct((TOK, 2048), BF16),) + tuple(jax.ShapeDtypeStruct((GROUP * r, w), BF16) for r, w in W_SHARDS),
        in_specs=[pl.BlockSpec(memory_space=pltpu.VMEM)] + [ANY] * (n_w + 1), out_specs=(ANY,) * (n_w + 1),
        scratch_shapes=[pltpu.VMEM(s, BF16) for s in W_SHARDS] + [pltpu.VMEM((RING, TOK, 2048), BF16)] * 2 + [pltpu.VMEM((RING, HALF_TOK, 2048), BF16)] * 2
        + [dma((n_w,)), dma((n_w,))] + [dma((n_w, 2, RING))] * 4 + [dma((n_w,))] * 2 + [dma((n_w, 2, RING))] * 4 + [dma((RING,)) for _ in range(3)] + [dma((2, RING)) for _ in range(2)] + [dma((2,))],
        compiler_params=pltpu.CompilerParams(collective_id=2, has_side_effects=True, vmem_limit_bytes=60 * 1024 * 1024),
        cost_estimate=pl.CostEstimate(flops=8 * 10**9, bytes_accessed=27 * 10**6, transcendentals=0), name='spread',
    )(mask, rows, *shards)
ROW_BLK = 64
SUB = 72
UNROLL = 4
IN_SLOTS = 6
OUT_SLOTS = 8


def table_kernel(starts, toks, rows, small, grad_h, *refs):
    passed, out_h, given, gain_out, kv_out = refs[0:5], refs[5], refs[6:11], refs[11], refs[12]
    acc, grad, ob, in_sem, out_sem = refs[13:18]
    hold, cut, ride_in, ride_out = refs[18:23], refs[23], refs[24], refs[25]
    n_in = GROUP * TOK // SUB
    n_out = out_h.shape[0] // ROW_BLK

    def load(blk):
        return pltpu.make_async_copy(grad_h.at[pl.ds(pl.multiple_of(blk * SUB, SUB), SUB), :], grad.at[blk % IN_SLOTS], in_sem.at[blk % IN_SLOTS])
    for blk in range(IN_SLOTS):
        load(blk).start()
    boards = [pltpu.make_async_copy(src, dst, ride_in.at[i]) for i, (src, dst) in enumerate(zip(passed, hold))]
    leaves = [pltpu.make_async_copy(cut if i == 2 else src, dst, ride_out.at[i]) for i, (src, dst) in enumerate(zip(hold, given))]
    for cp in boards:
        cp.start()
    gain_out[...] = small[0:1, :]
    kv_out[...] = small[1:2, 0:32]

    @pl.loop(0, out_h.shape[0] // 64)
    def _(i):
        acc[pl.ds(pl.multiple_of(i * 64, 64), 64), :] = jnp.zeros((64, 2048), F32)

    @pl.loop(0, n_in)
    def _(blk):
        first, last = starts[blk], starts[blk + 1]
        slot = blk % IN_SLOTS
        load(blk).wait()

        def add(k):
            acc[pl.ds(rows[k], 1), :] += grad[slot, pl.ds(toks[k] - blk * SUB, 1), :]
        quads = (last - first) // UNROLL

        @pl.loop(0, quads)
        def _(i):
            for j in range(UNROLL):
                add(first + i * UNROLL + j)

        @pl.loop(first + quads * UNROLL, last)
        def _(k):
            add(k)

        @pl.when(blk < n_in - IN_SLOTS)
        def _():
            load(blk + IN_SLOTS).start()
    for cp in boards:
        cp.wait()
    cut[...] = hold[2][...].T[0:576, :]
    for cp in leaves:
        cp.start()

    def store(blk):
        slot = blk % OUT_SLOTS
        return pltpu.make_async_copy(ob.at[slot], out_h.at[pl.ds(pl.multiple_of(blk * ROW_BLK, ROW_BLK), ROW_BLK), :], out_sem.at[slot])

    @pl.loop(0, n_out)
    def _(blk):
        @pl.when(blk >= OUT_SLOTS)
        def _():
            store(blk - OUT_SLOTS).wait()
        ob[blk % OUT_SLOTS] = acc[pl.ds(pl.multiple_of(blk * ROW_BLK, ROW_BLK), ROW_BLK), :].astype(BF16)
        store(blk).start()
    for blk in range(n_out - OUT_SLOTS, n_out):
        store(blk).wait()
    for cp in leaves:
        cp.wait()


def table_grad(starts, toks, rows, small, row_grads, vocab_dev, passed):
    smem = pl.BlockSpec(memory_space=pltpu.SMEM)
    vmem = pl.BlockSpec(memory_space=pltpu.VMEM)
    dma = pltpu.SemaphoreType.DMA
    shapes = [jax.ShapeDtypeStruct((vocab_dev, 2048), BF16)] + [jax.ShapeDtypeStruct((576, 128) if i == 2 else p.shape, p.dtype) for i, p in enumerate(passed)]
    shapes += [jax.ShapeDtypeStruct((1, 128), F32), jax.ShapeDtypeStruct((1, 32), F32)]
    return pl.pallas_call(
        table_kernel, out_shape=tuple(shapes),
        in_specs=[smem] * 3 + [vmem] + [ANY] * 6, out_specs=(ANY,) * 6 + (vmem,) * 2,
        scratch_shapes=[pltpu.VMEM((vocab_dev, 2048), F32), pltpu.VMEM((IN_SLOTS, SUB, 2048), F32), pltpu.VMEM((OUT_SLOTS, ROW_BLK, 2048), BF16), dma((IN_SLOTS,)), dma((OUT_SLOTS,))]
        + [pltpu.VMEM(p.shape, p.dtype) for p in passed] + [pltpu.VMEM((576, 128), F32), dma((5,)), dma((5,))],
        compiler_params=pltpu.CompilerParams(vmem_limit_bytes=67043328),
        cost_estimate=pl.CostEstimate(flops=10**9, bytes_accessed=90 * 10**6, transcendentals=0), name='table_grad',
    )(starts, toks, rows, small, row_grads, *passed)


def small_kernel(src, out, loc_sem, s_sem, r_sem):
    me = lax.axis_index('fsdp')
    meet_all(me)
    own = pltpu.make_async_copy(src, out.at[me], loc_sem)
    own.start()

    def send(step):
        return pltpu.make_async_remote_copy(src, out.at[me], s_sem.at[step], r_sem.at[step],
                                            device_id={'fsdp': (me + step) % GROUP}, device_id_type=MESH)
    for step in range(1, GROUP):
        send(step).start()
    for step in range(1, GROUP):
        send(step).wait()
    own.wait()


def small_gather(tile):
    dma = pltpu.SemaphoreType.DMA
    return pl.pallas_call(
        small_kernel, out_shape=jax.ShapeDtypeStruct((GROUP, 8, 128), F32),
        in_specs=[pl.BlockSpec(memory_space=pltpu.VMEM)], out_specs=pl.BlockSpec(memory_space=pltpu.VMEM),
        scratch_shapes=[dma, dma((GROUP,)), dma((GROUP,))],
        compiler_params=pltpu.CompilerParams(collective_id=0, has_side_effects=True),
        cost_estimate=pl.CostEstimate(flops=10**7, bytes_accessed=10**5, transcendentals=0), name='small_gather',
    )(tile)


def blank(shape, dtype):
    return pl.pallas_call(lambda out: None, out_shape=jax.ShapeDtypeStruct(shape, dtype), out_specs=ANY, name='blank')()


def block_step(rows_f32, grad_rows, full_weights, seq_count):
    gain_vec, w_query, w_kv_down, kv_gain, w_kv_up, w_out = full_weights
    kv_rank = kv_gain.shape[0]
    tok_count = rows_f32.shape[0]
    seq_len = tok_count // seq_count
    normed, norm_pull = jax.vjp(rms_scale, rows_f32, gain_vec)
    q_proj = jnp.dot(normed, w_query, preferred_element_type=jnp.float32).astype(jnp.bfloat16)
    kv_down = jnp.dot(normed, w_kv_down, preferred_element_type=jnp.float32).astype(jnp.bfloat16)
    latent, latent_pull = jax.vjp(rms_scale, kv_down[:, :kv_rank], kv_gain)
    kv_up = jnp.dot(latent, w_kv_up, preferred_element_type=jnp.float32).astype(jnp.bfloat16)
    attn_mix, attn_pull = jax.vjp(attend_local, q_proj.reshape(seq_count, seq_len, -1, NOPE_DIM + ROPE_DIM), kv_down[:, kv_rank:].reshape(seq_count, seq_len, ROPE_DIM), kv_up.reshape(seq_count, seq_len, -1, NOPE_DIM + VALUE_DIM))
    mix_rows = attn_mix.reshape(tok_count, -1)
    d_mix = lax.dot_general(grad_rows[:, :WO_CUT], w_out[0], COL_DIMS, preferred_element_type=jnp.float32)
    d_mix = (d_mix + lax.dot_general(grad_rows[:, WO_CUT:], w_out[1], COL_DIMS, preferred_element_type=jnp.float32)).astype(jnp.bfloat16)
    d_query, d_pe, d_up = attn_pull(d_mix.reshape(attn_mix.shape))
    d_query = d_query.reshape(tok_count, -1)
    d_up = d_up.reshape(tok_count, -1)
    d_latent = lax.dot_general(d_up, w_kv_up, COL_DIMS, preferred_element_type=jnp.float32).astype(jnp.bfloat16)
    d_ckv, d_kv_gain = latent_pull(d_latent)
    d_down = jnp.concatenate([d_ckv, d_pe.reshape(tok_count, ROPE_DIM)], axis=1)
    d_normed = lax.dot_general(d_query, w_query, COL_DIMS, preferred_element_type=jnp.float32)
    d_normed = d_normed + lax.dot_general(d_down, w_kv_down, COL_DIMS, preferred_element_type=jnp.float32)
    d_normed = d_normed.astype(jnp.bfloat16)
    _, d_gain = norm_pull(d_normed)
    return d_normed, normed, mix_rows, latent, d_query, d_down, d_up, d_gain, d_kv_gain


def solution(mesh):
    tok_spec = P(('dp', 'fsdp'), None)
    seq_spec = P(('dp', 'fsdp'), None, None)
    part_vec = P(('dp', 'fsdp'))
    vec_spec = P('fsdp')
    mat_spec = P('fsdp', None)

    def device_step(tok_ids, grad_out, emb_table, norm_gain, w_query, w_kv_down, kv_gain, w_kv_up, w_out):
        seq_count, seq_len = tok_ids.shape
        vocab_dev, d_model = emb_table.shape
        tok_count = seq_count * seq_len
        me = lax.axis_index('fsdp')
        grad_rows = grad_out.reshape(tok_count, d_model)
        bundle = lax.all_gather(jnp.concatenate([w_query, w_out[:, :WO_CUT]], axis=1), 'fsdp', tiled=True)
        fill = lambda rows: jnp.pad(rows, ((0, 0), (0, 128 - rows.shape[1])))
        tile = jnp.concatenate([fill(tok_ids.astype(F32)), norm_gain.astype(F32).reshape(1, 128), fill(kv_gain.astype(F32).reshape(1, 32)), jnp.zeros((3, 128), F32)], axis=0)
        table = small_gather(tile)
        all_ids = table[:, :seq_count, :seq_len].reshape(GROUP, tok_count).astype(jnp.int32)
        gain_full = table[:, 3, :].reshape(-1)
        kv_gain_full = table[:, 4, :32].reshape(-1)

        owner = all_ids // vocab_dev
        mine = (owner == me)
        local = all_ids - me * vocab_dev
        stamp = jnp.arange(GROUP * tok_count).reshape(GROUP, tok_count)
        keys = lax.sort(jnp.where(mine, stamp * 8192 + local, 2**30).reshape(-1))
        before = (jnp.arange(GROUP * tok_count)[None, :] < SUB * jnp.arange(GROUP * tok_count // SUB + 1)[:, None]) & mine.reshape(1, -1)
        starts = jnp.sum(before.astype(jnp.int32), axis=1)
        picked = jnp.take(emb_table, jnp.where(mine, local, 0).reshape(-1), axis=0, mode='clip')
        core = me % 2
        near = lax.dynamic_index_in_dim(owner.reshape(RING, 2, tok_count), core, 1, keepdims=False)
        mask = jnp.stack([near == me, near == me + 1 - 2 * core]).astype(BF16)
        mask = jnp.broadcast_to(mask[..., None], (2, RING, tok_count, 128))
        picked, keys, starts, w_kv_down = lax.optimization_barrier((picked, keys, starts, w_kv_down))
        tok_rows, full_kvb, full_kva, wo_last = spread(mask, picked.reshape(GROUP, tok_count, d_model), (w_kv_up, w_kv_down, w_out[:, WO_CUT:]))
        full_wq, full_wo = bundle[:, :3072], (bundle[:, 3072:], wo_last)
        tok_rows, grad_rows = lax.optimization_barrier((tok_rows, grad_rows))
        all_dy = lax.all_gather(grad_rows, 'fsdp', tiled=True)
        d_normed, normed, mix, latent, d_query, d_down, d_up, d_gain, d_kv_gain = block_step(
            tok_rows.astype(F32), grad_rows, (gain_full, full_wq, full_kva, kv_gain_full, full_kvb, full_wo), seq_count)
        small = jnp.concatenate([d_gain.reshape(GROUP, 1, 128), jnp.pad(d_kv_gain.reshape(GROUP, 1, 32), ((0, 0), (0, 0), (0, 96))), jnp.zeros((GROUP, 6, 128), F32)], axis=1)
        block_out, _, row_grads, g_out, g_query, g_down, g_up, g_small = grad_shards(mix, all_dy, normed.T, jnp.pad(d_down, ((0, 0), (0, D_DOWN - d_down.shape[1]))), d_query, latent.T, d_up, small, tok_rows, bundle, wo_last, d_normed, picked, gain_full.reshape(1, -1))
        grad_table, block_out, g_query, g_down, g_up, g_out, g_gain, g_kv_gain = table_grad(
            starts, keys >> 13, keys & 8191, g_small, row_grads, vocab_dev,
            (block_out, g_query, g_down, g_up, g_out))
        return (block_out.reshape(seq_count, seq_len, d_model), grad_table, g_gain.reshape(-1), g_query, g_down.T, g_kv_gain.reshape(-1), g_up, g_out)

    return jax.shard_map(device_step, mesh=mesh, in_specs=(tok_spec, seq_spec, mat_spec, vec_spec, mat_spec, mat_spec, vec_spec, mat_spec, mat_spec), out_specs=(seq_spec, tok_spec, part_vec, tok_spec, tok_spec, part_vec, tok_spec, tok_spec), check_vma=False)
```

```python
import math
import jax
import jax.numpy as jnp
from jax import lax
from jax.sharding import PartitionSpec as P
from jax.experimental import pallas as pl
from jax.experimental.pallas import tpu as pltpu

NOPE_DIM = 128
ROPE_DIM = 64
VALUE_DIM = 128
ROPE_THETA = 50000.0
RMS_EPS = 1e-6
ATTN_SCALE = (NOPE_DIM + ROPE_DIM) ** -0.5 * (0.1 * math.log(32.0) + 1.0) ** 2
ROW_DIMS = (((0,), (0,)), ((), ()))
COL_DIMS = (((1,), (1,)), ((), ()))


def rms_scale(in_vals, gain_vec):
    vals_f32 = in_vals.astype(jnp.float32)
    inv_rms = lax.rsqrt(jnp.mean(vals_f32 * vals_f32, axis=-1, keepdims=True) + RMS_EPS)
    return (vals_f32 * inv_rms * gain_vec).astype(jnp.bfloat16)


def rope_tables(seq_len):
    positions = jnp.arange(seq_len, dtype=jnp.float32)
    inv_freq = ROPE_THETA ** (-2.0 * jnp.arange(ROPE_DIM // 2, dtype=jnp.float32) / ROPE_DIM)
    rot_angle = positions[:, None] * inv_freq[None, :]
    rot_angle = jnp.concatenate([rot_angle, rot_angle], axis=-1)
    return jnp.cos(rot_angle), jnp.sin(rot_angle)


def apply_rope(in_vals, cos_tab, sin_tab):
    half_dim = ROPE_DIM // 2
    vals_f32 = in_vals.astype(jnp.float32)
    turned = jnp.concatenate([-vals_f32[..., half_dim:], vals_f32[..., :half_dim]], axis=-1)
    return (vals_f32 * cos_tab + turned * sin_tab).astype(jnp.bfloat16)


def attend_local(q_proj, pe_raw, kv_up):
    seq_len = q_proj.shape[1]
    cos_tab, sin_tab = rope_tables(seq_len)
    q_rot = apply_rope(q_proj[..., NOPE_DIM:], cos_tab[:, None, :], sin_tab[:, None, :])
    k_rot = apply_rope(pe_raw, cos_tab, sin_tab)
    scores = jnp.einsum('bshd,bthd->bhst', q_proj[..., :NOPE_DIM], kv_up[..., :NOPE_DIM], preferred_element_type=jnp.float32)
    scores = scores + jnp.einsum('bshd,btd->bhst', q_rot, k_rot, preferred_element_type=jnp.float32)
    positions = jnp.arange(seq_len)
    causal = positions[:, None] >= positions[None, :]
    scores = jnp.where(causal, scores * ATTN_SCALE, -1e30)
    attn_probs = jax.nn.softmax(scores, axis=-1).astype(jnp.bfloat16)
    attn_mix = jnp.einsum('bhst,bthd->bshd', attn_probs, kv_up[..., NOPE_DIM:], preferred_element_type=jnp.float32)
    return attn_mix.astype(jnp.bfloat16)


F32, BF16 = jnp.float32, jnp.bfloat16
MESH = pl.DeviceIdType.MESH
ANY = pl.BlockSpec(memory_space=pl.ANY)
RING = 8
GROUP = 16

def chip_at(pos):
    side = pos // 4
    return (pos + side * (7 - 2 * pos)) * 2 + side

def place():
    me = lax.axis_index('fsdp')
    core = me % 2
    chip = me // 2
    side = chip % 2
    zz = chip // 2
    return me, core, zz + side * (7 - 2 * zz)

def at_pos(pos, core):
    return chip_at(pos % RING) * 2 + core

def meet_all(me):
    barrier = pltpu.get_barrier_semaphore()
    for step in range(1, GROUP):
        pl.semaphore_signal(barrier, inc=1, device_id={'fsdp': (me + step) % GROUP}, device_id_type=MESH)
    pl.semaphore_wait(barrier, GROUP - 1)

TOK = 288
IN_BLK = 144
PIECE = 16
D_OUT, D_CAT, D_UP, D_DOWN = 2048, 3712, 4096, 640
WO_COL = 3072
WO_CUT = 1152
CUT = 1792
PARTS = (('u', 0, 0, 2304), ('u', 1, 2304, 1792), ('n', 0, 0, 896), ('n', 1, 1792, 1024), ('n', 0, 896, 896), ('n', 1, 2816, 896))
N_PARTS = len(PARTS)
ROWS = {'n': 128, 'u': 32}

def col_tiles(width):
    step = 512
    return [(c, min(step, width - c)) for c in range(0, width, step)]

def grad_kernel(mix_h, dy_h, nrm_h, dd_h, dq_h, lat_h, du_h, sm_h, h0_h, wo_h, wl_h, dn_h, h_h, gain, y_h, dn_all, grad_h, go_h, gq_h, gd_h, gu_h, gs_h,
                mix, dy, go, nrm, cat, lat, du, b0, b1, b2, b3, b4, b5, mixf, h0, wo, yacc, yv, own_dn, fdn, fdy, fh, fo, smr, ssum, loc_sem, xs_sem, xr_sem, s_sem, r_sem, ms_sem, mr_sem, cs_sem, cr_sem, dy_sem, y_sem, ns_sem, nr_sem, np_sem, nq_sem, f_sem, fo_sem, out_sem):
    me, core, pos = place()
    partner = me + 1 - 2 * core
    meet_all(me)
    acts = ((lat_h, lat), (du_h, du), (nrm_h, nrm), (dd_h, cat.at[:, :, 0:D_DOWN]), (dq_h, cat.at[:, :, D_DOWN:D_CAT]))
    local, cross = [], []
    for i, (src, dst) in enumerate(acts):
        cp = pltpu.make_async_copy(src, dst.at[core], loc_sem.at[i])
        cp.start()
        local.append(cp)
        rc = pltpu.make_async_remote_copy(src, dst.at[core], xs_sem.at[i], xr_sem.at[i], device_id={'fsdp': partner}, device_id_type=MESH)
        rc.start()
        cross.append(rc)
    peers = (at_pos(pos + 1, core), at_pos(pos + 7, core))

    def unit(dev, way):
        return pl.ds(pl.multiple_of(dev * TOK + way * IN_BLK, PIECE), IN_BLK)

    def origin(way, step):
        return at_pos(pos + 8 - step + way * 2 * step, core)

    def dn_hop(way, step, src=None):
        spot = dn_all.at[unit(origin(way, step), way), :]
        return pltpu.make_async_remote_copy(spot if src is None else src, spot, ns_sem.at[way, step], nr_sem.at[way, step + 1],
                                            device_id={'fsdp': peers[way]}, device_id_type=MESH)

    def dn_arrive(way, step):
        spot = dn_all.at[unit(origin(way, step), way), :]
        return pltpu.make_async_remote_copy(spot, spot, ns_sem.at[way, step], nr_sem.at[way, step],
                                            device_id={'fsdp': peers[way]}, device_id_type=MESH)

    def dn_share(way, step, src=None):
        spot = dn_all.at[unit(origin(way, step), way), :]
        return pltpu.make_async_remote_copy(spot if src is None else src, spot, np_sem.at[way, step], nq_sem.at[way, step],
                                            device_id={'fsdp': partner}, device_id_type=MESH)
    own_load = pltpu.make_async_copy(dn_h, own_dn, f_sem.at[0, 0])
    own_load.start()
    own_load.wait()
    for way in range(2):
        src = own_dn.at[way * IN_BLK:(way + 1) * IN_BLK, :]
        dn_hop(way, 0, src).start()
        dn_share(way, 0, src).start()
        pltpu.make_async_copy(src, dn_all.at[unit(me, way), :], fo_sem.at[way]).start()

    def row_grads(step):
        jobs = [(at_pos(pos + 8 - step + way * 2 * step, c), way) for way in range(2) for c in (core, 1 - core)]

        def fetch(slot):
            dev, way = jobs[slot]
            return [pltpu.make_async_copy(src.at[unit(dev, way), :], dst.at[slot], f_sem.at[i, slot])
                    for i, (src, dst) in enumerate(((dn_all, fdn), (dy_h, fdy), (h_h, fh)))]

        def put(slot):
            dev, way = jobs[slot]
            return pltpu.make_async_copy(fo.at[slot % 2], grad_h.at[unit(dev, way), :], fo_sem.at[slot % 2])
        for way in range(2):
            dn_share(way, step).wait_recv()
        for slot in range(4):
            for cp in fetch(slot):
                cp.start()

        for slot in range(4):
            for cp in fetch(slot):
                cp.wait()
            if slot >= 2:
                put(slot - 2).wait()

            @pl.loop(0, IN_BLK // 48)
            def _(g):
                r0 = pl.multiple_of(g * 48, PIECE)

                def tile(ref, p, c):
                    return ref[slot, pl.ds(r0 + p, PIECE), c:c + 128].astype(F32)
                scale = []
                for p in range(0, 48, PIECE):
                    sq = jnp.zeros((PIECE, 128), F32)
                    al = jnp.zeros((PIECE, 128), F32)
                    for c in range(0, 2048, 128):
                        h = tile(fh, p, c)
                        sq = sq + h * h
                        al = al + h * (tile(fdn, p, c) * gain[:, c:c + 128])
                    scale.append((jnp.sum(sq, axis=1, keepdims=True), jnp.sum(al, axis=1, keepdims=True)))
                for p, (sq, al) in zip(range(0, 48, PIECE), scale):
                    inv = lax.rsqrt(sq * (1.0 / 2048) + RMS_EPS)
                    coef = inv * inv * inv * (al * (1.0 / 2048))
                    for c in range(0, 2048, 128):
                        s = tile(fdn, p, c) * gain[:, c:c + 128]
                        fo[slot % 2, pl.ds(r0 + p, PIECE), c:c + 128] = tile(fdy, p, c) + inv * s - coef * tile(fh, p, c)
            put(slot).start()
        put(2).wait()
        put(3).wait()

    own_small = pltpu.make_async_copy(sm_h.at[me], smr.at[0], loc_sem.at[5])
    own_small.start()
    own_mix = pltpu.make_async_copy(mix_h.at[:, pl.ds(pl.multiple_of(me * 128, 128), 128)], mix.at[me], loc_sem.at[6])
    own_mix.start()
    smalls, mixes = [], []
    for i in range(1, GROUP):
        peer = (me + i) % GROUP
        rc = pltpu.make_async_remote_copy(sm_h.at[peer], smr.at[i], ms_sem.at[i], mr_sem.at[i], device_id={'fsdp': peer}, device_id_type=MESH)
        rc.start()
        smalls.append(rc)
    for i, (src, dst) in enumerate(((mix_h, mixf), (h0_h, h0))):
        pltpu.make_async_copy(src, dst, y_sem.at[2, i]).start()

    def wo_load(t):
        span = pl.ds(pl.multiple_of(t * 256, 256), 256)
        return [pltpu.make_async_copy(src, dst, y_sem.at[i, t % 2]) for i, (src, dst) in enumerate((
            (wo_h.at[span, WO_COL:WO_COL + WO_CUT], wo.at[t % 2, :, 0:WO_CUT]), (wl_h.at[span, :], wo.at[t % 2, :, WO_CUT:2048])))]
    for cp in wo_load(0):
        cp.start()
    bufs = (b0, b1, b2, b3, b4, b5)
    left_ops = {'n': (nrm, cat), 'u': (lat, du)}

    def mix_send(i):
        peer = (me + i) % GROUP
        return pltpu.make_async_remote_copy(mix_h.at[:, pl.ds(pl.multiple_of(peer * 128, 128), 128)], mix.at[me], cs_sem.at[i], cr_sem.at[i],
                                            device_id={'fsdp': peer}, device_id_type=MESH)

    def dy_load(blk):
        return pltpu.make_async_copy(dy_h.at[pl.ds(pl.multiple_of(blk * TOK, TOK), TOK), :], dy.at[blk % 2], dy_sem.at[blk % 2])

    def hop(p, step):
        return pltpu.make_async_remote_copy(bufs[p].at[step], bufs[p].at[step + 1], s_sem.at[p, step], r_sem.at[p, step + 1],
                                            device_id={'fsdp': peers[PARTS[p][1]]}, device_id_type=MESH)

    def work(p, step):
        kind, way, c0, width = PARTS[p]
        chip = chip_at((pos + 7 - step + way * (2 * step + 2)) % RING)
        lhs_ref, rhs_ref = left_ops[kind]
        rows = ROWS[kind]
        row = pl.multiple_of((chip * 2 + core) * rows, rows)
        lhs = [lhs_ref[b, pl.ds(row, rows), :] for b in range(2)]
        for c, w in col_tiles(width):
            part = sum(jnp.dot(lhs[b], rhs_ref[b, :, c0 + c:c0 + c + w], preferred_element_type=F32) for b in range(2))
            bufs[p][step, :, c:c + w] = bufs[p][step, :, c:c + w] + part

    dy_load(0).start()
    go[...] = jnp.zeros_like(go)
    for p in range(N_PARTS):
        bufs[p][0] = jnp.zeros(bufs[p].shape[1:], F32)
    first_use = {0: (0, 1), 2: (2, 3, 4)}

    for way in range(2):
        pltpu.make_async_copy(own_dn.at[way * IN_BLK:(way + 1) * IN_BLK, :], dn_all.at[unit(me, way), :], fo_sem.at[way]).wait()

    @pl.loop(0, RING)
    def _(step):
        @pl.when(step > 0)
        def _():
            for way in range(2):
                dn_arrive(way, step).wait_recv()

                @pl.when(step < RING - 1)
                def _():
                    dn_hop(way, step).start()
                dn_share(way, step).start()

            @pl.loop(step - 1, step + step // (RING - 1))
            def _(done):
                row_grads(done)

        for p in range(N_PARTS):
            if p in first_use:
                @pl.when(step == 0)
                def _():
                    for i in first_use[p]:
                        local[i].wait()
                        cross[i].wait_recv()

            @pl.when(step > 0)
            def _():
                hop(p, step - 1).wait_recv()
            work(p, step)

            @pl.when(step < RING - 1)
            def _():
                hop(p, step).start()

        @pl.when(step == 0)
        def _():
            own_mix.wait()
            for i in range(1, GROUP):
                mix_send(i).start()

        @pl.when(step == 2)
        def _():
            for i in range(1, GROUP):
                mix_send(i).wait()

        @pl.when((step > 1) & (step < 6))
        def _():
            @pl.loop(0, 4)
            def _(j):
                blk = (step - 2) * 4 + j
                dy_load(blk).wait()

                @pl.when(blk < GROUP - 1)
                def _():
                    dy_load(blk + 1).start()
                for c, w in col_tiles(2048):
                    go[:, c:c + w] += lax.dot_general(mix[blk], dy[blk % 2, :, c:c + w], (((0,), (0,)), ((), ())), preferred_element_type=F32)

        @pl.when(step == 6)
        def _():
            for i, (src, dst) in enumerate(((mix_h, mixf), (h0_h, h0))):
                pltpu.make_async_copy(src, dst, y_sem.at[2, i]).wait()

            yacc[...] = h0[...].astype(F32)

            @pl.loop(0, 8)
            def _(t):
                for cp in wo_load(t):
                    cp.wait()

                @pl.when(t < 7)
                def _():
                    for cp in wo_load(t + 1):
                        cp.start()

                @pl.loop(0, 4)
                def _(j):
                    here = pl.ds(pl.multiple_of(j * 512, 512), 512)
                    yacc[:, here] += jnp.dot(mixf[:, pl.ds(pl.multiple_of(t * 256, 256), 256)], wo[t % 2, :, here], preferred_element_type=F32)
            yv[...] = yacc[...].astype(BF16)

    last = RING - 1
    outs = []
    cp = pltpu.make_async_copy(go, go_h, out_sem.at[6])
    cp.start()
    outs.append(cp)
    cp = pltpu.make_async_copy(yv, y_h, out_sem.at[9])
    cp.start()
    outs.append(cp)
    targets = (((gu_h.at[:, 0:2304], 0, 2304),), ((gu_h.at[:, 2304:4096], 0, 1792),), ((gd_h, 0, 640), (gq_h.at[:, 0:256], 640, 896)),
               ((gq_h.at[:, 1152:2176], 0, 1024),), ((gq_h.at[:, 256:1152], 0, 896),), ((gq_h.at[:, 2176:3072], 0, 896),))
    for p in range(N_PARTS):
        for n, (dst, c0, c1) in enumerate(targets[p]):
            cp = pltpu.make_async_copy(bufs[p].at[last, :, c0:c1], dst, out_sem.at[p + 6 * n])
            cp.start()
            outs.append(cp)
    own_small.wait()
    for rc in smalls:
        rc.wait()
    ssum[...] = jnp.sum(smr[...], axis=0)
    cp = pltpu.make_async_copy(ssum, gs_h, out_sem.at[7])
    cp.start()
    outs.append(cp)
    for rc in cross:
        rc.wait_send()
    for p in range(N_PARTS):
        @pl.loop(0, last)
        def _(step):
            hop(p, step).wait_send()

    @pl.loop(0, RING)
    def _(step):
        for way in range(2):
            dn_share(way, step).wait_send()

            @pl.when(step < last)
            def _():
                dn_hop(way, step).wait_send()
    for cp in outs:
        cp.wait()


def grad_shards(mix, dy_all, nrm_t, dd, dq, lat_t, du, small, rows, weights, last_cols, dn, picked, gain):
    shapes = [(ROWS[k], RING, w) for k, _, _, w in PARTS]
    scratch = [pltpu.VMEM((GROUP, TOK, 128), BF16), pltpu.VMEM((2, TOK, 2048), BF16), pltpu.VMEM((128, 2048), F32), pltpu.VMEM((2, 2048, TOK), BF16),
               pltpu.VMEM((2, TOK, D_CAT), BF16), pltpu.VMEM((2, 512, TOK), BF16), pltpu.VMEM((2, TOK, D_UP), BF16)]
    scratch += [pltpu.VMEM((RING, r, w), F32) for r, _, w in shapes]
    scratch += [pltpu.VMEM((TOK, 2048), BF16), pltpu.VMEM((TOK, 2048), BF16), pltpu.VMEM((2, 256, 2048), BF16), pltpu.VMEM((TOK, 2048), F32), pltpu.VMEM((TOK, 2048), BF16)]
    scratch += [pltpu.VMEM((TOK, 2048), BF16)] + [pltpu.VMEM((4, IN_BLK, 2048), BF16)] * 3 + [pltpu.VMEM((2, IN_BLK, 2048), F32)]
    scratch += [pltpu.VMEM((GROUP, 8, 128), F32), pltpu.VMEM((8, 128), F32)]
    dma = pltpu.SemaphoreType.DMA
    scratch += [dma((7,)), dma((5,)), dma((5,)), dma((N_PARTS, RING)), dma((N_PARTS, RING)), dma((GROUP,)), dma((GROUP,)), dma((GROUP,)), dma((GROUP,)), dma((2,)), dma((3, 2)), dma((2, RING)), dma((2, RING)), dma((2, RING)), dma((2, RING)), dma((3, 4)), dma((2,)), dma((10,))]
    return pl.pallas_call(
        grad_kernel,
        out_shape=(jax.ShapeDtypeStruct((TOK, 2048), BF16), jax.ShapeDtypeStruct((GROUP * TOK, 2048), BF16), jax.ShapeDtypeStruct((GROUP * TOK, 2048), F32), jax.ShapeDtypeStruct((128, 2048), F32), jax.ShapeDtypeStruct((128, 3072), F32), jax.ShapeDtypeStruct((128, D_DOWN), F32), jax.ShapeDtypeStruct((32, D_UP), F32), jax.ShapeDtypeStruct((8, 128), F32)),
        in_specs=[ANY] * 13 + [pl.BlockSpec(memory_space=pltpu.VMEM)], out_specs=(ANY,) * 8, scratch_shapes=scratch,
        compiler_params=pltpu.CompilerParams(collective_id=1, has_side_effects=True, vmem_limit_bytes=63 * 1024 * 1024),
        cost_estimate=pl.CostEstimate(flops=8 * 10**9, bytes_accessed=20 * 10**6, transcendentals=0), name='grad_shards',
    )(mix, dy_all, nrm_t, dd, dq, lat_t, du, small, rows, weights, last_cols, dn, picked, gain)


W_SHARDS = ((32, 4096), (128, 576), (128, 896))
HALF_TOK = TOK // 2
CUTS = ((0, 80), (80, 64))


def spread_kernel(n_w, *refs):
    mask, rows_h = refs[0:2]
    srcs = refs[2:2 + n_w]
    got_h = refs[2 + n_w]
    outs = refs[3 + n_w:3 + 2 * n_w]
    stage = refs[3 + 2 * n_w:3 + 3 * n_w]
    own, mate, way0, way1 = refs[3 + 3 * n_w:7 + 3 * n_w]
    in_sem, own_sem, s_sem, r_sem, ps_sem, pr_sem, os_sem, or_sem, xs_sem, xr_sem, ts_sem, tr_sem, h_in, m_s, m_r, hs_sem, hr_sem, out_sem = refs[7 + 3 * n_w:]
    me, core, pos = place()
    twin = lax.axis_index('dp')
    partner = me + 1 - 2 * core
    barrier = pltpu.get_barrier_semaphore()
    peers = (at_pos(pos + 1, core), at_pos(pos + 7, core))
    for peer in peers + (partner,):
        pl.semaphore_signal(barrier, inc=1, device_id={'fsdp': peer}, device_id_type=MESH)
    pl.semaphore_signal(barrier, inc=1, device_id={'dp': 1 - twin}, device_id_type=MESH)
    pl.semaphore_wait(barrier, 4)
    loads = []
    for i in range(n_w):
        cp = pltpu.make_async_copy(srcs[i], stage[i], in_sem.at[i])
        cp.start()
        loads.append(cp)

    def row_load(q):
        return pltpu.make_async_copy(rows_h.at[at_pos(q, core)], own.at[q], h_in.at[q])

    def row_share(q):
        return pltpu.make_async_remote_copy(rows_h.at[at_pos(q, 1 - core)], mate.at[q], m_s.at[q], m_r.at[q],
                                            device_id={'fsdp': partner}, device_id_type=MESH)
    for j in (7, 1, 6, 2, 5, 3, 4, 0):
        row_share((pos + j) % RING).start()
        row_load((pos + j) % RING).start()

    def where(i, way, source, side):
        rows = W_SHARDS[i][0]
        part = rows // 4
        return outs[i].at[pl.ds(pl.multiple_of(source * rows + side * 2 * part + way * part, part), part), :]

    def whole(i):
        rows = W_SHARDS[i][0]
        return outs[i].at[pl.ds(pl.multiple_of(me * rows, rows), rows), :]

    def origin(way, step):
        return at_pos(pos + 8 - step + way * 2 * step, core)

    def hop(i, way, step, src=None):
        spot = where(i, way, origin(way, step), twin)
        return pltpu.make_async_remote_copy(spot if src is None else src, spot, s_sem.at[i, way, step], r_sem.at[i, way, step + 1],
                                            device_id={'fsdp': peers[way]}, device_id_type=MESH)

    def arrive(i, way, step):
        spot = where(i, way, origin(way, step), twin)
        return pltpu.make_async_remote_copy(spot, spot, s_sem.at[i, way, step], r_sem.at[i, way, step],
                                            device_id={'fsdp': peers[way]}, device_id_type=MESH)

    def share(i, way, step):
        spot = where(i, way, origin(way, step), twin)
        return pltpu.make_async_remote_copy(spot, spot, ps_sem.at[i, way, step], pr_sem.at[i, way, step],
                                            device_id={'fsdp': partner}, device_id_type=MESH)

    def share_own(i):
        return pltpu.make_async_remote_copy(stage[i], whole(i), os_sem.at[i], or_sem.at[i], device_id={'fsdp': partner}, device_id_type=MESH)

    def to_twin(i, way, step):
        spot = where(i, way, origin(way, step), twin)
        return pltpu.make_async_remote_copy(spot, spot, xs_sem.at[i, way, step], xr_sem.at[i, way, step],
                                            device_id={'dp': 1 - twin}, device_id_type=MESH)

    def share_twin(i, way, step):
        spot = where(i, way, origin(way, step), 1 - twin)
        return pltpu.make_async_remote_copy(spot, spot, ts_sem.at[i, way, step], tr_sem.at[i, way, step],
                                            device_id={'fsdp': partner}, device_id_type=MESH)
    ways = (way0, way1)

    def row_hop(way, cut, step):
        lo, n = CUTS[cut]
        return pltpu.make_async_remote_copy(ways[way].at[step, lo:lo + n, :], ways[way].at[step + 1, lo:lo + n, :], hs_sem.at[way, cut, step], hr_sem.at[way, cut, step + 1],
                                            device_id={'fsdp': peers[way]}, device_id_type=MESH)

    def fill(way, cut, step, first):
        q = (pos + 7 - step + way * (2 * step + 2)) % RING
        chip = chip_at(q)
        for c in range(CUTS[cut][0], sum(CUTS[cut]), 16):
            lo = way * HALF_TOK + c
            mine, theirs = mask[0, chip, lo:lo + 16, :], mask[1, chip, lo:lo + 16, :]
            for w in range(0, 2048, 128):
                part = own[q, lo:lo + 16, w:w + 128] * mine + mate[q, lo:lo + 16, w:w + 128] * theirs
                if not first:
                    part = part + ways[way][step, c:c + 16, w:w + 128]
                ways[way][step, c:c + 16, w:w + 128] = part

    kept = []
    for i in range(n_w):
        loads[i].wait()
        part = W_SHARDS[i][0] // 4
        for way in range(2):
            hop(i, way, 0, stage[i].at[pl.ds(pl.multiple_of(twin * 2 * part + way * part, part), part), :]).start()
        share_own(i).start()
        cp = pltpu.make_async_copy(stage[i], whole(i), own_sem.at[i])
        cp.start()
        kept.append(cp)
    for j in (7, 1, 6, 2, 5, 3, 4, 0):
        row_load((pos + j) % RING).wait()
        row_share((pos + j) % RING).wait_recv()
        if j in (7, 1):
            way = 0 if j == 7 else 1
            for cut in range(2):
                fill(way, cut, 0, True)
                row_hop(way, cut, 0).start()

    @pl.loop(1, RING)
    def _(step):
        for i in range(n_w):
            for way in range(2):
                arrive(i, way, step).wait_recv()

                @pl.when(step < RING - 1)
                def _():
                    hop(i, way, step).start()
                share(i, way, step).start()
                to_twin(i, way, step).start()
        for cut in range(2):
            for way in range(2):
                row_hop(way, cut, step - 1).wait_recv()
                fill(way, cut, step, False)

                @pl.when(step < RING - 1)
                def _():
                    row_hop(way, cut, step).start()

        @pl.when(step > 1)
        def _():
            for i in range(n_w):
                for way in range(2):
                    to_twin(i, way, step - 1).wait_recv()
                    share_twin(i, way, step - 1).start()

    for i in range(n_w):
        for way in range(2):
            to_twin(i, way, RING - 1).wait_recv()
            share_twin(i, way, RING - 1).start()
    for way in range(2):
        cp = pltpu.make_async_copy(ways[way].at[RING - 1], got_h.at[way * HALF_TOK:(way + 1) * HALF_TOK, :], out_sem.at[way])
        cp.start()
        kept.append(cp)
    for cp in kept:
        cp.wait()

    @pl.loop(0, RING)
    def _(step):
        row_share(step).wait_send()

        @pl.when(step < RING - 1)
        def _():
            for way in range(2):
                for cut in range(2):
                    row_hop(way, cut, step).wait_send()
        for i in range(n_w):
            for way in range(2):
                @pl.when(step < RING - 1)
                def _():
                    hop(i, way, step).wait_send()

                @pl.when(step > 0)
                def _():
                    share(i, way, step).wait()
                    to_twin(i, way, step).wait_send()
                    share_twin(i, way, step).wait()
    for i in range(n_w):
        share_own(i).wait()


def spread(mask, rows, shards):
    dma = pltpu.SemaphoreType.DMA
    n_w = len(shards)
    return pl.pallas_call(
        lambda *refs: spread_kernel(n_w, *refs),
        out_shape=(jax.ShapeDtypeStruct((TOK, 2048), BF16),) + tuple(jax.ShapeDtypeStruct((GROUP * r, w), BF16) for r, w in W_SHARDS),
        in_specs=[pl.BlockSpec(memory_space=pltpu.VMEM)] + [ANY] * (n_w + 1), out_specs=(ANY,) * (n_w + 1),
        scratch_shapes=[pltpu.VMEM(s, BF16) for s in W_SHARDS] + [pltpu.VMEM((RING, TOK, 2048), BF16)] * 2 + [pltpu.VMEM((RING, HALF_TOK, 2048), BF16)] * 2
        + [dma((n_w,)), dma((n_w,))] + [dma((n_w, 2, RING))] * 4 + [dma((n_w,))] * 2 + [dma((n_w, 2, RING))] * 4 + [dma((RING,)) for _ in range(3)] + [dma((2, 2, RING)) for _ in range(2)] + [dma((2,))],
        compiler_params=pltpu.CompilerParams(collective_id=2, has_side_effects=True, vmem_limit_bytes=60 * 1024 * 1024),
        cost_estimate=pl.CostEstimate(flops=8 * 10**9, bytes_accessed=27 * 10**6, transcendentals=0), name='spread',
    )(mask, rows, *shards)
ROW_BLK = 64
SUB = 72
UNROLL = 4
IN_SLOTS = 6
OUT_SLOTS = 8


def table_kernel(starts, toks, rows, small, grad_h, *refs):
    passed, out_h, given, gain_out, kv_out = refs[0:5], refs[5], refs[6:11], refs[11], refs[12]
    acc, grad, ob, in_sem, out_sem = refs[13:18]
    hold, cut, ride_in, ride_out = refs[18:23], refs[23], refs[24], refs[25]
    n_in = GROUP * TOK // SUB
    n_out = out_h.shape[0] // ROW_BLK

    def load(blk):
        return pltpu.make_async_copy(grad_h.at[pl.ds(pl.multiple_of(blk * SUB, SUB), SUB), :], grad.at[blk % IN_SLOTS], in_sem.at[blk % IN_SLOTS])
    for blk in range(IN_SLOTS):
        load(blk).start()
    boards = [pltpu.make_async_copy(src, dst, ride_in.at[i]) for i, (src, dst) in enumerate(zip(passed, hold))]
    leaves = [pltpu.make_async_copy(cut if i == 2 else src, dst, ride_out.at[i]) for i, (src, dst) in enumerate(zip(hold, given))]
    for cp in boards:
        cp.start()
    gain_out[...] = small[0:1, :]
    kv_out[...] = small[1:2, 0:32]

    @pl.loop(0, out_h.shape[0] // 64)
    def _(i):
        acc[pl.ds(pl.multiple_of(i * 64, 64), 64), :] = jnp.zeros((64, 2048), F32)

    @pl.loop(0, n_in)
    def _(blk):
        first, last = starts[blk], starts[blk + 1]
        slot = blk % IN_SLOTS
        load(blk).wait()

        def add(k):
            acc[pl.ds(rows[k], 1), :] += grad[slot, pl.ds(toks[k] - blk * SUB, 1), :]
        quads = (last - first) // UNROLL

        @pl.loop(0, quads)
        def _(i):
            for j in range(UNROLL):
                add(first + i * UNROLL + j)

        @pl.loop(first + quads * UNROLL, last)
        def _(k):
            add(k)

        @pl.when(blk < n_in - IN_SLOTS)
        def _():
            load(blk + IN_SLOTS).start()
    for cp in boards:
        cp.wait()
    cut[...] = hold[2][...].T[0:576, :]
    for cp in leaves:
        cp.start()

    def store(blk):
        slot = blk % OUT_SLOTS
        return pltpu.make_async_copy(ob.at[slot], out_h.at[pl.ds(pl.multiple_of(blk * ROW_BLK, ROW_BLK), ROW_BLK), :], out_sem.at[slot])

    @pl.loop(0, n_out)
    def _(blk):
        @pl.when(blk >= OUT_SLOTS)
        def _():
            store(blk - OUT_SLOTS).wait()
        ob[blk % OUT_SLOTS] = acc[pl.ds(pl.multiple_of(blk * ROW_BLK, ROW_BLK), ROW_BLK), :].astype(BF16)
        store(blk).start()
    for blk in range(n_out - OUT_SLOTS, n_out):
        store(blk).wait()
    for cp in leaves:
        cp.wait()


def table_grad(starts, toks, rows, small, row_grads, vocab_dev, passed):
    smem = pl.BlockSpec(memory_space=pltpu.SMEM)
    vmem = pl.BlockSpec(memory_space=pltpu.VMEM)
    dma = pltpu.SemaphoreType.DMA
    shapes = [jax.ShapeDtypeStruct((vocab_dev, 2048), BF16)] + [jax.ShapeDtypeStruct((576, 128) if i == 2 else p.shape, p.dtype) for i, p in enumerate(passed)]
    shapes += [jax.ShapeDtypeStruct((1, 128), F32), jax.ShapeDtypeStruct((1, 32), F32)]
    return pl.pallas_call(
        table_kernel, out_shape=tuple(shapes),
        in_specs=[smem] * 3 + [vmem] + [ANY] * 6, out_specs=(ANY,) * 6 + (vmem,) * 2,
        scratch_shapes=[pltpu.VMEM((vocab_dev, 2048), F32), pltpu.VMEM((IN_SLOTS, SUB, 2048), F32), pltpu.VMEM((OUT_SLOTS, ROW_BLK, 2048), BF16), dma((IN_SLOTS,)), dma((OUT_SLOTS,))]
        + [pltpu.VMEM(p.shape, p.dtype) for p in passed] + [pltpu.VMEM((576, 128), F32), dma((5,)), dma((5,))],
        compiler_params=pltpu.CompilerParams(vmem_limit_bytes=67043328),
        cost_estimate=pl.CostEstimate(flops=10**9, bytes_accessed=90 * 10**6, transcendentals=0), name='table_grad',
    )(starts, toks, rows, small, row_grads, *passed)


def small_kernel(src, out, loc_sem, s_sem, r_sem):
    me = lax.axis_index('fsdp')
    meet_all(me)
    own = pltpu.make_async_copy(src, out.at[me], loc_sem)
    own.start()

    def send(step):
        return pltpu.make_async_remote_copy(src, out.at[me], s_sem.at[step], r_sem.at[step],
                                            device_id={'fsdp': (me + step) % GROUP}, device_id_type=MESH)
    for step in range(1, GROUP):
        send(step).start()
    for step in range(1, GROUP):
        send(step).wait()
    own.wait()


def small_gather(tile):
    dma = pltpu.SemaphoreType.DMA
    return pl.pallas_call(
        small_kernel, out_shape=jax.ShapeDtypeStruct((GROUP, 8, 128), F32),
        in_specs=[pl.BlockSpec(memory_space=pltpu.VMEM)], out_specs=pl.BlockSpec(memory_space=pltpu.VMEM),
        scratch_shapes=[dma, dma((GROUP,)), dma((GROUP,))],
        compiler_params=pltpu.CompilerParams(collective_id=0, has_side_effects=True),
        cost_estimate=pl.CostEstimate(flops=10**7, bytes_accessed=10**5, transcendentals=0), name='small_gather',
    )(tile)


def blank(shape, dtype):
    return pl.pallas_call(lambda out: None, out_shape=jax.ShapeDtypeStruct(shape, dtype), out_specs=ANY, name='blank')()


def block_step(rows_f32, grad_rows, full_weights, seq_count):
    gain_vec, w_query, w_kv_down, kv_gain, w_kv_up, w_out = full_weights
    kv_rank = kv_gain.shape[0]
    tok_count = rows_f32.shape[0]
    seq_len = tok_count // seq_count
    normed, norm_pull = jax.vjp(rms_scale, rows_f32, gain_vec)
    q_proj = jnp.dot(normed, w_query, preferred_element_type=jnp.float32).astype(jnp.bfloat16)
    kv_down = jnp.dot(normed, w_kv_down, preferred_element_type=jnp.float32).astype(jnp.bfloat16)
    latent, latent_pull = jax.vjp(rms_scale, kv_down[:, :kv_rank], kv_gain)
    kv_up = jnp.dot(latent, w_kv_up, preferred_element_type=jnp.float32).astype(jnp.bfloat16)
    attn_mix, attn_pull = jax.vjp(attend_local, q_proj.reshape(seq_count, seq_len, -1, NOPE_DIM + ROPE_DIM), kv_down[:, kv_rank:].reshape(seq_count, seq_len, ROPE_DIM), kv_up.reshape(seq_count, seq_len, -1, NOPE_DIM + VALUE_DIM))
    mix_rows = attn_mix.reshape(tok_count, -1)
    d_mix = lax.dot_general(grad_rows[:, :WO_CUT], w_out[0], COL_DIMS, preferred_element_type=jnp.float32)
    d_mix = (d_mix + lax.dot_general(grad_rows[:, WO_CUT:], w_out[1], COL_DIMS, preferred_element_type=jnp.float32)).astype(jnp.bfloat16)
    d_query, d_pe, d_up = attn_pull(d_mix.reshape(attn_mix.shape))
    d_query = d_query.reshape(tok_count, -1)
    d_up = d_up.reshape(tok_count, -1)
    d_latent = lax.dot_general(d_up, w_kv_up, COL_DIMS, preferred_element_type=jnp.float32).astype(jnp.bfloat16)
    d_ckv, d_kv_gain = latent_pull(d_latent)
    d_down = jnp.concatenate([d_ckv, d_pe.reshape(tok_count, ROPE_DIM)], axis=1)
    d_normed = lax.dot_general(d_query, w_query, COL_DIMS, preferred_element_type=jnp.float32)
    d_normed = d_normed + lax.dot_general(d_down, w_kv_down, COL_DIMS, preferred_element_type=jnp.float32)
    d_normed = d_normed.astype(jnp.bfloat16)
    _, d_gain = norm_pull(d_normed)
    return d_normed, normed, mix_rows, latent, d_query, d_down, d_up, d_gain, d_kv_gain


def solution(mesh):
    tok_spec = P(('dp', 'fsdp'), None)
    seq_spec = P(('dp', 'fsdp'), None, None)
    part_vec = P(('dp', 'fsdp'))
    vec_spec = P('fsdp')
    mat_spec = P('fsdp', None)

    def device_step(tok_ids, grad_out, emb_table, norm_gain, w_query, w_kv_down, kv_gain, w_kv_up, w_out):
        seq_count, seq_len = tok_ids.shape
        vocab_dev, d_model = emb_table.shape
        tok_count = seq_count * seq_len
        me = lax.axis_index('fsdp')
        grad_rows = grad_out.reshape(tok_count, d_model)
        bundle = lax.all_gather(jnp.concatenate([w_query, w_out[:, :WO_CUT]], axis=1), 'fsdp', tiled=True)
        fill = lambda rows: jnp.pad(rows, ((0, 0), (0, 128 - rows.shape[1])))
        tile = jnp.concatenate([fill(tok_ids.astype(F32)), norm_gain.astype(F32).reshape(1, 128), fill(kv_gain.astype(F32).reshape(1, 32)), jnp.zeros((3, 128), F32)], axis=0)
        table = small_gather(tile)
        all_ids = table[:, :seq_count, :seq_len].reshape(GROUP, tok_count).astype(jnp.int32)
        gain_full = table[:, 3, :].reshape(-1)
        kv_gain_full = table[:, 4, :32].reshape(-1)

        owner = all_ids // vocab_dev
        mine = (owner == me)
        local = all_ids - me * vocab_dev
        stamp = jnp.arange(GROUP * tok_count).reshape(GROUP, tok_count)
        keys = lax.sort(jnp.where(mine, stamp * 8192 + local, 2**30).reshape(-1))
        before = (jnp.arange(GROUP * tok_count)[None, :] < SUB * jnp.arange(GROUP * tok_count // SUB + 1)[:, None]) & mine.reshape(1, -1)
        starts = jnp.sum(before.astype(jnp.int32), axis=1)
        picked = jnp.take(emb_table, jnp.where(mine, local, 0).reshape(-1), axis=0, mode='clip')
        core = me % 2
        near = lax.dynamic_index_in_dim(owner.reshape(RING, 2, tok_count), core, 1, keepdims=False)
        mask = jnp.stack([near == me, near == me + 1 - 2 * core]).astype(BF16)
        mask = jnp.broadcast_to(mask[..., None], (2, RING, tok_count, 128))
        picked, keys, starts, w_kv_down = lax.optimization_barrier((picked, keys, starts, w_kv_down))
        tok_rows, full_kvb, full_kva, wo_last = spread(mask, picked.reshape(GROUP, tok_count, d_model), (w_kv_up, w_kv_down, w_out[:, WO_CUT:]))
        full_wq, full_wo = bundle[:, :3072], (bundle[:, 3072:], wo_last)
        tok_rows, grad_rows = lax.optimization_barrier((tok_rows, grad_rows))
        all_dy = lax.all_gather(grad_rows, 'fsdp', tiled=True)
        d_normed, normed, mix, latent, d_query, d_down, d_up, d_gain, d_kv_gain = block_step(
            tok_rows.astype(F32), grad_rows, (gain_full, full_wq, full_kva, kv_gain_full, full_kvb, full_wo), seq_count)
        small = jnp.concatenate([d_gain.reshape(GROUP, 1, 128), jnp.pad(d_kv_gain.reshape(GROUP, 1, 32), ((0, 0), (0, 0), (0, 96))), jnp.zeros((GROUP, 6, 128), F32)], axis=1)
        block_out, _, row_grads, g_out, g_query, g_down, g_up, g_small = grad_shards(mix, all_dy, normed.T, jnp.pad(d_down, ((0, 0), (0, D_DOWN - d_down.shape[1]))), d_query, latent.T, d_up, small, tok_rows, bundle, wo_last, d_normed, picked, gain_full.reshape(1, -1))
        grad_table, block_out, g_query, g_down, g_up, g_out, g_gain, g_kv_gain = table_grad(
            starts, keys >> 13, keys & 8191, g_small, row_grads, vocab_dev,
            (block_out, g_query, g_down, g_up, g_out))
        return (block_out.reshape(seq_count, seq_len, d_model), grad_table, g_gain.reshape(-1), g_query, g_down.T, g_kv_gain.reshape(-1), g_up, g_out)

    return jax.shard_map(device_step, mesh=mesh, in_specs=(tok_spec, seq_spec, mat_spec, vec_spec, mat_spec, mat_spec, vec_spec, mat_spec, mat_spec), out_specs=(seq_spec, tok_spec, part_vec, tok_spec, tok_spec, part_vec, tok_spec, tok_spec), check_vma=False)
```
